32 devices in a mesh: gx: 4 (over y, core), gy: 4 (over z), gz: 2 (over x).
Axes of the slice: x: 2, y: 2, z: 4, core: 2. Of those that a mesh axis runs over, the one named last changes fastest.
Arguments:
- order_param: float32 [16, 64, 256], P('gx', 'gy', 'gz'), may hold values from -1 to 1
- density: float32 [16, 64, 256], P('gx', 'gy', 'gz'), may hold values from 0.7 to 1.3
- velocity: float32 [3, 16, 64, 256], P(None, 'gx', 'gy', 'gz'), may hold values from -0.3 to 0.3
Outputs:
- final_order: float32 [16, 64, 256], P('gx', 'gy', 'gz')
- populations: float32 [19, 16, 64, 256], P(None, 'gx', 'gy', 'gz')
The draws below stay inside these ranges and needn't reach their ends.
All inputs are finite; a program needn't handle non-finite values.
Results may differ from the reference program's by a relative error of at most 0.0001.
Values sent between devices are 32-bit elements; how exact they have to be, the bound alone decides.
A program may use at most 64 MiB of HBM per device.

```python
import jax
import jax.numpy as jnp

ITERS = 5
NX = 16
NY = 64
NZ = 256


def block_scale(rng, extent, shards, smallest, top_value):
    factor_of, own = 1.0, jax.random.fold_in(rng, 6)
    for dim, shards_of in shards:
        draws = jnp.exp(jax.random.uniform(jax.random.fold_in(own, dim), (shards_of,), jnp.float32, smallest / len(shards), top_value / len(shards)))
        factor_of = factor_of * jnp.repeat(draws, extent[dim] // shards_of).reshape([-1 if axis == dim else 1 for axis in range(len(extent))])
    return factor_of


def bell_draw(rng, shape, deviation, reach, split=(), held_as=jnp.bfloat16):
    entries = jax.random.normal(rng, shape, jnp.float32) * deviation
    if len(split) > 0:
        entries = block_scale(rng, shape, split, -0.22, 0.18) * entries
    return jnp.clip(entries, min=-reach, max=reach).astype(held_as)


def setup_inputs(seed: int = 0) -> dict:
    seeds = jax.random.split(jax.random.key(seed), 4)
    return {
        "order_param": jnp.clip(jax.random.uniform(seeds[0], (NX, NY, NZ), jnp.float32, -1.0, 1.0) * block_scale(seeds[0], (NX, NY, NZ), ((0, 4), (1, 4), (2, 2)), -0.4, 0.0), -1.0, 1.0),
        "density": jnp.clip(0.7 + 0.59999996 * jax.random.uniform(seeds[1], (NX, NY, NZ), jnp.float32) ** block_scale(seeds[1], (NX, NY, NZ), ((0, 4), (1, 4), (2, 2)), -0.2, 0.2), 0.7, 1.3),
        "velocity": bell_draw(seeds[2], (3, NX, NY, NZ), 0.1, 0.3, ((1, 4), (2, 4), (3, 2)), jnp.float32),
    }


DIRECTIONS = [(0, 0, 0), (1, 0, 0), (-1, 0, 0), (0, 1, 0), (0, -1, 0), (0, 0, 1), (0, 0, -1),
              (1, 1, 0), (-1, -1, 0), (1, -1, 0), (-1, 1, 0), (1, 0, 1), (-1, 0, -1), (1, 0, -1),
              (-1, 0, 1), (0, 1, 1), (0, -1, -1), (0, 1, -1), (0, -1, 1)]
WEIGHTS = [1.0 / 3.0] + [1.0 / 18.0] * 6 + [1.0 / 36.0] * 12
quadratic = -0.1
quartic = 0.1
stiffness = 0.02
mobility = 0.5
relax_time = 0.8


def equilibrium(dens, flow):
    usq = flow[0] * flow[0] + flow[1] * flow[1] + flow[2] * flow[2]
    out = []
    for i in range(19):
        along = jnp.zeros_like(dens)
        for d in range(3):
            if DIRECTIONS[i][d] != 0:
                along = along + DIRECTIONS[i][d] * flow[d]
        out.append(WEIGHTS[i] * dens * (1.0 + 3.0 * along + 4.5 * along * along - 1.5 * usq))
    return jnp.stack(out)


def moments(pops):
    dens = jnp.sum(pops, axis=0)
    moms = []
    for d in range(3):
        total = jnp.zeros_like(dens)
        for i in range(19):
            if DIRECTIONS[i][d] == 1:
                total = total + pops[i]
            elif DIRECTIONS[i][d] == -1:
                total = total - pops[i]
        moms.append(total)
    return dens, jnp.stack(moms)


def reference(order_param, density, velocity):
    order = order_param
    pops = equilibrium(density, velocity)
    for step in range(ITERS):
        beside = -6.0 * order
        for d in range(3):
            beside = beside + jnp.roll(order, 1, d) + jnp.roll(order, -1, d)
        chem = quadratic * order + quartic * order * order * order - stiffness * beside
        force = jnp.stack([-order * (jnp.roll(chem, -1, d) - jnp.roll(chem, 1, d)) * 0.5 for d in range(3)])
        dens, moms = moments(pops)
        vel = moms / dens
        base = equilibrium(dens, vel)
        moved = equilibrium(dens, vel + force / dens)
        post = pops - (pops - base) / relax_time + moved - base
        pops = jnp.stack([jnp.roll(post[i], DIRECTIONS[i], (0, 1, 2)) for i in range(19)])
        dens2, moms2 = moments(pops)
        flow = moms2 / dens2
        change = jnp.zeros_like(order)
        for d in range(3):
            flux = 0.25 * (flow[d] + jnp.roll(flow[d], -1, d)) * (order + jnp.roll(order, -1, d)) - mobility * (jnp.roll(chem, -1, d) - chem)
            change = change + flux - jnp.roll(flux, 1, d)
        order = order - change
    return order, pops
```

```python
import functools

import jax
import jax.numpy as jnp
from jax import lax
from jax.experimental import pallas as pl
from jax.experimental.pallas import tpu as pltpu
from jax.sharding import PartitionSpec as P

ITERS = 5
MESH = pl.DeviceIdType.MESH
AXES = ("gx", "gy", "gz")
DIRS = [
    (0, 0, 0),
    (1, 0, 0),
    (-1, 0, 0),
    (0, 1, 0),
    (0, -1, 0),
    (0, 0, 1),
    (0, 0, -1),
    (1, 1, 0),
    (-1, -1, 0),
    (1, -1, 0),
    (-1, 1, 0),
    (1, 0, 1),
    (-1, 0, -1),
    (1, 0, -1),
    (-1, 0, 1),
    (0, 1, 1),
    (0, -1, -1),
    (0, 1, -1),
    (0, -1, 1),
]
WEIGHTS = [1.0 / 3.0] + [1.0 / 18.0] * 6 + [1.0 / 36.0] * 12
quadratic = -0.1
quartic = 0.1
stiffness = 0.02
mobility = 0.5
relax_time = 0.8

SIGNS = (1, -1)
INDEX = {1: 0, -1: 1}
TRAVEL = {0: 0, 1: 1, -1: 2}
CROSS = [{s: [i for i in range(19) if DIRS[i][d] == s] for s in SIGNS} for d in range(3)]
EDGES = [(a, b) for a in SIGNS for b in SIGNS]
ZPAIRS = [
    (DIRS.index((a, b, 1)), DIRS.index((a, b, -1)))
    for a, b in ((0, 0), (1, 0), (-1, 0), (0, 1), (0, -1))
]
LANES = 8
DEEP = 3
HALF = 64
MOMS = 4


def kernel(sizes, order_in, dens_in, vel_in, order, pops, *scratch):
    (post, mom, sx, rx, rxo, sy, ry, sz, fz, fy, fl) = scratch[0:11]
    (cx_, cy_, cz_, rcx, rcy, rcz) = scratch[11:17]
    (sa, ra, sc, rc) = scratch[17:21]
    X, Y, Z = order.shape
    E = Y + 16
    own_rows = slice(8, 8 + Y)
    block = 2 * DEEP
    width = X * block
    me = [lax.axis_index(a) for a in AXES]
    zsides = (1,) if sizes[2] == 2 else SIGNS

    def device(off):
        return {
            a: lax.rem(me[k] + (off[k] + sizes[k]), sizes[k]) if off[k] else me[k]
            for k, a in enumerate(AXES)
        }

    partners = [
        (a, b, c)
        for a in (0, 1, -1)
        for b in (0, 1, -1)
        for c in (0, 1, -1)
        if (a, b, c) != (0, 0, 0)
    ]
    barrier = pltpu.get_barrier_semaphore()
    for off in partners:
        pl.semaphore_signal(barrier, inc=1, device_id=device(off), device_id_type=MESH)

    lane = lax.broadcasted_iota(jnp.int32, (Y, Z), 1)
    row = lax.broadcasted_iota(jnp.int32, (Y, Z), 0)
    elane = lax.broadcasted_iota(jnp.int32, (E, Z), 1)
    left = elane < HALF
    frame = jnp.where(left, elane, elane - HALF)
    inner = lax.rem(frame, block) < DEEP
    zsign = jnp.where(left, 1.0, -1.0)
    low_col = lane < HALF

    def roll(v, s, axis):
        s = s % v.shape[axis]
        return v if s == 0 else pltpu.roll(v, s, axis)

    def zend(s):
        return 0 if s == 1 else Z - 1

    def yend(s):
        return 0 if s == 1 else Y - 1

    def xsrc(s):
        return X - 1 if s == 1 else 0

    def ysrc(s):
        return Y - 1 if s == 1 else 0

    def ybase(s):
        return 4 if s == 1 else 0

    def zat(px, s):
        return (px + DEEP) * block + (DEEP - 1 if s == 1 else HALF + DEEP)

    def zshift(v, s, packed, at):
        lanes = lane if v.shape[0] == Y else elane
        col = roll(packed, zend(s) - at, 1)
        return jnp.where(lanes == zend(s), col, roll(v, s, 1))

    def yshift(v, s, halo):
        return jnp.where(row == yend(s), jnp.broadcast_to(halo, v.shape), roll(v, s, 0))

    def pack(planes, s):
        acc = jnp.zeros((Y, Z), jnp.float32)
        for x in range(X):
            at = 1 + x
            acc = jnp.where(lane == at, roll(planes[x], at - (Z - 1 if s == 1 else 0), 1), acc)
        return acc

    def run(messages, ssem, rsem, first=0):
        copies = []
        for k, (src, dst, off) in enumerate(messages, first):
            copy = pltpu.make_async_remote_copy(
                src_ref=src,
                dst_ref=dst,
                send_sem=ssem.at[k],
                recv_sem=rsem.at[k],
                device_id=device(off),
                device_id_type=MESH,
            )
            copy.start()
            copies.append(copy)
        return copies

    def finish(copies):
        for copy in copies:
            copy.wait_recv()
        for copy in copies:
            copy.wait_send()

    def moments(ps):
        rho = ps[0]
        for i in range(1, 19):
            rho = rho + ps[i]
        moms = []
        for d in range(3):
            up = functools.reduce(lambda a, b: a + b, [ps[i] for i in CROSS[d][1]])
            down = functools.reduce(lambda a, b: a + b, [ps[i] for i in CROSS[d][-1]])
            moms.append(up - down)
        return rho, moms

    def chemical(o, beside):
        return quadratic * o + quartic * o * o * o - stiffness * (beside - 6.0 * o)

    def along(i, w):
        a = None
        for d in range(3):
            if DIRS[i][d]:
                t = w[d] if DIRS[i][d] == 1 else -w[d]
                a = t if a is None else a + t
        return a

    keep = 1.0 - 1.0 / relax_time
    mix = 1.0 / relax_time - 1.0

    def relaxed(x, ps, rho, u):
        flat = (mix * rho) * (1.0 - 1.5 * (u[0] * u[0] + u[1] * u[1] + u[2] * u[2]))
        out = [keep * ps[0] + WEIGHTS[0] * flat]
        for i in range(1, 19, 2):
            a = along(i, u)
            even = WEIGHTS[i] * flat + (4.5 * mix * WEIGHTS[i]) * rho * (a * a)
            odd = (3.0 * mix * WEIGHTS[i]) * rho * a
            out.append(keep * ps[i] + even + odd)
            out.append(keep * ps[i + 1] + even - odd)
        return out

    def place(acc, v, slot, x):
        at = slot * width + x * block
        mask = (lane >= at) & (lane < at + block)
        return jnp.where(mask, roll(v, at - (Z - DEEP), 1), acc)

    def ready(x, ps, rho, u):
        out = relaxed(x, ps, rho, u)
        heads = [rho] + u
        for i in range(19):
            post[i, x] = out[i]
        for g in range(MOMS):
            mom[g, x] = heads[g]
        for s in SIGNS:
            if x == xsrc(s):
                for g in range(MOMS):
                    sx[INDEX[s], g] = heads[g]
                for k, i in enumerate(CROSS[0][s]):
                    sx[INDEX[s], MOMS + k] = out[i]
            y, at = ysrc(s), ybase(s) + x
            for g in range(MOMS):
                sy[INDEX[s], 3 + X + g, at : at + 1, :] = heads[g][y : y + 1, :]
            for k, i in enumerate(CROSS[1][s]):
                sy[INDEX[s], 3 + X + MOMS + k, at : at + 1, :] = out[i][y : y + 1, :]
        first = sz[0]
        for g in range(MOMS):
            first = place(first, heads[g], 1 + g, x)
        sz[0] = first
        second = sz[1]
        for k, (up, down) in enumerate(ZPAIRS):
            second = place(second, jnp.where(low_col, out[down], out[up]), k, x)
        sz[1] = second

    def forced(rho, inv, u, force):
        v = [u[d] + force[d] * inv for d in range(3)]
        flat = rho * (1.0 - 1.5 * (v[0] * v[0] + v[1] * v[1] + v[2] * v[2]))
        return v, flat

    def one(i, rho, a, flat):
        return WEIGHTS[i] * (flat + rho * (a * (3.0 + 4.5 * a)))

    for ref in (sy, cy_, sz):
        ref[...] = jnp.zeros_like(ref)

    for x in range(X):
        order[x] = order_in[x]
        r = dens_in[x]
        u = [vel_in[d, x] for d in range(3)]
        usq = 1.0 - 1.5 * (u[0] * u[0] + u[1] * u[1] + u[2] * u[2])
        ps = []
        for i in range(19):
            a = along(i, u)
            if a is None:
                ps.append(WEIGHTS[i] * r * usq)
            else:
                ps.append(WEIGHTS[i] * r * (usq + 3.0 * a + 4.5 * a * a))
        rho, moms = moments(ps)
        inv = 1.0 / rho
        ready(x, ps, rho, [m * inv for m in moms])
    pl.semaphore_wait(barrier, len(partners))

    outer_first = sorted(range(X), key=lambda x: (min(x, X - 1 - x), x))

    def step(n, carry):
        par = lax.rem(n, 2)
        O = [order[x] for x in range(X)]
        for x in range(X):
            for s in SIGNS:
                sy[INDEX[s], 3 + x] = O[x][Y - 8 :, :] if s == 1 else O[x][:8, :]
        first = sz[0]
        for x in range(X):
            first = place(first, O[x], 0, x)
        sz[0] = first

        messages = []
        for c in zsides:
            for b in (1, -1, 0):
                for a in (1, -1, 0):
                    dst = fz.at[par, INDEX[c], TRAVEL[a]]
                    if b == 0:
                        src, dst = sz, dst.at[:, pl.ds(8, Y), :]
                    elif b == 1:
                        src, dst = sz.at[:, pl.ds(Y - 4, 4), :], dst.at[:, pl.ds(4, 4), :]
                    else:
                        src, dst = sz.at[:, pl.ds(0, 4), :], dst.at[:, pl.ds(8 + Y, 4), :]
                    messages.append((src, dst, (a, b, c)))
        for s in SIGNS:
            si = INDEX[s]
            rows = pl.ds(ybase(s), 4)
            span = pl.ds(3, X + MOMS + 5)
            messages.append((sy.at[si, span, rows, :], ry.at[par, si, span, rows, :], (0, s, 0)))
        for a, b in EDGES:
            bi = INDEX[b]
            rows = pl.ds(ybase(b), 4)
            src = pl.ds(3 + X - 3 if a == 1 else 3, 3)
            dst = pl.ds(0 if a == 1 else 3 + X + MOMS + 5, 3)
            messages.append((sy.at[bi, src, rows, :], ry.at[par, bi, dst, rows, :], (a, b, 0)))
            span = pl.ds(3 + X, MOMS + 5)
            src = pl.ds(ybase(b) + xsrc(a), 1)
            dst = pl.ds((ybase(b) + (-1 if a == 1 else X)) % 8, 1)
            messages.append((sy.at[bi, span, src, :], ry.at[par, bi, span, dst, :], (a, b, 0)))
        for s in SIGNS:
            si = INDEX[s]
            planes = order.at[pl.ds(X - 3, 3)] if s == 1 else order.at[pl.ds(0, 3)]
            messages.append((planes, rxo.at[par, si], (s, 0, 0)))
            messages.append((sx.at[si], rx.at[par, si], (s, 0, 0)))
        flying = run(messages, sa, ra.at[par])
        finish(flying)

        OE = {}
        for px in range(-DEEP, X + DEEP):
            if px < 0:
                mid, at = rxo[par, 0, px + DEEP], px + DEEP
            elif px >= X:
                mid, at = rxo[par, 1, px - X], 3 + X + MOMS + 5 + px - X
            else:
                mid, at = O[px], 3 + px
            OE[px] = jnp.concatenate([ry[par, 0, at], mid, ry[par, 1, at]], axis=0)

        def far(slot):
            plane, off = slot // 5, (slot % 5) * width
            base = DEEP * block
            out = []
            for c in zsides:
                parts = [fz[par, INDEX[c], TRAVEL[a], plane] for a in (0, 1, -1)]
                v = roll(parts[0], base - off, 1)
                v = jnp.where(frame < base, roll(parts[1], base - width - off, 1), v)
                v = jnp.where(frame >= base + width, roll(parts[2], base + width - off, 1), v)
                out.append(v)
            return out

        def far2(slot):
            plane, off = slot // 5, (slot % 5) * width
            base = DEEP * block
            halves = []
            for k, c in enumerate(zsides):
                parts = [fz[par, INDEX[c], TRAVEL[a], plane] for a in (0, 1, -1)]
                add = HALF * k
                v = roll(parts[0], base - off + add, 1)
                v = jnp.where(frame < base, roll(parts[1], base - width - off + add, 1), v)
                v = jnp.where(frame >= base + width, roll(parts[2], base + width - off + add, 1), v)
                halves.append(v)
            if len(halves) == 1:
                halves.append(roll(halves[0], HALF, 1))
            return jnp.where(left, halves[0], halves[1])

        near = jnp.zeros((E, Z), jnp.float32)
        for px in range(-DEEP, X + DEEP):
            at = (px + DEEP) * block
            mask = (elane >= at) & (elane < at + block)
            near = jnp.where(mask, roll(OE[px], at - (Z - DEEP), 1), near)
        near = jnp.where(left, near, roll(near, HALF, 1))
        OZ = jnp.where(left == inner, far2(0), near)

        C, pairs = {}, []
        for px in range(-2, X + 2):
            o = OE[px]
            around = {
                (0, 1): OE[px - 1],
                (0, -1): OE[px + 1],
                (1, 1): roll(o, 1, 0),
                (1, -1): roll(o, -1, 0),
                (2, 1): zshift(o, 1, OZ, zat(px, 1)),
                (2, -1): zshift(o, -1, OZ, zat(px, -1)),
            }
            C[px] = chemical(o, functools.reduce(lambda a, b: a + b, around.values()))
            if 0 <= px < X:
                pairs.append({k: O[px] + v[own_rows, :] for k, v in around.items()})
        beside = roll(OZ, 1, 0) + roll(OZ, -1, 0) + roll(OZ, 1, 1) + roll(OZ, -1, 1)
        beside = beside + roll(OZ, block, 1) + roll(OZ, -block, 1)
        CZ = chemical(OZ, beside)

        F, diffused = {}, []
        for px in range(-1, X + 1):
            c = C[px]
            y_dn, y_up = roll(c, 1, 0), roll(c, -1, 0)
            z_dn, z_up = zshift(c, 1, CZ, zat(px, 1)), zshift(c, -1, CZ, zat(px, -1))
            scale = -0.5 * OE[px]
            F[px] = [
                scale * (C[px + 1] - C[px - 1]),
                scale * (y_up - y_dn),
                scale * (z_up - z_dn),
            ]
            if 0 <= px < X:
                lap = C[px + 1] + C[px - 1] + y_up + y_dn + z_up + z_dn - 6.0 * c
                diffused.append(lap[own_rows, :])
            for s in SIGNS:
                at = (ybase(s) + px) % 8
                y = 7 if s == 1 else 8 + Y
                for d in range(3):
                    fy[INDEX[s], d, at : at + 1, :] = F[px][d][y : y + 1, :]
        scale = -0.5 * OZ
        FZ = [
            scale * (roll(CZ, -block, 1) - roll(CZ, block, 1)),
            scale * (roll(CZ, -1, 0) - roll(CZ, 1, 0)),
            scale * (roll(CZ, -1, 1) - roll(CZ, 1, 1)),
        ]

        XH, YH, ZH = {}, {}, {}
        for s in SIGNS:
            si = INDEX[s]
            rho = rx[par, si, 0]
            u = [rx[par, si, 1 + d] for d in range(3)]
            px = -1 if s == 1 else X
            v, flat = forced(rho, 1.0 / rho, u, [f[own_rows, :] for f in F[px]])
            for k, i in enumerate(CROSS[0][s]):
                XH[i] = rx[par, si, MOMS + k] + one(i, rho, along(i, v), flat)
            g = 3 + X
            rho = ry[par, si, g]
            u = [ry[par, si, g + 1 + d] for d in range(3)]
            v, flat = forced(rho, 1.0 / rho, u, [fy[si, d] for d in range(3)])
            for k, i in enumerate(CROSS[1][s]):
                YH[i] = ry[par, si, g + MOMS + k] + one(i, rho, along(i, v), flat)
        rho = far2(1)
        u = [far2(2 + d) for d in range(3)]
        v, flat = forced(rho, 1.0 / rho, u, FZ)
        for k, (up, down) in enumerate(ZPAIRS):
            a = zsign * v[2]
            for d in range(2):
                if DIRS[up][d]:
                    a = a + v[d] if DIRS[up][d] == 1 else a - v[d]
            h = far2(5 + k) + one(up, rho, a, flat)
            h = roll(h, DIRS[up][1], 0)[own_rows, :]
            ZH[up] = ZH[down] = h

        for x in range(X):
            rho = mom[0, x]
            u = [mom[1 + d, x] for d in range(3)]
            v, flat = forced(rho, 1.0 / rho, u, [f[own_rows, :] for f in F[x]])
            post[0, x] = post[0, x] + WEIGHTS[0] * flat
            for i in range(1, 19, 2):
                a = along(i, v)
                even = WEIGHTS[i] * flat + (4.5 * WEIGHTS[i]) * rho * (a * a)
                odd = (3.0 * WEIGHTS[i]) * rho * a
                post[i, x] = post[i, x] + even + odd
                post[i + 1, x] = post[i + 1, x] + even - odd

        flows = {}
        for x in outer_first:
            ps = []
            for i, (cx, cy, cz) in enumerate(DIRS):
                xs = x - cx
                p = post[i, xs] if 0 <= xs < X else XH[i]
                if cy:
                    at = (ybase(cy) + xs) % 8
                    p = yshift(p, cy, YH[i][at : at + 1, :])
                if cz:
                    p = zshift(p, cz, ZH[i], zat(xs, cz))
                pops[i, x] = p
                ps.append(p)
            rho, moms = moments(ps)
            inv = 1.0 / rho
            flows[x] = [m * inv for m in moms]
            mom[0, x] = rho
            for s in SIGNS:
                if x == xsrc(s):
                    cx_[INDEX[s]] = flows[x][0]
                y = ysrc(s)
                cy_[INDEX[s], 1 + x : 2 + x, :] = flows[x][1][y : y + 1, :]
        messages = []
        for s in SIGNS:
            messages.append((cy_.at[INDEX[s]], rcy.at[INDEX[s]], (0, s, 0)))
        for s in SIGNS:
            cz_[INDEX[s]] = pack([flows[x][2] for x in range(X)], s)
            messages.append((cz_.at[INDEX[s]], rcz.at[INDEX[s]], (0, 0, s)))
        for s in SIGNS:
            messages.append((cx_.at[INDEX[s]], rcx.at[INDEX[s]], (s, 0, 0)))
        flying = run(messages, sc, rc)

        for x in range(X):
            ready(x, [pops[i, x] for i in range(19)], mom[0, x], flows[x])
        finish(flying)

        for x in range(X):
            f, pair = flows[x], pairs[x]
            fx_up = flows[x + 1][0] if x + 1 < X else rcx[1]
            fx_dn = flows[x - 1][0] if x > 0 else rcx[0]
            change = (f[0] + fx_up) * pair[(0, -1)] - (f[0] + fx_dn) * pair[(0, 1)]
            for s in SIGNS:
                gy = yshift(f[1], s, rcy[INDEX[s], 1 + x : 2 + x, :])
                gz = zshift(f[2], s, rcz[INDEX[s]], 1 + x)
                part = (f[1] + gy) * pair[(1, s)] + (f[2] + gz) * pair[(2, s)]
                change = change - part if s == 1 else change + part
            order[x] = O[x] - (0.25 * change - mobility * diffused[x])
        return carry

    lax.fori_loop(0, ITERS, step, 0)


def on_device(sizes, order_param, density, velocity):
    X, Y, Z = order_param.shape
    f32 = jnp.float32
    plane, rows, tall = (Y, Z), (8, Z), (Y + 16, Z)
    tiles = X + 6 + MOMS + 5
    vmem = [
        (19, X, Y, Z), (MOMS, X, Y, Z),
        (2, MOMS + 5) + plane, (2, 2, MOMS + 5) + plane, (2, 2, 3) + plane,
        (2, tiles) + rows, (2, 2, tiles) + rows,
        (2,) + plane, (2, 2, 3, 2) + tall,
        (2, 3) + rows, (8, Z),
        (2,) + plane, (2,) + rows, (2,) + plane,
        (2,) + plane, (2,) + rows, (2,) + plane,
    ]
    count = (9 if sizes[2] == 2 else 18) + 14
    sems = [(count,), (2, count), (6,), (6,)]
    spec = pl.BlockSpec(memory_space=pltpu.VMEM)
    return pl.pallas_call(
        functools.partial(kernel, sizes),
        out_shape=(
            jax.ShapeDtypeStruct((X, Y, Z), f32),
            jax.ShapeDtypeStruct((19, X, Y, Z), f32),
        ),
        in_specs=[spec] * 3,
        out_specs=(spec, spec),
        scratch_shapes=[pltpu.VMEM(s, f32) for s in vmem]
        + [pltpu.SemaphoreType.DMA(n) for n in sems],
        compiler_params=pltpu.CompilerParams(collective_id=0, has_side_effects=True),
    )(order_param, density, velocity)


def solution(mesh):
    sizes = tuple(mesh.shape[a] for a in AXES)
    return jax.shard_map(
        functools.partial(on_device, sizes),
        mesh=mesh,
        in_specs=(P("gx", "gy", "gz"), P("gx", "gy", "gz"), P(None, "gx", "gy", "gz")),
        out_specs=(P("gx", "gy", "gz"), P(None, "gx", "gy", "gz")),
        check_vma=False,
    )
```

```python
import functools

import jax
import jax.numpy as jnp
from jax import lax
from jax.experimental import pallas as pl
from jax.experimental.pallas import tpu as pltpu
from jax.sharding import PartitionSpec as P

ITERS = 5
MESH = pl.DeviceIdType.MESH
AXES = ("gx", "gy", "gz")
DIRS = [
    (0, 0, 0),
    (1, 0, 0),
    (-1, 0, 0),
    (0, 1, 0),
    (0, -1, 0),
    (0, 0, 1),
    (0, 0, -1),
    (1, 1, 0),
    (-1, -1, 0),
    (1, -1, 0),
    (-1, 1, 0),
    (1, 0, 1),
    (-1, 0, -1),
    (1, 0, -1),
    (-1, 0, 1),
    (0, 1, 1),
    (0, -1, -1),
    (0, 1, -1),
    (0, -1, 1),
]
WEIGHTS = [1.0 / 3.0] + [1.0 / 18.0] * 6 + [1.0 / 36.0] * 12
quadratic = -0.1
quartic = 0.1
stiffness = 0.02
mobility = 0.5
relax_time = 0.8

SIGNS = (1, -1)
INDEX = {1: 0, -1: 1}
TRAVEL = {0: 0, 1: 1, -1: 2}
CROSS = [{s: [i for i in range(19) if DIRS[i][d] == s] for s in SIGNS} for d in range(3)]
EDGES = [(a, b) for a in SIGNS for b in SIGNS]
ZPAIRS = [
    (DIRS.index((a, b, 1)), DIRS.index((a, b, -1)))
    for a, b in ((0, 0), (1, 0), (-1, 0), (0, 1), (0, -1))
]
DEEP = 3
HALF = 64
MOMS = 4


def kernel(sizes, order_in, dens_in, vel_in, order, pops, *scratch):
    (post, mom, base, oe, oz) = scratch[0:5]
    (sx, rx, sy, ry, rxy, sl, rl, sz, fz, fy) = scratch[5:15]
    (cx_, cy_, cz_, rcx, rcy, rcz) = scratch[15:21]
    (sa, ra, sc, rc) = scratch[21:25]
    X, Y, Z = order.shape
    E = Y + 16
    own_rows = slice(8, 8 + Y)
    block = 2 * DEEP
    width = X * block
    me = [lax.axis_index(a) for a in AXES]
    zsides = (1,) if sizes[2] == 2 else SIGNS

    def device(off):
        return {
            a: lax.rem(me[k] + (off[k] + sizes[k]), sizes[k]) if off[k] else me[k]
            for k, a in enumerate(AXES)
        }

    partners = [
        (a, b, c)
        for a in (0, 1, -1)
        for b in (0, 1, -1)
        for c in (0, 1, -1)
        if (a, b, c) != (0, 0, 0)
    ]
    barrier = pltpu.get_barrier_semaphore()
    for off in partners:
        pl.semaphore_signal(barrier, inc=1, device_id=device(off), device_id_type=MESH)

    lane = lax.broadcasted_iota(jnp.int32, (Y, Z), 1)
    row = lax.broadcasted_iota(jnp.int32, (Y, Z), 0)
    elane = lax.broadcasted_iota(jnp.int32, (E, Z), 1)
    erow = lax.broadcasted_iota(jnp.int32, (E, Z), 0)
    left = elane < HALF
    frame = jnp.where(left, elane, elane - HALF)
    column = lax.rem(frame, block)
    facing = lax.rem(elane, block) < DEEP
    zsign = jnp.where(left, 1.0, -1.0)
    low_col = lane < HALF
    face_z = column == DEEP
    face_x = (frame // block == DEEP) | (frame // block == DEEP + X)
    face_y = (erow == 8) | (erow == 8 + Y)
    below = jnp.where(erow == 8, 1.0, jnp.where(erow == 7, -1.0, 0.0))
    above = jnp.where(erow == 8 + Y, 1.0, jnp.where(erow == 7 + Y, -1.0, 0.0))

    def roll(v, s, axis):
        s = s % v.shape[axis]
        return v if s == 0 else pltpu.roll(v, s, axis)

    def zend(s):
        return 0 if s == 1 else Z - 1

    def yend(s):
        return 0 if s == 1 else Y - 1

    def xsrc(s):
        return X - 1 if s == 1 else 0

    def ysrc(s):
        return Y - 1 if s == 1 else 0

    def deep_rows(s):
        return pl.ds(8 - DEEP if s == 1 else 0, DEEP)

    def flat_rows(s):
        return pl.ds(0 if s == 1 else 4, X)

    def zat(px, s):
        return (px + DEEP) * block + (DEEP - 1 if s == 1 else HALF + DEEP)

    def zshift(v, s, packed, at):
        lanes = lane if v.shape[0] == Y else elane
        col = roll(packed, zend(s) - at, 1)
        return jnp.where(lanes == zend(s), col, roll(v, s, 1))

    def yshift(v, s, halo):
        return jnp.where(row == yend(s), jnp.broadcast_to(halo, v.shape), roll(v, s, 0))

    def pack(planes, s):
        acc = jnp.zeros((Y, Z), jnp.float32)
        for x in range(X):
            at = 1 + x
            acc = jnp.where(lane == at, roll(planes[x], at - (Z - 1 if s == 1 else 0), 1), acc)
        return acc

    def copies(messages, ssem, rsem):
        return [
            pltpu.make_async_remote_copy(
                src_ref=src,
                dst_ref=dst,
                send_sem=ssem.at[k],
                recv_sem=rsem.at[k],
                device_id=device(off),
                device_id_type=MESH,
            )
            for k, (src, dst, off) in enumerate(messages)
        ]

    def launch(flying):
        for copy in flying:
            copy.start()

    def finish(flying):
        for copy in flying:
            copy.wait_recv()
        for copy in flying:
            copy.wait_send()

    def bundle(par):
        messages = []
        for c in zsides:
            for b in (1, -1, 0):
                for a in (1, -1, 0):
                    dst = fz.at[par, INDEX[c], TRAVEL[a]]
                    rows = {1: pl.ds(Y - DEEP, DEEP), -1: pl.ds(0, DEEP), 0: pl.ds(0, Y)}[b]
                    land = {1: 8 - DEEP, -1: 8 + Y, 0: 8}[b]
                    land = pl.ds(land, DEEP if b else Y)
                    planes = pl.ds(0, 1 if a and b else 2)
                    messages.append((sz.at[planes, rows, :], dst.at[planes, land, :], (a, b, c)))
        for a, b in EDGES:
            bi, ai, rows = INDEX[b], INDEX[a], deep_rows(b)
            src = pl.ds(X - 1 if a == 1 else 0, 5)
            messages.append((sy.at[bi, src, rows, :], rxy.at[par, bi, ai, :, rows, :], (a, b, 0)))
            messages.append((sl.at[bi, ai], rl.at[par, bi, ai], (a, b, 0)))
        for s in SIGNS:
            si = INDEX[s]
            for span, rows in ((MOMS + 5, flat_rows(s)), (X + 4, deep_rows(s))):
                span = pl.ds(0, span)
                messages.append((sy.at[si, span, rows, :], ry.at[par, si, span, rows, :], (0, s, 0)))
        for s in SIGNS:
            messages.append((sx.at[INDEX[s]], rx.at[par, INDEX[s]], (s, 0, 0)))
        return copies(messages, sa, ra.at[par])

    def farewell():
        messages = []
        for s in SIGNS:
            messages.append((cy_.at[INDEX[s]], rcy.at[INDEX[s]], (0, s, 0)))
        for s in SIGNS:
            messages.append((cz_.at[INDEX[s]], rcz.at[INDEX[s]], (0, 0, s)))
        for s in SIGNS:
            messages.append((cx_.at[INDEX[s]], rcx.at[INDEX[s]], (s, 0, 0)))
        return copies(messages, sc, rc)

    def moments(ps):
        rho = ps[0]
        for i in range(1, 19):
            rho = rho + ps[i]
        moms = []
        for d in range(3):
            up = functools.reduce(lambda a, b: a + b, [ps[i] for i in CROSS[d][1]])
            down = functools.reduce(lambda a, b: a + b, [ps[i] for i in CROSS[d][-1]])
            moms.append(up - down)
        return rho, moms

    def chemical(o, beside):
        return quadratic * o + quartic * o * o * o - stiffness * (beside - 6.0 * o)

    def along(i, w):
        a = None
        for d in range(3):
            if DIRS[i][d]:
                t = w[d] if DIRS[i][d] == 1 else -w[d]
                a = t if a is None else a + t
        return a

    keep = 1.0 - 1.0 / relax_time
    mix = 1.0 / relax_time - 1.0

    def relaxed(ps, rho, u):
        flat = (mix * rho) * (1.0 - 1.5 * (u[0] * u[0] + u[1] * u[1] + u[2] * u[2]))
        out = [keep * ps[0] + WEIGHTS[0] * flat]
        for i in range(1, 19, 2):
            a = along(i, u)
            even = WEIGHTS[i] * flat + (4.5 * mix * WEIGHTS[i]) * rho * (a * a)
            odd = (3.0 * mix * WEIGHTS[i]) * rho * a
            out.append(keep * ps[i] + even + odd)
            out.append(keep * ps[i + 1] + even - odd)
        return out

    def place(acc, v, slot, x):
        at = slot * width + x * block
        mask = (lane >= at) & (lane < at + block)
        return jnp.where(mask, roll(v, at - (Z - DEEP), 1), acc)

    def ready():
        first = jnp.zeros((Y, Z), jnp.float32)
        second = jnp.zeros((Y, Z), jnp.float32)
        for x in range(X):
            rho = mom[0, x]
            u = [mom[1 + d, x] for d in range(3)]
            out = relaxed([pops[i, x] for i in range(19)], rho, u)
            heads, b = [rho] + u, base[x]
            for i in range(19):
                post[i, x] = out[i]
            for s in SIGNS:
                si = INDEX[s]
                if x == xsrc(s):
                    for g in range(MOMS):
                        sx[si, g] = heads[g]
                    for k, i in enumerate(CROSS[0][s]):
                        sx[si, MOMS + k] = out[i]
                slot = x - (X - DEEP) if s == 1 else x
                if 0 <= slot < DEEP:
                    sx[si, MOMS + 5 + slot] = b
                    sx[si, MOMS + 6 + DEEP, slot : slot + 1, :] = u[1][0:1, :]
                    sx[si, MOMS + 6 + DEEP, DEEP + slot : DEEP + slot + 1, :] = u[1][Y - 1 :, :]
                y, at = ysrc(s), (0 if s == 1 else 4) + x
                for g in range(MOMS):
                    sy[si, g, at : at + 1, :] = heads[g][y : y + 1, :]
                for k, i in enumerate(CROSS[1][s]):
                    sy[si, MOMS + k, at : at + 1, :] = out[i][y : y + 1, :]
                rows = slice(Y - DEEP, Y) if s == 1 else slice(0, DEEP)
                sy[si, 2 + x, deep_rows(s), :] = b[rows, :]
                if x == 0:
                    sy[si, 0, deep_rows(s), :] = u[0][rows, :]
                if x == X - 1:
                    sy[si, X + 3, deep_rows(s), :] = u[0][rows, :]
                for a in SIGNS:
                    if x == xsrc(a):
                        for k, v in enumerate(heads + [out[DIRS.index((a, s, 0))]]):
                            sl[si, INDEX[a], k : k + 1, :] = v[y : y + 1, :]
                    slot = x - (X - DEEP) if a == 1 else x - 1
                    if 0 <= slot < DEEP - 1:
                        sl[si, INDEX[a], 5 + slot : 6 + slot, :] = u[1][y : y + 1, :]
            for g, v in enumerate([b] + heads):
                first = place(first, v, g, x)
            for k, (up, down) in enumerate(ZPAIRS):
                second = place(second, jnp.where(low_col, out[down], out[up]), k, x)
        sz[0] = first
        sz[1] = second
        for s in SIGNS:
            si = INDEX[s]
            sx[si, MOMS + 5 + DEEP] = first
            rows = slice(Y - DEEP, Y) if s == 1 else slice(0, DEEP)
            for at in (1, X + 2):
                sy[si, at, deep_rows(s), :] = first[rows, :]

    def forced(rho, inv, u, force):
        v = [u[d] + force[d] * inv for d in range(3)]
        flat = rho * (1.0 - 1.5 * (v[0] * v[0] + v[1] * v[1] + v[2] * v[2]))
        return v, flat

    def one(i, rho, a, flat):
        return WEIGHTS[i] * (flat + rho * (a * (3.0 + 4.5 * a)))

    for ref in (sx, sy, sl, cy_, oe, oz):
        ref[...] = jnp.zeros_like(ref)

    for x in range(X):
        base[x] = order_in[x]
        r = dens_in[x]
        u = [vel_in[d, x] for d in range(3)]
        usq = 1.0 - 1.5 * (u[0] * u[0] + u[1] * u[1] + u[2] * u[2])
        ps = []
        for i in range(19):
            a = along(i, u)
            if a is None:
                ps.append(WEIGHTS[i] * r * usq)
            else:
                ps.append(WEIGHTS[i] * r * (usq + 3.0 * a + 4.5 * a * a))
            pops[i, x] = ps[i]
        rho, moms = moments(ps)
        inv = 1.0 / rho
        mom[0, x] = rho
        for d in range(3):
            mom[1 + d, x] = moms[d] * inv
    ready()
    pl.semaphore_wait(barrier, len(partners))
    launch(bundle(0))

    outer_first = sorted(range(X), key=lambda x: (min(x, X - 1 - x), x))

    def step(n, carry):
        par = lax.rem(n, 2)
        finish(bundle(par))
        low, high = ry.at[par, 0], ry.at[par, 1]

        def tall(a):
            if a == 0:
                near = [low[1], sz[0], high[1]]
            else:
                at = DEEP if a == 1 else 1
                mid = rx[par, INDEX[a], MOMS + 5 + DEEP]
                near = [rxy[par, 0, INDEX[a], at], mid, rxy[par, 1, INDEX[a], at]]
            near = jnp.concatenate(near, axis=0)
            far = [fz[par, INDEX[c], TRAVEL[a], 0] for c in zsides]
            halves = [jnp.where(facing, far[0], near), jnp.where(facing, near, far[-1])]
            return [roll(v, -a * width, 1) for v in halves]

        parts = [tall(a) for a in (0, 1, -1)]
        ends = [
            [roll(fz[par, INDEX[c], TRAVEL[a], 1], -a * width, 1) for a in (0, 1, -1)] for c in zsides
        ]

        def gather(three, slot, add):
            at = slot * width
            rel = lax.rem(elane + (Z - at), Z)
            v = jnp.where(rel < width, three[0], jnp.where(rel < HALF, three[2], three[1]))
            return roll(v, DEEP * block - at + add, 1)

        def packed(slot):
            halves = [gather([p[k] for p in parts], slot, HALF * k) for k in range(2)]
            return jnp.where(left, halves[0], halves[1])

        def packed_far(slot):
            halves = [gather(three, slot, HALF * k) for k, three in enumerate(ends)]
            if len(halves) == 1:
                halves.append(roll(halves[0], HALF, 1))
            return jnp.where(left, halves[0], halves[1])

        rho_z = packed(1)
        u_z = [packed(2 + d) for d in range(3)]
        old = oz[...]
        OZ = packed(0)
        for d, (shift, axis, mask) in enumerate(((block, 1, face_x), (1, 0, face_y), (1, 1, face_z))):
            t = 0.25 * (u_z[d] + roll(u_z[d], shift, axis)) * (old + roll(old, shift, axis))
            t = jnp.where(mask, t, 0.0)
            OZ = OZ + (t - roll(t, -shift, axis))
        oz[...] = OZ

        def around(px, s):
            if px < 0:
                return rxy[par, INDEX[s], 0, px + DEEP]
            if px >= X:
                return rxy[par, INDEX[s], 1, 2 + px - X]
            return ry[par, INDEX[s], 2 + px]

        def speed(px):
            if px < 0:
                tiles, mid = [rxy[par, k, 0, 4] for k in range(2)], rx[par, 0, 1]
            elif px >= X:
                tiles, mid = [rxy[par, k, 1, 0] for k in range(2)], rx[par, 1, 1]
            else:
                tiles, mid = [ry[par, k, 0 if px == 0 else X + 3] for k in range(2)], mom[1, px]
            return jnp.concatenate([tiles[0], mid, tiles[1]], axis=0)

        def outside(px, s):
            si = INDEX[s]
            if px < 0:
                at = 2 if px == -1 else 5 + px + DEEP
                return rl[par, si, 0, at : at + 1, :]
            if px >= X:
                at = 2 if px == X else 5 + px - X - 1
                return rl[par, si, 1, at : at + 1, :]
            at = (0 if s == 1 else 4) + px
            return ry[par, si, 2, at : at + 1, :]

        def inside(px, s):
            if 0 <= px < X:
                y = yend(s)
                return mom[2, px, y : y + 1, :]
            side, slot = (0, px + DEEP) if px < 0 else (1, px - X)
            at = slot if s == 1 else DEEP + slot
            return rx[par, side, MOMS + 6 + DEEP, at : at + 1, :]

        across = {}
        for lo, hi in ((-1, 0), (X - 1, X)):
            t = 0.25 * (speed(lo) + speed(hi)) * (oe[lo + DEEP] + oe[hi + DEEP])
            across[lo], across[hi] = -t, t
        OE = {}
        for px in range(-DEEP, X + DEEP):
            if px < 0:
                mid = rx[par, 0, MOMS + 5 + px + DEEP]
            elif px >= X:
                mid = rx[par, 1, MOMS + 5 + px - X]
            else:
                mid = base[px]
            v = jnp.concatenate([around(px, 1), mid, around(px, -1)], axis=0)
            if px in across:
                v = v + across[px]
            for s, sign, y in ((1, below, 8), (-1, above, 8 + Y)):
                pair = oe[px + DEEP, y - 1 : y, :] + oe[px + DEEP, y : y + 1, :]
                t = 0.25 * (outside(px, s) + inside(px, s)) * pair
                v = v + sign * jnp.broadcast_to(t, v.shape)
            at = (px + DEEP) * block
            v = jnp.where(elane == 0, roll(OZ, -(at + DEEP), 1), v)
            v = jnp.where(elane == Z - 1, roll(OZ, Z - 1 - (HALF + at + DEEP - 1), 1), v)
            OE[px] = v
        for px in range(-DEEP, X + DEEP):
            oe[px + DEEP] = OE[px]
        O = [OE[x][own_rows, :] for x in range(X)]

        C = {}
        for px in range(-2, X + 2):
            o = OE[px]
            beside = OE[px - 1] + OE[px + 1] + roll(o, 1, 0) + roll(o, -1, 0)
            beside = beside + zshift(o, 1, OZ, zat(px, 1)) + zshift(o, -1, OZ, zat(px, -1))
            C[px] = chemical(o, beside)
        beside = roll(OZ, 1, 0) + roll(OZ, -1, 0) + roll(OZ, 1, 1) + roll(OZ, -1, 1)
        beside = beside + roll(OZ, block, 1) + roll(OZ, -block, 1)
        CZ = chemical(OZ, beside)

        F = {}
        for px in range(-1, X + 1):
            c = C[px]
            y_dn, y_up = roll(c, 1, 0), roll(c, -1, 0)
            z_dn, z_up = zshift(c, 1, CZ, zat(px, 1)), zshift(c, -1, CZ, zat(px, -1))
            scale = -0.5 * OE[px]
            F[px] = [
                scale * (C[px + 1] - C[px - 1]),
                scale * (y_up - y_dn),
                scale * (z_up - z_dn),
            ]
            if 0 <= px < X:
                lap = C[px + 1] + C[px - 1] + y_up + y_dn + z_up + z_dn - 6.0 * c
                base[px] = O[px] + mobility * lap[own_rows, :]
                for s in SIGNS:
                    at = (0 if s == 1 else 4) + px
                    y = 7 if s == 1 else 8 + Y
                    for d in range(3):
                        fy[INDEX[s], d, at : at + 1, :] = F[px][d][y : y + 1, :]
        scale = -0.5 * OZ
        FZ = [
            scale * (roll(CZ, -block, 1) - roll(CZ, block, 1)),
            scale * (roll(CZ, -1, 0) - roll(CZ, 1, 0)),
            scale * (roll(CZ, -1, 1) - roll(CZ, 1, 1)),
        ]

        XH, YH, LH, ZH = {}, {}, {}, {}
        for s in SIGNS:
            si = INDEX[s]
            rho = rx[par, si, 0]
            u = [rx[par, si, 1 + d] for d in range(3)]
            px = -1 if s == 1 else X
            v, flat = forced(rho, 1.0 / rho, u, [f[own_rows, :] for f in F[px]])
            for k, i in enumerate(CROSS[0][s]):
                XH[i] = rx[par, si, MOMS + k] + one(i, rho, along(i, v), flat)
            rho = ry[par, si, 0]
            u = [ry[par, si, 1 + d] for d in range(3)]
            v, flat = forced(rho, 1.0 / rho, u, [fy[si, d] for d in range(3)])
            for k, i in enumerate(CROSS[1][s]):
                YH[i] = ry[par, si, MOMS + k] + one(i, rho, along(i, v), flat)
            for a in SIGNS:
                i = DIRS.index((a, s, 0))
                head = [rl[par, si, INDEX[a], k : k + 1, :] for k in range(5)]
                y, px = (7 if s == 1 else 8 + Y), (-1 if a == 1 else X)
                force = [f[y : y + 1, :] for f in F[px]]
                v, flat = forced(head[0], 1.0 / head[0], head[1:4], force)
                LH[i] = head[4] + one(i, head[0], along(i, v), flat)
        v, flat = forced(rho_z, 1.0 / rho_z, u_z, FZ)
        for k, (up, down) in enumerate(ZPAIRS):
            a = zsign * v[2]
            for d in range(2):
                if DIRS[up][d]:
                    a = a + v[d] if DIRS[up][d] == 1 else a - v[d]
            h = packed_far(k) + one(up, rho_z, a, flat)
            ZH[up] = ZH[down] = roll(h, DIRS[up][1], 0)[own_rows, :]

        for x in range(X):
            rho = mom[0, x]
            u = [mom[1 + d, x] for d in range(3)]
            v, flat = forced(rho, 1.0 / rho, u, [f[own_rows, :] for f in F[x]])
            post[0, x] = post[0, x] + WEIGHTS[0] * flat
            for i in range(1, 19, 2):
                a = along(i, v)
                even = WEIGHTS[i] * flat + (4.5 * WEIGHTS[i]) * rho * (a * a)
                odd = (3.0 * WEIGHTS[i]) * rho * a
                post[i, x] = post[i, x] + even + odd
                post[i + 1, x] = post[i + 1, x] + even - odd

        flows = {}
        for x in outer_first:
            ps = []
            for i, (cx, cy, cz) in enumerate(DIRS):
                xs = x - cx
                own = 0 <= xs < X
                p = post[i, xs] if own else XH[i]
                if cy:
                    at = (0 if cy == 1 else 4) + xs
                    p = yshift(p, cy, YH[i][at : at + 1, :] if own else LH[i])
                if cz:
                    p = zshift(p, cz, ZH[i], zat(xs, cz))
                pops[i, x] = p
                ps.append(p)
            rho, moms = moments(ps)
            inv = 1.0 / rho
            flows[x] = [m * inv for m in moms]
            mom[0, x] = rho
            for d in range(3):
                mom[1 + d, x] = flows[x][d]

        @pl.when(n == ITERS - 1)
        def _():
            for s in SIGNS:
                cx_[INDEX[s]] = mom[1, xsrc(s)]
                y = ysrc(s)
                for x in range(X):
                    cy_[INDEX[s], 1 + x : 2 + x, :] = mom[2, x, y : y + 1, :]
                cz_[INDEX[s]] = pack([mom[3, x] for x in range(X)], s)
            launch(farewell())

        tx = {0: 0.0, X: 0.0}
        for x in range(1, X):
            tx[x] = (flows[x][0] + flows[x - 1][0]) * (O[x] + O[x - 1])
        for x in range(X):
            f, o = flows[x], O[x]
            ty = jnp.where(row == 0, 0.0, (f[1] + roll(f[1], 1, 0)) * (o + roll(o, 1, 0)))
            tz = jnp.where(lane == 0, 0.0, (f[2] + roll(f[2], 1, 1)) * (o + roll(o, 1, 1)))
            change = tx[x + 1] - tx[x] + (roll(ty, -1, 0) - ty) + (roll(tz, -1, 1) - tz)
            base[x] = base[x] - 0.25 * change

        @pl.when(n < ITERS - 1)
        def _():
            ready()
            launch(bundle(1 - par))

        return carry

    lax.fori_loop(0, ITERS, step, 0)
    finish(farewell())

    OZ = oz[own_rows, :]
    for x in range(X):
        o, u = oe[x + DEEP, own_rows, :], [mom[1 + d, x] for d in range(3)]
        change = jnp.zeros((Y, Z), jnp.float32)
        if x == 0:
            change = change + (u[0] + rcx[0]) * (o + oe[DEEP - 1, own_rows, :])
        if x == X - 1:
            change = change - (u[0] + rcx[1]) * (o + oe[DEEP + X, own_rows, :])
        for s in SIGNS:
            at = 7 if s == 1 else 8 + Y
            other = rcy[INDEX[s], 1 + x : 2 + x, :]
            y = yend(s)
            t = (mom[2, x, y : y + 1, :] + other) * (
                oe[x + DEEP, at : at + 1, :] + oe[x + DEEP, 8 + y : 9 + y, :]
            )
            t = jnp.where(row == y, jnp.broadcast_to(t, (Y, Z)), 0.0)
            side = roll(OZ, zend(s) - zat(x, s), 1)
            beside = roll(rcz[INDEX[s]], zend(s) - (1 + x), 1)
            t = t + jnp.where(lane == zend(s), (u[2] + beside) * (o + side), 0.0)
            change = change + t if s == 1 else change - t
        order[x] = base[x] + 0.25 * change


def on_device(sizes, order_param, density, velocity):
    X, Y, Z = order_param.shape
    f32 = jnp.float32
    plane, rows, tall = (Y, Z), (8, Z), (Y + 16, Z)
    planes, tiles = MOMS + 5 + DEEP + 2, max(MOMS + 5, X + 4)
    vmem = [
        (19, X, Y, Z), (MOMS, X, Y, Z), (X, Y, Z), (X + 2 * DEEP,) + tall, tall,
        (2, planes) + plane, (2, 2, planes) + plane,
        (2, tiles) + rows, (2, 2, tiles) + rows, (2, 2, 2, 5) + rows,
        (2, 2) + rows, (2, 2, 2) + rows,
        (2,) + plane, (2, 2, 3, 2) + tall, (2, 3) + rows,
        (2,) + plane, (2,) + rows, (2,) + plane,
        (2,) + plane, (2,) + rows, (2,) + plane,
    ]
    count = (9 if sizes[2] == 2 else 18) + 14
    sems = [(count,), (2, count), (6,), (6,)]
    spec = pl.BlockSpec(memory_space=pltpu.VMEM)
    return pl.pallas_call(
        functools.partial(kernel, sizes),
        out_shape=(
            jax.ShapeDtypeStruct((X, Y, Z), f32),
            jax.ShapeDtypeStruct((19, X, Y, Z), f32),
        ),
        in_specs=[spec] * 3,
        out_specs=(spec, spec),
        scratch_shapes=[pltpu.VMEM(s, f32) for s in vmem]
        + [pltpu.SemaphoreType.DMA(n) for n in sems],
        compiler_params=pltpu.CompilerParams(collective_id=0, has_side_effects=True),
    )(order_param, density, velocity)


def solution(mesh):
    sizes = tuple(mesh.shape[a] for a in AXES)
    return jax.shard_map(
        functools.partial(on_device, sizes),
        mesh=mesh,
        in_specs=(P("gx", "gy", "gz"), P("gx", "gy", "gz"), P(None, "gx", "gy", "gz")),
        out_specs=(P("gx", "gy", "gz"), P(None, "gx", "gy", "gz")),
        check_vma=False,
    )
```

```python
import functools

import jax
import jax.numpy as jnp
from jax import lax
from jax.experimental import pallas as pl
from jax.experimental.pallas import tpu as pltpu
from jax.sharding import PartitionSpec as P

ITERS = 5
MESH = pl.DeviceIdType.MESH
AXES = ("gx", "gy", "gz")
DIRS = [
    (0, 0, 0),
    (1, 0, 0),
    (-1, 0, 0),
    (0, 1, 0),
    (0, -1, 0),
    (0, 0, 1),
    (0, 0, -1),
    (1, 1, 0),
    (-1, -1, 0),
    (1, -1, 0),
    (-1, 1, 0),
    (1, 0, 1),
    (-1, 0, -1),
    (1, 0, -1),
    (-1, 0, 1),
    (0, 1, 1),
    (0, -1, -1),
    (0, 1, -1),
    (0, -1, 1),
]
WEIGHTS = [1.0 / 3.0] + [1.0 / 18.0] * 6 + [1.0 / 36.0] * 12
quadratic = -0.1
quartic = 0.1
stiffness = 0.02
mobility = 0.5
relax_time = 0.8

SIGNS = (1, -1)
INDEX = {1: 0, -1: 1}
TRAVEL = {0: 0, 1: 1, -1: 2}
CROSS = [{s: [i for i in range(19) if DIRS[i][d] == s] for s in SIGNS} for d in range(3)]
EDGES = [(a, b) for a in SIGNS for b in SIGNS]
ZPAIRS = [
    (DIRS.index((a, b, 1)), DIRS.index((a, b, -1)))
    for a, b in ((0, 0), (1, 0), (-1, 0), (0, 1), (0, -1))
]
DEEP = 3
HALF = 64
MOMS = 4


def kernel(sizes, order_in, dens_in, vel_in, order, pops, *scratch):
    (post, mom, base, oe, oz) = scratch[0:5]
    (sx, rx, sy, ry, rxy, sl, rl, sz, fz, fy) = scratch[5:15]
    (cx_, cy_, cz_, rcx, rcy, rcz) = scratch[15:21]
    (sa, ra, sc, rc) = scratch[21:25]
    X, Y, Z = order.shape
    E = Y + 16
    own_rows = slice(8, 8 + Y)
    block = 2 * DEEP
    width = X * block
    me = [lax.axis_index(a) for a in AXES]
    zsides = (1,) if sizes[2] == 2 else SIGNS

    def device(off):
        return {
            a: lax.rem(me[k] + (off[k] + sizes[k]), sizes[k]) if off[k] else me[k]
            for k, a in enumerate(AXES)
        }

    partners = [
        (a, b, c)
        for a in (0, 1, -1)
        for b in (0, 1, -1)
        for c in (0, 1, -1)
        if (a, b, c) != (0, 0, 0)
    ]
    barrier = pltpu.get_barrier_semaphore()
    for off in partners:
        pl.semaphore_signal(barrier, inc=1, device_id=device(off), device_id_type=MESH)

    lane = lax.broadcasted_iota(jnp.int32, (Y, Z), 1)
    row = lax.broadcasted_iota(jnp.int32, (Y, Z), 0)
    elane = lax.broadcasted_iota(jnp.int32, (E, Z), 1)
    erow = lax.broadcasted_iota(jnp.int32, (E, Z), 0)
    left = elane < HALF
    frame = jnp.where(left, elane, elane - HALF)
    column = lax.rem(frame, block)
    facing = lax.rem(elane, block) < DEEP
    zsign = jnp.where(left, 1.0, -1.0)
    low_col = lane < HALF
    face_z = column == DEEP
    face_x = (frame // block == DEEP) | (frame // block == DEEP + X)
    face_y = (erow == 8) | (erow == 8 + Y)
    below = jnp.where(erow == 8, 1.0, jnp.where(erow == 7, -1.0, 0.0))
    above = jnp.where(erow == 8 + Y, 1.0, jnp.where(erow == 7 + Y, -1.0, 0.0))

    def roll(v, s, axis):
        s = s % v.shape[axis]
        return v if s == 0 else pltpu.roll(v, s, axis)

    def zend(s):
        return 0 if s == 1 else Z - 1

    def yend(s):
        return 0 if s == 1 else Y - 1

    def xsrc(s):
        return X - 1 if s == 1 else 0

    def ysrc(s):
        return Y - 1 if s == 1 else 0

    def deep_rows(s):
        return pl.ds(8 - DEEP if s == 1 else 0, DEEP)

    def flat_rows(s):
        return pl.ds(0 if s == 1 else 4, X)

    def zat(px, s):
        return (px + DEEP) * block + (DEEP - 1 if s == 1 else HALF + DEEP)

    def zshift(v, s, packed, at):
        lanes = lane if v.shape[0] == Y else elane
        col = roll(packed, zend(s) - at, 1)
        return jnp.where(lanes == zend(s), col, roll(v, s, 1))

    def yshift(v, s, halo):
        return jnp.where(row == yend(s), jnp.broadcast_to(halo, v.shape), roll(v, s, 0))

    def pack(planes, s):
        acc = jnp.zeros((Y, Z), jnp.float32)
        for x in range(X):
            at = 1 + x
            acc = jnp.where(lane == at, roll(planes[x], at - (Z - 1 if s == 1 else 0), 1), acc)
        return acc

    def copies(messages, ssem, rsem):
        return [
            pltpu.make_async_remote_copy(
                src_ref=src,
                dst_ref=dst,
                send_sem=ssem.at[k],
                recv_sem=rsem.at[k],
                device_id=device(off),
                device_id_type=MESH,
            )
            for k, (src, dst, off) in enumerate(messages)
        ]

    def launch(flying):
        for copy in flying:
            copy.start()

    def finish(flying):
        for copy in flying:
            copy.wait_recv()
        for copy in flying:
            copy.wait_send()

    def bundle(par):
        messages = []
        for c in zsides:
            for b in (1, -1, 0):
                for a in (1, -1, 0):
                    dst = fz.at[par, INDEX[c], TRAVEL[a]]
                    rows = {1: pl.ds(Y - DEEP, DEEP), -1: pl.ds(0, DEEP), 0: pl.ds(0, Y)}[b]
                    land = {1: 8 - DEEP, -1: 8 + Y, 0: 8}[b]
                    land = pl.ds(land, DEEP if b else Y)
                    planes = pl.ds(0, 1 if a and b else 2)
                    messages.append((sz.at[planes, rows, :], dst.at[planes, land, :], (a, b, c)))
        for a, b in EDGES:
            bi, ai, rows = INDEX[b], INDEX[a], deep_rows(b)
            src = pl.ds(X - 1 if a == 1 else 0, 5)
            messages.append((sy.at[bi, src, rows, :], rxy.at[par, bi, ai, :, rows, :], (a, b, 0)))
            messages.append((sl.at[bi, ai], rl.at[par, bi, ai], (a, b, 0)))
        for s in SIGNS:
            si = INDEX[s]
            for span, rows in ((MOMS + 5, flat_rows(s)), (X + 4, deep_rows(s))):
                span = pl.ds(0, span)
                messages.append((sy.at[si, span, rows, :], ry.at[par, si, span, rows, :], (0, s, 0)))
        for s in SIGNS:
            messages.append((sx.at[INDEX[s]], rx.at[par, INDEX[s]], (s, 0, 0)))
        return copies(messages, sa, ra.at[par])

    def farewell():
        messages = []
        for s in SIGNS:
            messages.append((cy_.at[INDEX[s]], rcy.at[INDEX[s]], (0, s, 0)))
        for s in SIGNS:
            messages.append((cz_.at[INDEX[s]], rcz.at[INDEX[s]], (0, 0, s)))
        for s in SIGNS:
            messages.append((cx_.at[INDEX[s]], rcx.at[INDEX[s]], (s, 0, 0)))
        return copies(messages, sc, rc)

    def moments(ps):
        rho = ps[0]
        for i in range(1, 19):
            rho = rho + ps[i]
        moms = []
        for d in range(3):
            up = functools.reduce(lambda a, b: a + b, [ps[i] for i in CROSS[d][1]])
            down = functools.reduce(lambda a, b: a + b, [ps[i] for i in CROSS[d][-1]])
            moms.append(up - down)
        return rho, moms

    def chemical(o, beside):
        return quadratic * o + quartic * o * o * o - stiffness * (beside - 6.0 * o)

    def along(i, w):
        a = None
        for d in range(3):
            if DIRS[i][d]:
                t = w[d] if DIRS[i][d] == 1 else -w[d]
                a = t if a is None else a + t
        return a

    keep = 1.0 - 1.0 / relax_time
    mix = 1.0 / relax_time - 1.0

    def relaxed(ps, rho, u):
        flat = (mix * rho) * (1.0 - 1.5 * (u[0] * u[0] + u[1] * u[1] + u[2] * u[2]))
        out = [keep * ps[0] + WEIGHTS[0] * flat]
        for i in range(1, 19, 2):
            a = along(i, u)
            even = WEIGHTS[i] * flat + (4.5 * mix * WEIGHTS[i]) * rho * (a * a)
            odd = (3.0 * mix * WEIGHTS[i]) * rho * a
            out.append(keep * ps[i] + even + odd)
            out.append(keep * ps[i + 1] + even - odd)
        return out

    def place(acc, v, slot, x):
        at = slot * width + x * block
        mask = (lane >= at) & (lane < at + block)
        return jnp.where(mask, roll(v, at - (Z - DEEP), 1), acc)

    def ready():
        first = jnp.zeros((Y, Z), jnp.float32)
        second = jnp.zeros((Y, Z), jnp.float32)
        for x in range(X):
            rho = mom[0, x]
            u = [mom[1 + d, x] for d in range(3)]
            out = relaxed([pops[i, x] for i in range(19)], rho, u)
            heads, b = [rho] + u, base[x]
            for i in range(19):
                post[i, x] = out[i]
            for s in SIGNS:
                si = INDEX[s]
                if x == xsrc(s):
                    for g in range(MOMS):
                        sx[si, g] = heads[g]
                    for k, i in enumerate(CROSS[0][s]):
                        sx[si, MOMS + k] = out[i]
                slot = x - (X - DEEP) if s == 1 else x
                if 0 <= slot < DEEP:
                    sx[si, MOMS + 5 + slot] = b
                    sx[si, MOMS + 6 + DEEP, slot : slot + 1, :] = u[1][0:1, :]
                    sx[si, MOMS + 6 + DEEP, DEEP + slot : DEEP + slot + 1, :] = u[1][Y - 1 :, :]
                y, at = ysrc(s), (0 if s == 1 else 4) + x
                for g in range(MOMS):
                    sy[si, g, at : at + 1, :] = heads[g][y : y + 1, :]
                for k, i in enumerate(CROSS[1][s]):
                    sy[si, MOMS + k, at : at + 1, :] = out[i][y : y + 1, :]
                rows = slice(Y - DEEP, Y) if s == 1 else slice(0, DEEP)
                sy[si, 2 + x, deep_rows(s), :] = b[rows, :]
                if x == 0:
                    sy[si, 0, deep_rows(s), :] = u[0][rows, :]
                if x == X - 1:
                    sy[si, X + 3, deep_rows(s), :] = u[0][rows, :]
                for a in SIGNS:
                    if x == xsrc(a):
                        for k, v in enumerate(heads + [out[DIRS.index((a, s, 0))]]):
                            sl[si, INDEX[a], k : k + 1, :] = v[y : y + 1, :]
                    slot = x - (X - DEEP) if a == 1 else x - 1
                    if 0 <= slot < DEEP - 1:
                        sl[si, INDEX[a], 5 + slot : 6 + slot, :] = u[1][y : y + 1, :]
            for g, v in enumerate([b] + heads):
                first = place(first, v, g, x)
            for k, (up, down) in enumerate(ZPAIRS):
                second = place(second, jnp.where(low_col, out[down], out[up]), k, x)
        sz[0] = first
        sz[1] = second
        for s in SIGNS:
            si = INDEX[s]
            sx[si, MOMS + 5 + DEEP] = first
            rows = slice(Y - DEEP, Y) if s == 1 else slice(0, DEEP)
            for at in (1, X + 2):
                sy[si, at, deep_rows(s), :] = first[rows, :]

    def forced(rho, inv, u, force):
        v = [u[d] + force[d] * inv for d in range(3)]
        flat = rho * (1.0 - 1.5 * (v[0] * v[0] + v[1] * v[1] + v[2] * v[2]))
        return v, flat

    def one(i, rho, a, flat):
        return WEIGHTS[i] * (flat + rho * (a * (3.0 + 4.5 * a)))

    for ref in (sx, sy, sl, cy_, oe, oz):
        ref[...] = jnp.zeros_like(ref)

    for x in range(X):
        base[x] = order_in[x]
        r = dens_in[x]
        u = [vel_in[d, x] for d in range(3)]
        usq = 1.0 - 1.5 * (u[0] * u[0] + u[1] * u[1] + u[2] * u[2])
        ps = []
        for i in range(19):
            a = along(i, u)
            if a is None:
                ps.append(WEIGHTS[i] * r * usq)
            else:
                ps.append(WEIGHTS[i] * r * (usq + 3.0 * a + 4.5 * a * a))
            pops[i, x] = ps[i]
        rho, moms = moments(ps)
        inv = 1.0 / rho
        mom[0, x] = rho
        for d in range(3):
            mom[1 + d, x] = moms[d] * inv
    ready()
    pl.semaphore_wait(barrier, len(partners))
    launch(bundle(0))

    outer_first = sorted(range(X), key=lambda x: (min(x, X - 1 - x), x))

    def step(n, carry):
        par = lax.rem(n, 2)
        finish(bundle(par))
        low, high = ry.at[par, 0], ry.at[par, 1]

        def tall(a):
            if a == 0:
                near = [low[1], sz[0], high[1]]
            else:
                at = DEEP if a == 1 else 1
                mid = rx[par, INDEX[a], MOMS + 5 + DEEP]
                near = [rxy[par, 0, INDEX[a], at], mid, rxy[par, 1, INDEX[a], at]]
            near = jnp.concatenate(near, axis=0)
            far = [fz[par, INDEX[c], TRAVEL[a], 0] for c in zsides]
            halves = [jnp.where(facing, far[0], near), jnp.where(facing, near, far[-1])]
            return [roll(v, -a * width, 1) for v in halves]

        parts = [tall(a) for a in (0, 1, -1)]
        ends = [
            [roll(fz[par, INDEX[c], TRAVEL[a], 1], -a * width, 1) for a in (0, 1, -1)] for c in zsides
        ]

        def gather(three, slot, add):
            at = slot * width
            rel = lax.rem(elane + (Z - at), Z)
            v = jnp.where(rel < width, three[0], jnp.where(rel < HALF, three[2], three[1]))
            return roll(v, DEEP * block - at + add, 1)

        def packed(slot):
            halves = [gather([p[k] for p in parts], slot, HALF * k) for k in range(2)]
            return jnp.where(left, halves[0], halves[1])

        def packed_far(slot):
            halves = [gather(three, slot, HALF * k) for k, three in enumerate(ends)]
            if len(halves) == 1:
                halves.append(roll(halves[0], HALF, 1))
            return jnp.where(left, halves[0], halves[1])

        rho_z = packed(1)
        u_z = [packed(2 + d) for d in range(3)]
        old = oz[...]
        OZ = packed(0)
        for d, (shift, axis, mask) in enumerate(((block, 1, face_x), (1, 0, face_y), (1, 1, face_z))):
            t = 0.25 * (u_z[d] + roll(u_z[d], shift, axis)) * (old + roll(old, shift, axis))
            t = jnp.where(mask, t, 0.0)
            OZ = OZ + (t - roll(t, -shift, axis))
        oz[...] = OZ

        def around(px, s):
            if px < 0:
                return rxy[par, INDEX[s], 0, px + DEEP]
            if px >= X:
                return rxy[par, INDEX[s], 1, 2 + px - X]
            return ry[par, INDEX[s], 2 + px]

        def speed(px):
            if px < 0:
                tiles, mid = [rxy[par, k, 0, 4] for k in range(2)], rx[par, 0, 1]
            elif px >= X:
                tiles, mid = [rxy[par, k, 1, 0] for k in range(2)], rx[par, 1, 1]
            else:
                tiles, mid = [ry[par, k, 0 if px == 0 else X + 3] for k in range(2)], mom[1, px]
            return jnp.concatenate([tiles[0], mid, tiles[1]], axis=0)

        def outside(px, s):
            si = INDEX[s]
            if px < 0:
                at = 2 if px == -1 else 5 + px + DEEP
                return rl[par, si, 0, at : at + 1, :]
            if px >= X:
                at = 2 if px == X else 5 + px - X - 1
                return rl[par, si, 1, at : at + 1, :]
            at = (0 if s == 1 else 4) + px
            return ry[par, si, 2, at : at + 1, :]

        def inside(px, s):
            if 0 <= px < X:
                y = yend(s)
                return mom[2, px, y : y + 1, :]
            side, slot = (0, px + DEEP) if px < 0 else (1, px - X)
            at = slot if s == 1 else DEEP + slot
            return rx[par, side, MOMS + 6 + DEEP, at : at + 1, :]

        across = {}
        for lo, hi in ((-1, 0), (X - 1, X)):
            t = 0.25 * (speed(lo) + speed(hi)) * (oe[lo + DEEP] + oe[hi + DEEP])
            across[lo], across[hi] = -t, t
        OE = {}
        for px in range(-DEEP, X + DEEP):
            if px < 0:
                mid = rx[par, 0, MOMS + 5 + px + DEEP]
            elif px >= X:
                mid = rx[par, 1, MOMS + 5 + px - X]
            else:
                mid = base[px]
            v = jnp.concatenate([around(px, 1), mid, around(px, -1)], axis=0)
            if px in across:
                v = v + across[px]
            for s, sign, y in ((1, below, 8), (-1, above, 8 + Y)):
                pair = oe[px + DEEP, y - 1 : y, :] + oe[px + DEEP, y : y + 1, :]
                t = 0.25 * (outside(px, s) + inside(px, s)) * pair
                v = v + sign * jnp.broadcast_to(t, v.shape)
            at = (px + DEEP) * block
            v = jnp.where(elane == 0, roll(OZ, -(at + DEEP), 1), v)
            v = jnp.where(elane == Z - 1, roll(OZ, Z - 1 - (HALF + at + DEEP - 1), 1), v)
            OE[px] = v
        for px in range(-DEEP, X + DEEP):
            oe[px + DEEP] = OE[px]
        O = [OE[x][own_rows, :] for x in range(X)]

        C = {}
        for px in range(-2, X + 2):
            o = OE[px]
            beside = OE[px - 1] + OE[px + 1] + roll(o, 1, 0) + roll(o, -1, 0)
            beside = beside + zshift(o, 1, OZ, zat(px, 1)) + zshift(o, -1, OZ, zat(px, -1))
            C[px] = chemical(o, beside)
        beside = roll(OZ, 1, 0) + roll(OZ, -1, 0) + roll(OZ, 1, 1) + roll(OZ, -1, 1)
        beside = beside + roll(OZ, block, 1) + roll(OZ, -block, 1)
        CZ = chemical(OZ, beside)

        F = {}
        for px in range(-1, X + 1):
            c = C[px]
            y_dn, y_up = roll(c, 1, 0), roll(c, -1, 0)
            z_dn, z_up = zshift(c, 1, CZ, zat(px, 1)), zshift(c, -1, CZ, zat(px, -1))
            scale = -0.5 * OE[px]
            F[px] = [
                scale * (C[px + 1] - C[px - 1]),
                scale * (y_up - y_dn),
                scale * (z_up - z_dn),
            ]
            if 0 <= px < X:
                lap = C[px + 1] + C[px - 1] + y_up + y_dn + z_up + z_dn - 6.0 * c
                base[px] = O[px] + mobility * lap[own_rows, :]
                for s in SIGNS:
                    at = (0 if s == 1 else 4) + px
                    y = 7 if s == 1 else 8 + Y
                    for d in range(3):
                        fy[INDEX[s], d, at : at + 1, :] = F[px][d][y : y + 1, :]
        scale = -0.5 * OZ
        FZ = [
            scale * (roll(CZ, -block, 1) - roll(CZ, block, 1)),
            scale * (roll(CZ, -1, 0) - roll(CZ, 1, 0)),
            scale * (roll(CZ, -1, 1) - roll(CZ, 1, 1)),
        ]

        XH, YH, LH, ZH = {}, {}, {}, {}
        for s in SIGNS:
            si = INDEX[s]
            rho = rx[par, si, 0]
            u = [rx[par, si, 1 + d] for d in range(3)]
            px = -1 if s == 1 else X
            v, flat = forced(rho, 1.0 / rho, u, [f[own_rows, :] for f in F[px]])
            for k, i in enumerate(CROSS[0][s]):
                XH[i] = rx[par, si, MOMS + k] + one(i, rho, along(i, v), flat)
            rho = ry[par, si, 0]
            u = [ry[par, si, 1 + d] for d in range(3)]
            v, flat = forced(rho, 1.0 / rho, u, [fy[si, d] for d in range(3)])
            for k, i in enumerate(CROSS[1][s]):
                YH[i] = ry[par, si, MOMS + k] + one(i, rho, along(i, v), flat)
            for a in SIGNS:
                i = DIRS.index((a, s, 0))
                head = [rl[par, si, INDEX[a], k : k + 1, :] for k in range(5)]
                y, px = (7 if s == 1 else 8 + Y), (-1 if a == 1 else X)
                force = [f[y : y + 1, :] for f in F[px]]
                v, flat = forced(head[0], 1.0 / head[0], head[1:4], force)
                LH[i] = head[4] + one(i, head[0], along(i, v), flat)
        v, flat = forced(rho_z, 1.0 / rho_z, u_z, FZ)
        for k, (up, down) in enumerate(ZPAIRS):
            a = zsign * v[2]
            for d in range(2):
                if DIRS[up][d]:
                    a = a + v[d] if DIRS[up][d] == 1 else a - v[d]
            h = packed_far(k) + one(up, rho_z, a, flat)
            ZH[up] = ZH[down] = roll(h, DIRS[up][1], 0)[own_rows, :]

        for x in range(X):
            rho = mom[0, x]
            u = [mom[1 + d, x] for d in range(3)]
            v, flat = forced(rho, 1.0 / rho, u, [f[own_rows, :] for f in F[x]])
            post[0, x] = post[0, x] + WEIGHTS[0] * flat
            for i in range(1, 19, 2):
                a = along(i, v)
                even = WEIGHTS[i] * flat + (4.5 * WEIGHTS[i]) * rho * (a * a)
                odd = (3.0 * WEIGHTS[i]) * rho * a
                post[i, x] = post[i, x] + even + odd
                post[i + 1, x] = post[i + 1, x] + even - odd

        flows = {}
        for x in outer_first:
            ps = []
            for i, (cx, cy, cz) in enumerate(DIRS):
                xs = x - cx
                own = 0 <= xs < X
                p = post[i, xs] if own else XH[i]
                if cy:
                    at = (0 if cy == 1 else 4) + xs
                    p = yshift(p, cy, YH[i][at : at + 1, :] if own else LH[i])
                if cz:
                    p = zshift(p, cz, ZH[i], zat(xs, cz))
                pops[i, x] = p
                ps.append(p)
            rho, moms = moments(ps)
            inv = 1.0 / rho
            flows[x] = [m * inv for m in moms]
            mom[0, x] = rho
            for d in range(3):
                mom[1 + d, x] = flows[x][d]

        @pl.when(n == ITERS - 1)
        def _():
            for s in SIGNS:
                cx_[INDEX[s]] = mom[1, xsrc(s)]
                y = ysrc(s)
                for x in range(X):
                    cy_[INDEX[s], 1 + x : 2 + x, :] = mom[2, x, y : y + 1, :]
                cz_[INDEX[s]] = pack([mom[3, x] for x in range(X)], s)
            launch(farewell())

        tx = {0: 0.0, X: 0.0}
        for x in range(1, X):
            tx[x] = (flows[x][0] + flows[x - 1][0]) * (O[x] + O[x - 1])
        for x in range(X):
            f, o = flows[x], O[x]
            ty = jnp.where(row == 0, 0.0, (f[1] + roll(f[1], 1, 0)) * (o + roll(o, 1, 0)))
            tz = jnp.where(lane == 0, 0.0, (f[2] + roll(f[2], 1, 1)) * (o + roll(o, 1, 1)))
            change = tx[x + 1] - tx[x] + (roll(ty, -1, 0) - ty) + (roll(tz, -1, 1) - tz)
            base[x] = base[x] - 0.25 * change

        @pl.when(n < ITERS - 1)
        def _():
            ready()
            launch(bundle(1 - par))

        return carry

    lax.fori_loop(0, ITERS, step, 0)
    finish(farewell())

    OZ = oz[own_rows, :]
    for x in range(X):
        o, u = oe[x + DEEP, own_rows, :], [mom[1 + d, x] for d in range(3)]
        change = jnp.zeros((Y, Z), jnp.float32)
        if x == 0:
            change = change + (u[0] + rcx[0]) * (o + oe[DEEP - 1, own_rows, :])
        if x == X - 1:
            change = change - (u[0] + rcx[1]) * (o + oe[DEEP + X, own_rows, :])
        for s in SIGNS:
            at = 7 if s == 1 else 8 + Y
            other = rcy[INDEX[s], 1 + x : 2 + x, :]
            y = yend(s)
            t = (mom[2, x, y : y + 1, :] + other) * (
                oe[x + DEEP, at : at + 1, :] + oe[x + DEEP, 8 + y : 9 + y, :]
            )
            t = jnp.where(row == y, jnp.broadcast_to(t, (Y, Z)), 0.0)
            side = roll(OZ, zend(s) - zat(x, s), 1)
            beside = roll(rcz[INDEX[s]], zend(s) - (1 + x), 1)
            t = t + jnp.where(lane == zend(s), (u[2] + beside) * (o + side), 0.0)
            change = change + t if s == 1 else change - t
        order[x] = base[x] + 0.25 * change


def on_device(sizes, order_param, density, velocity):
    X, Y, Z = order_param.shape
    f32 = jnp.float32
    plane, rows, tall = (Y, Z), (8, Z), (Y + 16, Z)
    planes, tiles = MOMS + 5 + DEEP + 2, max(MOMS + 5, X + 4)
    vmem = [
        (19, X, Y, Z), (MOMS, X, Y, Z), (X, Y, Z), (X + 2 * DEEP,) + tall, tall,
        (2, planes) + plane, (2, 2, planes) + plane,
        (2, tiles) + rows, (2, 2, tiles) + rows, (2, 2, 2, 5) + rows,
        (2, 2) + rows, (2, 2, 2) + rows,
        (2,) + plane, (2, 2, 3, 2) + tall, (2, 3) + rows,
        (2,) + plane, (2,) + rows, (2,) + plane,
        (2,) + plane, (2,) + rows, (2,) + plane,
    ]
    count = (9 if sizes[2] == 2 else 18) + 14
    sems = [(count,), (2, count), (6,), (6,)]
    spec = pl.BlockSpec(memory_space=pltpu.VMEM)
    return pl.pallas_call(
        functools.partial(kernel, sizes),
        out_shape=(pltpu.VMEM((X, Y, Z), f32), pltpu.VMEM((19, X, Y, Z), f32)),
        in_specs=[spec] * 3,
        out_specs=(spec, spec),
        scratch_shapes=[pltpu.VMEM(s, f32) for s in vmem]
        + [pltpu.SemaphoreType.DMA(n) for n in sems],
        compiler_params=pltpu.CompilerParams(collective_id=0, has_side_effects=True),
    )(order_param, density, velocity)


def solution(mesh):
    sizes = tuple(mesh.shape[a] for a in AXES)
    return jax.shard_map(
        functools.partial(on_device, sizes),
        mesh=mesh,
        in_specs=(P("gx", "gy", "gz"), P("gx", "gy", "gz"), P(None, "gx", "gy", "gz")),
        out_specs=(P("gx", "gy", "gz"), P(None, "gx", "gy", "gz")),
        check_vma=False,
    )
```

```python
import functools
import math

import jax
import jax.numpy as jnp
from jax import lax
from jax.experimental import pallas as pl
from jax.experimental.pallas import tpu as pltpu
from jax.sharding import PartitionSpec as P

ITERS = 5
MESH = pl.DeviceIdType.MESH
AXES = ("gx", "gy", "gz")
DIRS = [
    (0, 0, 0),
    (1, 0, 0),
    (-1, 0, 0),
    (0, 1, 0),
    (0, -1, 0),
    (0, 0, 1),
    (0, 0, -1),
    (1, 1, 0),
    (-1, -1, 0),
    (1, -1, 0),
    (-1, 1, 0),
    (1, 0, 1),
    (-1, 0, -1),
    (1, 0, -1),
    (-1, 0, 1),
    (0, 1, 1),
    (0, -1, -1),
    (0, 1, -1),
    (0, -1, 1),
]
WEIGHTS = [1.0 / 3.0] + [1.0 / 18.0] * 6 + [1.0 / 36.0] * 12
quadratic = -0.1
quartic = 0.1
stiffness = 0.02
mobility = 0.5
relax_time = 0.8

SIGNS = (1, -1)
INDEX = {1: 0, -1: 1}
TRAVEL = {0: 0, 1: 1, -1: 2}
CROSS = [{s: [i for i in range(19) if DIRS[i][d] == s] for s in SIGNS} for d in range(3)]
EDGES = [(a, b) for a in SIGNS for b in SIGNS]
ZPAIRS = [
    (DIRS.index((a, b, 1)), DIRS.index((a, b, -1)))
    for a, b in ((0, 0), (1, 0), (-1, 0), (0, 1), (0, -1))
]
DEEP = 3
HALF = 64
MOMS = 4


def kernel(sizes, order_in, dens_in, vel_in, order, pops, *scratch):
    (post, mom, base, oe, oz, dens, vel, bulk) = scratch[0:8]
    (sx, rx, sy, ry, rxy, sz, fz, fy) = scratch[8:16]
    (cx_, cy_, cz_, rcx, rcy, rcz) = scratch[16:22]
    (si_, sa, ra, sc, rc) = scratch[22:27]
    X, Y, Z = order.shape
    E = Y + 16
    own_rows = slice(8, 8 + Y)
    block = 2 * DEEP
    width = X * block
    me = [lax.axis_index(a) for a in AXES]
    zsides = (1,) if sizes[2] == 2 else SIGNS

    def device(off):
        return {
            a: lax.rem(me[k] + (off[k] + sizes[k]), sizes[k]) if off[k] else me[k]
            for k, a in enumerate(AXES)
        }

    partners = [
        (a, b, c)
        for a in (1, -1, 0)
        for b in (1, -1, 0)
        for c in zsides + (0,)
        if (a, b, c) != (0, 0, 0)
    ]
    place_of = {off: device(off) for off in partners}
    if sizes[2] == 2:
        place_of[(0, 0, -1)] = place_of[(0, 0, 1)]
    barrier = pltpu.get_barrier_semaphore()
    for off in partners:
        pl.semaphore_signal(barrier, inc=1, device_id=place_of[off], device_id_type=MESH)
    loads = [
        pltpu.make_async_copy(src, dst, si_.at[k])
        for k, (src, dst) in enumerate(((order_in, base), (dens_in, dens), (vel_in, vel)))
    ]
    for load in loads:
        load.start()

    lane = lax.broadcasted_iota(jnp.int32, (Y, Z), 1)
    row = lax.broadcasted_iota(jnp.int32, (Y, Z), 0)
    elane = lax.broadcasted_iota(jnp.int32, (E, Z), 1)
    erow = lax.broadcasted_iota(jnp.int32, (E, Z), 0)
    left = elane < HALF
    frame = jnp.where(left, elane, elane - HALF)
    column = lax.rem(frame, block)
    facing = lax.rem(elane, block) < DEEP
    zsign = jnp.where(left, 1.0, -1.0)
    low_col = lane < HALF
    face_z = column == DEEP
    face_x = (frame // block == DEEP) | (frame // block == DEEP + X)
    face_y = (erow == 8) | (erow == 8 + Y)
    below = jnp.where(erow == 8, 1.0, jnp.where(erow == 7, -1.0, 0.0))
    above = jnp.where(erow == 8 + Y, 1.0, jnp.where(erow == 7 + Y, -1.0, 0.0))

    def roll(v, s, axis):
        s = s % v.shape[axis]
        return v if s == 0 else pltpu.roll(v, s, axis)

    def zend(s):
        return 0 if s == 1 else Z - 1

    def yend(s):
        return 0 if s == 1 else Y - 1

    def xsrc(s):
        return X - 1 if s == 1 else 0

    def ysrc(s):
        return Y - 1 if s == 1 else 0

    def deep_rows(s):
        return pl.ds(8 - DEEP if s == 1 else 0, DEEP)

    def flat_rows(s):
        return pl.ds(0 if s == 1 else 4, X)

    def line_row(k, s):
        return (8 - DEEP if s == 1 else 0) + k % DEEP

    def zat(px, s):
        return (px + DEEP) * block + (DEEP - 1 if s == 1 else HALF + DEEP)

    def zshift(v, s, packed, at):
        lanes = lane if v.shape[0] == Y else elane
        col = roll(packed, zend(s) - at, 1)
        return jnp.where(lanes == zend(s), col, roll(v, s, 1))

    def yshift(v, s, halo):
        return jnp.where(row == yend(s), jnp.broadcast_to(halo, v.shape), roll(v, s, 0))

    def pack(planes, s):
        acc = jnp.zeros((Y, Z), jnp.float32)
        for x in range(X):
            at = 1 + x
            acc = jnp.where(lane == at, roll(planes[x], at - (Z - 1 if s == 1 else 0), 1), acc)
        return acc

    def launch(messages, ssem, rsem):
        for src, dst, off in messages:
            pltpu.make_async_remote_copy(
                src_ref=src,
                dst_ref=dst,
                send_sem=ssem,
                recv_sem=rsem,
                device_id=place_of[off],
                device_id_type=MESH,
            ).start()

    def finish(messages, ssem, rsem):
        lines = sum(math.prod(src.shape[:-1]) for src, _, _ in messages)
        span = bulk.at[pl.ds(0, lines)]
        for sem in (rsem, ssem):
            pltpu.make_async_copy(span, span, sem).wait()

    def bundle(par):
        messages = []

        def beside(a, b, c):
            dst = fz.at[par, INDEX[c], TRAVEL[a]]
            rows = {1: pl.ds(Y - DEEP, DEEP), -1: pl.ds(0, DEEP), 0: pl.ds(0, Y)}[b]
            land = pl.ds({1: 8 - DEEP, -1: 8 + Y, 0: 8}[b], DEEP if b else Y)
            planes = pl.ds(0, 1 if a and b else 2)
            messages.append((sz.at[planes, rows, :], dst.at[planes, land, :], (a, b, c)))

        for c in zsides:
            for a, b in EDGES + [(0, 1), (0, -1)]:
                beside(a, b, c)
        for a, b in EDGES:
            bi, ai, rows = INDEX[b], INDEX[a], deep_rows(b)
            src = pl.ds(X + 2 if a == 1 else 0, 8)
            messages.append((sy.at[bi, src, rows, :], rxy.at[par, bi, ai, :, rows, :], (a, b, 0)))
        for s in SIGNS:
            si = INDEX[s]
            messages.append((sy.at[si, pl.ds(2, MOMS + 5)], ry.at[par, si], (0, s, 0)))
        for c in zsides:
            for a in SIGNS:
                beside(a, 0, c)
        for s in SIGNS:
            messages.append((sx.at[INDEX[s]], rx.at[par, INDEX[s]], (s, 0, 0)))
        for c in zsides:
            beside(0, 0, c)
        return messages, sa.at[0], ra.at[par]

    def farewell():
        messages = []
        for s in SIGNS:
            messages.append((cy_.at[INDEX[s]], rcy.at[INDEX[s]], (0, s, 0)))
        for s in SIGNS:
            messages.append((cz_.at[INDEX[s]], rcz.at[INDEX[s]], (0, 0, s)))
        for s in SIGNS:
            messages.append((cx_.at[INDEX[s]], rcx.at[INDEX[s]], (s, 0, 0)))
        return messages, sc.at[0], rc.at[0]

    def moments(ps):
        rho = ps[0]
        for i in range(1, 19):
            rho = rho + ps[i]
        moms = []
        for d in range(3):
            up = functools.reduce(lambda a, b: a + b, [ps[i] for i in CROSS[d][1]])
            down = functools.reduce(lambda a, b: a + b, [ps[i] for i in CROSS[d][-1]])
            moms.append(up - down)
        return rho, moms

    def chemical(o, beside):
        return quadratic * o + quartic * o * o * o - stiffness * (beside - 6.0 * o)

    def along(i, w):
        a = None
        for d in range(3):
            if DIRS[i][d]:
                t = w[d] if DIRS[i][d] == 1 else -w[d]
                a = t if a is None else a + t
        return a

    keep = 1.0 - 1.0 / relax_time
    mix = 1.0 / relax_time - 1.0

    def relax(x):
        ps = [pops[i, x] for i in range(19)]
        rho, u = mom[0, x], [mom[1 + d, x] for d in range(3)]
        flat = (mix * rho) * (1.0 - 1.5 * (u[0] * u[0] + u[1] * u[1] + u[2] * u[2]))
        out = [keep * ps[0] + WEIGHTS[0] * flat]
        for i in range(1, 19, 2):
            a = along(i, u)
            even = WEIGHTS[i] * flat + (4.5 * mix * WEIGHTS[i]) * rho * (a * a)
            odd = (3.0 * mix * WEIGHTS[i]) * rho * a
            out.append(keep * ps[i] + even + odd)
            out.append(keep * ps[i + 1] + even - odd)
        for i in range(19):
            post[i, x] = out[i]

    def place(acc, v, slot, x):
        at = slot * width + x * block
        mask = (lane >= at) & (lane < at + block)
        return jnp.where(mask, roll(v, at - (Z - DEEP), 1), acc)

    def ready():
        first = jnp.zeros((Y, Z), jnp.float32)
        second = jnp.zeros((Y, Z), jnp.float32)
        for x in range(X):
            heads, b = [mom[g, x] for g in range(MOMS)], base[x]
            u = heads[1:]
            out = [pops[i, x] for i in range(19)]
            for s in SIGNS:
                si = INDEX[s]
                if x == xsrc(s):
                    for g in range(MOMS):
                        sx[si, g] = heads[g]
                    for k, i in enumerate(CROSS[0][s]):
                        sx[si, MOMS + k] = out[i]
                slot = x - (X - DEEP) if s == 1 else x
                if 0 <= slot < DEEP:
                    sx[si, MOMS + 5 + slot] = b
                    sx[si, MOMS + 6 + DEEP, slot : slot + 1, :] = u[1][0:1, :]
                    sx[si, MOMS + 6 + DEEP, DEEP + slot : DEEP + slot + 1, :] = u[1][Y - 1 :, :]
                y, at = ysrc(s), (0 if s == 1 else 4) + x
                for g in range(MOMS):
                    sy[si, 2 + g, at : at + 1, :] = heads[g][y : y + 1, :]
                for k, i in enumerate(CROSS[1][s]):
                    sy[si, 2 + MOMS + k, at : at + 1, :] = out[i][y : y + 1, :]
                rows = slice(Y - DEEP, Y) if s == 1 else slice(0, DEEP)
                sy[si, 5 + x, deep_rows(s), :] = b[rows, :]
                if x == 0:
                    sy[si, 3, deep_rows(s), :] = u[0][rows, :]
                if x == X - 1:
                    sy[si, X + 6, deep_rows(s), :] = u[0][rows, :]
                for a in SIGNS:
                    lines = {}
                    if x == xsrc(a):
                        lines = dict(enumerate(heads + [out[DIRS.index((a, s, 0))]]))
                    slot = x - (X - DEEP) if a == 1 else x - 1
                    if 0 <= slot < DEEP - 1:
                        lines[5 + slot] = u[1]
                    for k, v in lines.items():
                        at, sub = (X + 7 if a == 1 else 0) + k // DEEP, line_row(k, s)
                        sy[si, at, sub : sub + 1, :] = v[y : y + 1, :]
            for g, v in enumerate([b] + heads):
                first = place(first, v, g, x)
            for k, (up, down) in enumerate(ZPAIRS):
                second = place(second, jnp.where(low_col, out[down], out[up]), k, x)
        sz[0] = first
        sz[1] = second
        for s in SIGNS:
            si = INDEX[s]
            sx[si, MOMS + 5 + DEEP] = first
            rows = slice(Y - DEEP, Y) if s == 1 else slice(0, DEEP)
            for at in (4, X + 5):
                sy[si, at, deep_rows(s), :] = first[rows, :]

    def forced(rho, inv, u, force):
        v = [u[d] + force[d] * inv for d in range(3)]
        flat = rho * (1.0 - 1.5 * (v[0] * v[0] + v[1] * v[1] + v[2] * v[2]))
        return v, flat

    def collide(rho, u, force):
        v, flat = forced(rho, 1.0 / rho, u, force)
        thin = mix * rho
        flat = flat + thin * (1.0 - 1.5 * (u[0] * u[0] + u[1] * u[1] + u[2] * u[2]))

        def hit(i, p, along_of):
            a, b = along_of(i, u), along_of(i, v)
            both = thin * (a * (3.0 + 4.5 * a)) + rho * (b * (3.0 + 4.5 * b))
            return keep * p + WEIGHTS[i] * (flat + both)

        return hit

    for ref in (sx, sy, cy_, oe, oz):
        ref[...] = jnp.zeros_like(ref)
    for load in loads:
        load.wait()

    for x in range(X):
        r = dens[x]
        u = [vel[d, x] for d in range(3)]
        usq = 1.0 - 1.5 * (u[0] * u[0] + u[1] * u[1] + u[2] * u[2])
        ps = []
        for i in range(19):
            a = along(i, u)
            if a is None:
                ps.append(WEIGHTS[i] * r * usq)
            else:
                ps.append(WEIGHTS[i] * r * (usq + 3.0 * a + 4.5 * a * a))
            pops[i, x] = ps[i]
        rho, moms = moments(ps)
        inv = 1.0 / rho
        mom[0, x] = rho
        for d in range(3):
            mom[1 + d, x] = moms[d] * inv
    ready()
    pl.semaphore_wait(barrier, len(partners))
    launch(*bundle(0))
    for x in range(X):
        relax(x)

    outer_first = sorted(range(X), key=lambda x: (min(x, X - 1 - x), x))

    def step(n, carry):
        par = lax.rem(n, 2)
        finish(*bundle(par))
        low, high = ry.at[par, 0], ry.at[par, 1]

        def tall(a):
            if a == 0:
                near = [low[2], sz[0], high[2]]
            else:
                at = DEEP if a == 1 else DEEP + 1
                mid = rx[par, INDEX[a], MOMS + 5 + DEEP]
                near = [rxy[par, 0, INDEX[a], at], mid, rxy[par, 1, INDEX[a], at]]
            near = jnp.concatenate(near, axis=0)
            far = [fz[par, INDEX[c], TRAVEL[a], 0] for c in zsides]
            halves = [jnp.where(facing, far[0], near), jnp.where(facing, near, far[-1])]
            return [roll(v, -a * width, 1) for v in halves]

        parts = [tall(a) for a in (0, 1, -1)]
        ends = [
            [roll(fz[par, INDEX[c], TRAVEL[a], 1], -a * width, 1) for a in (0, 1, -1)] for c in zsides
        ]

        def gather(three, slot, add):
            at = slot * width
            rel = lax.rem(elane + (Z - at), Z)
            v = jnp.where(rel < width, three[0], jnp.where(rel < HALF, three[2], three[1]))
            return roll(v, DEEP * block - at + add, 1)

        def packed(slot):
            halves = [gather([p[k] for p in parts], slot, HALF * k) for k in range(2)]
            return jnp.where(left, halves[0], halves[1])

        def packed_far(slot):
            halves = [gather(three, slot, HALF * k) for k, three in enumerate(ends)]
            if len(halves) == 1:
                halves.append(roll(halves[0], HALF, 1))
            return jnp.where(left, halves[0], halves[1])

        rho_z = packed(1)
        u_z = [packed(2 + d) for d in range(3)]
        old = oz[...]
        OZ = packed(0)
        for d, (shift, axis, mask) in enumerate(((block, 1, face_x), (1, 0, face_y), (1, 1, face_z))):
            t = 0.25 * (u_z[d] + roll(u_z[d], shift, axis)) * (old + roll(old, shift, axis))
            t = jnp.where(mask, t, 0.0)
            OZ = OZ + (t - roll(t, -shift, axis))
        oz[...] = OZ

        def around(px, s):
            if px < 0:
                return rxy[par, INDEX[s], 0, px + DEEP]
            if px >= X:
                return rxy[par, INDEX[s], 1, DEEP + 2 + px - X]
            return ry[par, INDEX[s], 3 + px]

        def speed(px):
            if px < 0:
                tiles, mid = [rxy[par, k, 0, 4] for k in range(2)], rx[par, 0, 1]
            elif px >= X:
                tiles, mid = [rxy[par, k, 1, DEEP] for k in range(2)], rx[par, 1, 1]
            else:
                tiles, mid = [ry[par, k, 1 if px == 0 else X + 4] for k in range(2)], mom[1, px]
            return jnp.concatenate([tiles[0], mid, tiles[1]], axis=0)

        def line(k, a, s):
            at, sub = (DEEP + 2 if a == 1 else 0) + k // DEEP, line_row(k, s)
            return rxy[par, INDEX[s], INDEX[a], at, sub : sub + 1, :]

        def outside(px, s):
            if px < 0:
                return line(2 if px == -1 else 5 + px + DEEP, 1, s)
            if px >= X:
                return line(2 if px == X else 5 + px - X - 1, -1, s)
            at = (0 if s == 1 else 4) + px
            return ry[par, INDEX[s], 2, at : at + 1, :]

        def inside(px, s):
            if 0 <= px < X:
                y = yend(s)
                return mom[2, px, y : y + 1, :]
            side, slot = (0, px + DEEP) if px < 0 else (1, px - X)
            at = slot if s == 1 else DEEP + slot
            return rx[par, side, MOMS + 6 + DEEP, at : at + 1, :]

        across = {}
        for lo, hi in ((-1, 0), (X - 1, X)):
            t = 0.25 * (speed(lo) + speed(hi)) * (oe[lo + DEEP] + oe[hi + DEEP])
            across[lo], across[hi] = -t, t
        OE = {}
        for px in range(-DEEP, X + DEEP):
            if px < 0:
                mid = rx[par, 0, MOMS + 5 + px + DEEP]
            elif px >= X:
                mid = rx[par, 1, MOMS + 5 + px - X]
            else:
                mid = base[px]
            v = jnp.concatenate([around(px, 1), mid, around(px, -1)], axis=0)
            if px in across:
                v = v + across[px]
            for s, sign, y in ((1, below, 8), (-1, above, 8 + Y)):
                pair = oe[px + DEEP, y - 1 : y, :] + oe[px + DEEP, y : y + 1, :]
                t = 0.25 * (outside(px, s) + inside(px, s)) * pair
                v = v + sign * jnp.broadcast_to(t, v.shape)
            at = (px + DEEP) * block
            v = jnp.where(elane == 0, roll(OZ, -(at + DEEP), 1), v)
            v = jnp.where(elane == Z - 1, roll(OZ, Z - 1 - (HALF + at + DEEP - 1), 1), v)
            OE[px] = v
        for px in range(-DEEP, X + DEEP):
            oe[px + DEEP] = OE[px]
        O = [OE[x][own_rows, :] for x in range(X)]

        C = {}
        for px in range(-2, X + 2):
            o = OE[px]
            beside = OE[px - 1] + OE[px + 1] + roll(o, 1, 0) + roll(o, -1, 0)
            beside = beside + zshift(o, 1, OZ, zat(px, 1)) + zshift(o, -1, OZ, zat(px, -1))
            C[px] = chemical(o, beside)
        beside = roll(OZ, 1, 0) + roll(OZ, -1, 0) + roll(OZ, 1, 1) + roll(OZ, -1, 1)
        beside = beside + roll(OZ, block, 1) + roll(OZ, -block, 1)
        CZ = chemical(OZ, beside)

        F = {}
        for px in range(-1, X + 1):
            c = C[px]
            y_dn, y_up = roll(c, 1, 0), roll(c, -1, 0)
            z_dn, z_up = zshift(c, 1, CZ, zat(px, 1)), zshift(c, -1, CZ, zat(px, -1))
            scale = -0.5 * OE[px]
            F[px] = [
                scale * (C[px + 1] - C[px - 1]),
                scale * (y_up - y_dn),
                scale * (z_up - z_dn),
            ]
            if 0 <= px < X:
                lap = C[px + 1] + C[px - 1] + y_up + y_dn + z_up + z_dn - 6.0 * c
                base[px] = O[px] + mobility * lap[own_rows, :]
                for s in SIGNS:
                    at = (0 if s == 1 else 4) + px
                    y = 7 if s == 1 else 8 + Y
                    for d in range(3):
                        fy[INDEX[s], d, at : at + 1, :] = F[px][d][y : y + 1, :]
        scale = -0.5 * OZ
        FZ = [
            scale * (roll(CZ, -block, 1) - roll(CZ, block, 1)),
            scale * (roll(CZ, -1, 0) - roll(CZ, 1, 0)),
            scale * (roll(CZ, -1, 1) - roll(CZ, 1, 1)),
        ]

        XH, YH, LH, ZH = {}, {}, {}, {}
        own = lambda i, w: along(i, w)
        for s in SIGNS:
            si = INDEX[s]
            rho = rx[par, si, 0]
            u = [rx[par, si, 1 + d] for d in range(3)]
            px = -1 if s == 1 else X
            hit = collide(rho, u, [f[own_rows, :] for f in F[px]])
            for k, i in enumerate(CROSS[0][s]):
                XH[i] = hit(i, rx[par, si, MOMS + k], own)
            rho = ry[par, si, 0]
            u = [ry[par, si, 1 + d] for d in range(3)]
            hit = collide(rho, u, [fy[si, d] for d in range(3)])
            for k, i in enumerate(CROSS[1][s]):
                YH[i] = hit(i, ry[par, si, MOMS + k], own)
            for a in SIGNS:
                i = DIRS.index((a, s, 0))
                head = [line(k, a, s) for k in range(5)]
                y, px = (7 if s == 1 else 8 + Y), (-1 if a == 1 else X)
                hit = collide(head[0], head[1:4], [f[y : y + 1, :] for f in F[px]])
                LH[i] = hit(i, head[4], own)

        def sided(i, w):
            a = zsign * w[2]
            for d in range(2):
                if DIRS[i][d]:
                    a = a + w[d] if DIRS[i][d] == 1 else a - w[d]
            return a

        hit = collide(rho_z, u_z, FZ)
        for k, (up, down) in enumerate(ZPAIRS):
            h = hit(up, packed_far(k), sided)
            ZH[up] = ZH[down] = roll(h, DIRS[up][1], 0)[own_rows, :]

        for x in range(X):
            rho = mom[0, x]
            u = [mom[1 + d, x] for d in range(3)]
            v, flat = forced(rho, 1.0 / rho, u, [f[own_rows, :] for f in F[x]])
            post[0, x] = post[0, x] + WEIGHTS[0] * flat
            for i in range(1, 19, 2):
                a = along(i, v)
                even = WEIGHTS[i] * flat + (4.5 * WEIGHTS[i]) * rho * (a * a)
                odd = (3.0 * WEIGHTS[i]) * rho * a
                post[i, x] = post[i, x] + even + odd
                post[i + 1, x] = post[i + 1, x] + even - odd

        flows = {}
        for x in outer_first:
            ps = []
            for i, (cx, cy, cz) in enumerate(DIRS):
                xs = x - cx
                own = 0 <= xs < X
                p = post[i, xs] if own else XH[i]
                if cy:
                    at = (0 if cy == 1 else 4) + xs
                    p = yshift(p, cy, YH[i][at : at + 1, :] if own else LH[i])
                if cz:
                    p = zshift(p, cz, ZH[i], zat(xs, cz))
                pops[i, x] = p
                ps.append(p)
            rho, moms = moments(ps)
            inv = 1.0 / rho
            flows[x] = [m * inv for m in moms]
            mom[0, x] = rho
            for d in range(3):
                mom[1 + d, x] = flows[x][d]

        @pl.when(n == ITERS - 1)
        def _():
            for s in SIGNS:
                cx_[INDEX[s]] = mom[1, xsrc(s)]
                y = ysrc(s)
                for x in range(X):
                    cy_[INDEX[s], 1 + x : 2 + x, :] = mom[2, x, y : y + 1, :]
                cz_[INDEX[s]] = pack([mom[3, x] for x in range(X)], s)
            launch(*farewell())

        tx = {0: 0.0, X: 0.0}
        for x in range(1, X):
            tx[x] = (flows[x][0] + flows[x - 1][0]) * (O[x] + O[x - 1])
        for x in range(X):
            f, o = flows[x], O[x]
            ty = jnp.where(row == 0, 0.0, (f[1] + roll(f[1], 1, 0)) * (o + roll(o, 1, 0)))
            tz = jnp.where(lane == 0, 0.0, (f[2] + roll(f[2], 1, 1)) * (o + roll(o, 1, 1)))
            change = tx[x + 1] - tx[x] + (roll(ty, -1, 0) - ty) + (roll(tz, -1, 1) - tz)
            base[x] = base[x] - 0.25 * change

        @pl.when(n < ITERS - 1)
        def _():
            ready()
            launch(*bundle(1 - par))
            for x in range(X):
                relax(x)

        return carry

    lax.fori_loop(0, ITERS, step, 0)
    finish(*farewell())

    OZ = oz[own_rows, :]
    for x in range(X):
        o, u = oe[x + DEEP, own_rows, :], [mom[1 + d, x] for d in range(3)]
        change = jnp.zeros((Y, Z), jnp.float32)
        if x == 0:
            change = change + (u[0] + rcx[0]) * (o + oe[DEEP - 1, own_rows, :])
        if x == X - 1:
            change = change - (u[0] + rcx[1]) * (o + oe[DEEP + X, own_rows, :])
        for s in SIGNS:
            at = 7 if s == 1 else 8 + Y
            other = rcy[INDEX[s], 1 + x : 2 + x, :]
            y = yend(s)
            t = (mom[2, x, y : y + 1, :] + other) * (
                oe[x + DEEP, at : at + 1, :] + oe[x + DEEP, 8 + y : 9 + y, :]
            )
            t = jnp.where(row == y, jnp.broadcast_to(t, (Y, Z)), 0.0)
            side = roll(OZ, zend(s) - zat(x, s), 1)
            beside = roll(rcz[INDEX[s]], zend(s) - (1 + x), 1)
            t = t + jnp.where(lane == zend(s), (u[2] + beside) * (o + side), 0.0)
            change = change + t if s == 1 else change - t
        order[x] = base[x] + 0.25 * change


def on_device(sizes, order_param, density, velocity):
    X, Y, Z = order_param.shape
    f32 = jnp.float32
    plane, rows, tall = (Y, Z), (8, Z), (Y + 16, Z)
    planes = MOMS + 5 + DEEP + 2
    lines = 2 * planes * Y + 2 * 8 * (MOMS + 5) + 4 * 8 * DEEP
    lines += (1 if sizes[2] == 2 else 2) * (6 * Y + 8 * DEEP)
    vmem = [
        (19, X, Y, Z), (MOMS, X, Y, Z), (X, Y, Z), (X + 2 * DEEP,) + tall, tall,
        (X, Y, Z), (3, X, Y, Z), (lines, Z),
        (2, planes) + plane, (2, 2, planes) + plane,
        (2, X + 10) + rows, (2, 2, MOMS + 5) + rows, (2, 2, 2, 8) + rows,
        (2,) + plane, (2, 2, 3, 2) + tall, (2, 3) + rows,
        (2,) + plane, (2,) + rows, (2,) + plane,
        (2,) + plane, (2,) + rows, (2,) + plane,
    ]
    sems = [(3,), (1,), (2,), (1,), (1,)]
    spec = pl.BlockSpec(memory_space=pltpu.VMEM)
    return pl.pallas_call(
        functools.partial(kernel, sizes),
        out_shape=(pltpu.VMEM((X, Y, Z), f32), pltpu.VMEM((19, X, Y, Z), f32)),
        in_specs=[pl.BlockSpec(memory_space=pl.ANY)] * 3,
        out_specs=(spec, spec),
        scratch_shapes=[pltpu.VMEM(s, f32) for s in vmem]
        + [pltpu.SemaphoreType.DMA(n) for n in sems],
        compiler_params=pltpu.CompilerParams(collective_id=0, has_side_effects=True),
    )(order_param, density, velocity)


def solution(mesh):
    sizes = tuple(mesh.shape[a] for a in AXES)
    return jax.shard_map(
        functools.partial(on_device, sizes),
        mesh=mesh,
        in_specs=(P("gx", "gy", "gz"), P("gx", "gy", "gz"), P(None, "gx", "gy", "gz")),
        out_specs=(P("gx", "gy", "gz"), P(None, "gx", "gy", "gz")),
        check_vma=False,
    )
```

```python
import functools
import math

import jax
import jax.numpy as jnp
from jax import lax
from jax.experimental import pallas as pl
from jax.experimental.pallas import tpu as pltpu
from jax.sharding import PartitionSpec as P

ITERS = 5
MESH = pl.DeviceIdType.MESH
AXES = ("gx", "gy", "gz")
DIRS = [
    (0, 0, 0),
    (1, 0, 0),
    (-1, 0, 0),
    (0, 1, 0),
    (0, -1, 0),
    (0, 0, 1),
    (0, 0, -1),
    (1, 1, 0),
    (-1, -1, 0),
    (1, -1, 0),
    (-1, 1, 0),
    (1, 0, 1),
    (-1, 0, -1),
    (1, 0, -1),
    (-1, 0, 1),
    (0, 1, 1),
    (0, -1, -1),
    (0, 1, -1),
    (0, -1, 1),
]
WEIGHTS = [1.0 / 3.0] + [1.0 / 18.0] * 6 + [1.0 / 36.0] * 12
quadratic = -0.1
quartic = 0.1
stiffness = 0.02
mobility = 0.5
relax_time = 0.8

SIGNS = (1, -1)
INDEX = {1: 0, -1: 1}
TRAVEL = {0: 0, 1: 1, -1: 2}
CROSS = [{s: [i for i in range(19) if DIRS[i][d] == s] for s in SIGNS} for d in range(3)]
EDGES = [(a, b) for a in SIGNS for b in SIGNS]
ZPAIRS = [
    (DIRS.index((a, b, 1)), DIRS.index((a, b, -1)))
    for a, b in ((0, 0), (1, 0), (-1, 0), (0, 1), (0, -1))
]
DEEP = 3
HALF = 64
MOMS = 4


def kernel(sizes, order_in, dens_in, vel_in, order, pops, *scratch):
    (post, mom, base, oe, oz, dens, vel, bulk) = scratch[0:8]
    (sx, rx, sy, ry, rxy, sz, fz, fy) = scratch[8:16]
    (cx_, cy_, cz_, rcx, rcy, rcz) = scratch[16:22]
    (si_, sa, ra, sc, rc) = scratch[22:27]
    X, Y, Z = order.shape
    E = Y + 16
    own_rows = slice(8, 8 + Y)
    block = 2 * DEEP
    width = X * block
    me = [lax.axis_index(a) for a in AXES]
    zsides = (1,) if sizes[2] == 2 else SIGNS

    def device(off):
        return {
            a: lax.rem(me[k] + (off[k] + sizes[k]), sizes[k]) if off[k] else me[k]
            for k, a in enumerate(AXES)
        }

    partners = [
        (a, b, c)
        for a in (1, -1, 0)
        for b in (1, -1, 0)
        for c in zsides + (0,)
        if (a, b, c) != (0, 0, 0)
    ]
    place_of = {off: device(off) for off in partners}
    if sizes[2] == 2:
        place_of[(0, 0, -1)] = place_of[(0, 0, 1)]
    barrier = pltpu.get_barrier_semaphore()
    for off in partners:
        pl.semaphore_signal(barrier, inc=1, device_id=place_of[off], device_id_type=MESH)
    loads = [
        pltpu.make_async_copy(src, dst, si_.at[k])
        for k, (src, dst) in enumerate(((order_in, base), (dens_in, dens), (vel_in, vel)))
    ]
    for load in loads:
        load.start()

    lane = lax.broadcasted_iota(jnp.int32, (Y, Z), 1)
    row = lax.broadcasted_iota(jnp.int32, (Y, Z), 0)
    elane = lax.broadcasted_iota(jnp.int32, (E, Z), 1)
    erow = lax.broadcasted_iota(jnp.int32, (E, Z), 0)
    left = elane < HALF
    frame = jnp.where(left, elane, elane - HALF)
    column = lax.rem(frame, block)
    facing = lax.rem(elane, block) < DEEP
    zsign = jnp.where(left, 1.0, -1.0)
    low_col = lane < HALF
    face_z = column == DEEP
    face_x = (frame // block == DEEP) | (frame // block == DEEP + X)
    face_y = (erow == 8) | (erow == 8 + Y)
    hrow = lax.broadcasted_iota(jnp.int32, (16, Z), 0)
    seam = jnp.where(hrow == 8, 1.0, jnp.where(hrow == 7, -1.0, 0.0))
    last = column == DEEP - 1

    def roll(v, s, axis):
        s = s % v.shape[axis]
        return v if s == 0 else pltpu.roll(v, s, axis)

    def zend(s):
        return 0 if s == 1 else Z - 1

    def yend(s):
        return 0 if s == 1 else Y - 1

    def xsrc(s):
        return X - 1 if s == 1 else 0

    def ysrc(s):
        return Y - 1 if s == 1 else 0

    def deep_rows(s):
        return pl.ds(8 - DEEP if s == 1 else 0, DEEP)

    def flat_rows(s):
        return pl.ds(0 if s == 1 else 4, X)

    def line_row(k, s):
        return (8 - DEEP if s == 1 else 0) + k % DEEP

    def halo_pair(v):
        return jnp.where(last, v, roll(v, -(HALF + 2), 1))

    def pick(pair, px):
        return roll(pair, -((px + DEEP) * block + DEEP - 1), 1)

    def zshift(v, s, col):
        lanes = lane if v.shape[0] == Y else elane
        return jnp.where(lanes == zend(s), col, roll(v, s, 1))

    def yshift(v, s, halo):
        return jnp.where(row == yend(s), jnp.broadcast_to(halo, v.shape), roll(v, s, 0))

    def pack(planes, s):
        acc = jnp.zeros((Y, Z), jnp.float32)
        for x in range(X):
            at = 1 + x
            acc = jnp.where(lane == at, roll(planes[x], at - (Z - 1 if s == 1 else 0), 1), acc)
        return acc

    def launch(messages, ssem, rsem):
        for src, dst, off in messages:
            pltpu.make_async_remote_copy(
                src_ref=src,
                dst_ref=dst,
                send_sem=ssem,
                recv_sem=rsem,
                device_id=place_of[off],
                device_id_type=MESH,
            ).start()

    def finish(messages, ssem, rsem):
        lines = sum(math.prod(src.shape[:-1]) for src, _, _ in messages)
        span = bulk.at[pl.ds(0, lines)]
        for sem in (rsem, ssem):
            pltpu.make_async_copy(span, span, sem).wait()

    def bundle(par):
        messages = []

        def beside(a, b, c):
            dst = fz.at[par, INDEX[c], TRAVEL[a]]
            rows = {1: pl.ds(Y - DEEP, DEEP), -1: pl.ds(0, DEEP), 0: pl.ds(0, Y)}[b]
            land = pl.ds({1: 8 - DEEP, -1: 8 + Y, 0: 8}[b], DEEP if b else Y)
            planes = pl.ds(0, 1 if a and b else 2)
            messages.append((sz.at[planes, rows, :], dst.at[planes, land, :], (a, b, c)))

        for c in zsides:
            for a, b in EDGES + [(0, 1), (0, -1)]:
                beside(a, b, c)
        for a, b in EDGES:
            bi, ai, rows = INDEX[b], INDEX[a], deep_rows(b)
            src = pl.ds(X + 2 if a == 1 else 0, 8)
            messages.append((sy.at[bi, src, rows, :], rxy.at[par, bi, ai, :, rows, :], (a, b, 0)))
        for s in SIGNS:
            si = INDEX[s]
            messages.append((sy.at[si, pl.ds(2, MOMS + 5)], ry.at[par, si], (0, s, 0)))
        for c in zsides:
            for a in SIGNS:
                beside(a, 0, c)
        for s in SIGNS:
            messages.append((sx.at[INDEX[s]], rx.at[par, INDEX[s]], (s, 0, 0)))
        for c in zsides:
            beside(0, 0, c)
        return messages, sa.at[0], ra.at[par]

    def farewell():
        messages = []
        for s in SIGNS:
            messages.append((cy_.at[INDEX[s]], rcy.at[INDEX[s]], (0, s, 0)))
        for s in SIGNS:
            messages.append((cz_.at[INDEX[s]], rcz.at[INDEX[s]], (0, 0, s)))
        for s in SIGNS:
            messages.append((cx_.at[INDEX[s]], rcx.at[INDEX[s]], (s, 0, 0)))
        return messages, sc.at[0], rc.at[0]

    def moments(ps):
        rho = ps[0]
        for i in range(1, 19):
            rho = rho + ps[i]
        moms = []
        for d in range(3):
            up = functools.reduce(lambda a, b: a + b, [ps[i] for i in CROSS[d][1]])
            down = functools.reduce(lambda a, b: a + b, [ps[i] for i in CROSS[d][-1]])
            moms.append(up - down)
        return rho, moms

    def chemical(o, beside):
        return quadratic * o + quartic * o * o * o - stiffness * (beside - 6.0 * o)

    def along(i, w):
        a = None
        for d in range(3):
            if DIRS[i][d]:
                t = w[d] if DIRS[i][d] == 1 else -w[d]
                a = t if a is None else a + t
        return a

    keep = 1.0 - 1.0 / relax_time
    mix = 1.0 / relax_time - 1.0

    def relax(x):
        ps = [pops[i, x] for i in range(19)]
        rho, u = mom[0, x], [mom[1 + d, x] for d in range(3)]
        flat = (mix * rho) * (1.0 - 1.5 * (u[0] * u[0] + u[1] * u[1] + u[2] * u[2]))
        out = [keep * ps[0] + WEIGHTS[0] * flat]
        for i in range(1, 19, 2):
            a = along(i, u)
            even = WEIGHTS[i] * flat + (4.5 * mix * WEIGHTS[i]) * rho * (a * a)
            odd = (3.0 * mix * WEIGHTS[i]) * rho * a
            out.append(keep * ps[i] + even + odd)
            out.append(keep * ps[i + 1] + even - odd)
        for i in range(19):
            post[i, x] = out[i]

    def place(acc, v, slot, x):
        at = slot * width + x * block
        mask = (lane >= at) & (lane < at + block)
        return jnp.where(mask, roll(v, at - (Z - DEEP), 1), acc)

    def ready():
        first = jnp.zeros((Y, Z), jnp.float32)
        second = jnp.zeros((Y, Z), jnp.float32)
        for x in range(X):
            heads, b = [mom[g, x] for g in range(MOMS)], base[x]
            u = heads[1:]
            out = [pops[i, x] for i in range(19)]
            for s in SIGNS:
                si = INDEX[s]
                y, at = ysrc(s), (0 if s == 1 else 4) + x
                for g in range(MOMS):
                    sy[si, 2 + g, at : at + 1, :] = heads[g][y : y + 1, :]
                for k, i in enumerate(CROSS[1][s]):
                    sy[si, 2 + MOMS + k, at : at + 1, :] = out[i][y : y + 1, :]
                rows = slice(Y - DEEP, Y) if s == 1 else slice(0, DEEP)
                sy[si, 5 + x, deep_rows(s), :] = b[rows, :]
                if x == 0:
                    sy[si, 3, deep_rows(s), :] = u[0][rows, :]
                if x == X - 1:
                    sy[si, X + 6, deep_rows(s), :] = u[0][rows, :]
                for a in SIGNS:
                    lines = {}
                    if x == xsrc(a):
                        lines = dict(enumerate(heads + [out[DIRS.index((a, s, 0))]]))
                    slot = x - (X - DEEP) if a == 1 else x - 1
                    if 0 <= slot < DEEP - 1:
                        lines[5 + slot] = u[1]
                    for k, v in lines.items():
                        at, sub = (X + 7 if a == 1 else 0) + k // DEEP, line_row(k, s)
                        sy[si, at, sub : sub + 1, :] = v[y : y + 1, :]
            for g, v in enumerate([b] + heads):
                first = place(first, v, g, x)
            for k, (up, down) in enumerate(ZPAIRS):
                second = place(second, jnp.where(low_col, out[down], out[up]), k, x)
        sz[0] = first
        sz[1] = second
        for s in SIGNS:
            si = INDEX[s]
            rows = slice(Y - DEEP, Y) if s == 1 else slice(0, DEEP)
            for at in (4, X + 5):
                sy[si, at, deep_rows(s), :] = first[rows, :]

    def ready_planes():
        for s in SIGNS:
            si, edge = INDEX[s], xsrc(s)
            for g in range(MOMS):
                sx[si, g] = mom[g, edge]
            for k, i in enumerate(CROSS[0][s]):
                sx[si, MOMS + k] = pops[i, edge]
            for slot in range(DEEP):
                x = slot + (X - DEEP if s == 1 else 0)
                sx[si, MOMS + 5 + slot] = base[x]
                sx[si, MOMS + 6 + DEEP, slot : slot + 1, :] = mom[2, x, 0:1, :]
                sx[si, MOMS + 6 + DEEP, DEEP + slot : DEEP + slot + 1, :] = mom[2, x, Y - 1 :, :]
            sx[si, MOMS + 5 + DEEP] = sz[0]

    def send(par):
        messages, ssem, rsem = bundle(par)
        first = [m for m in messages if m[2][1]]
        launch(first, ssem, rsem)
        ready_planes()
        launch(messages[len(first) :], ssem, rsem)
        for x in range(X):
            relax(x)

    def forced(rho, inv, u, force):
        v = [u[d] + force[d] * inv for d in range(3)]
        flat = rho * (1.0 - 1.5 * (v[0] * v[0] + v[1] * v[1] + v[2] * v[2]))
        return v, flat

    def collide(rho, u, force):
        v, flat = forced(rho, 1.0 / rho, u, force)
        thin = mix * rho
        flat = flat + thin * (1.0 - 1.5 * (u[0] * u[0] + u[1] * u[1] + u[2] * u[2]))

        def hit(i, p, along_of):
            a, b = along_of(i, u), along_of(i, v)
            both = thin * (a * (3.0 + 4.5 * a)) + rho * (b * (3.0 + 4.5 * b))
            return keep * p + WEIGHTS[i] * (flat + both)

        return hit

    for ref in (sx, sy, cy_, oe, oz):
        ref[...] = jnp.zeros_like(ref)
    for load in loads:
        load.wait()

    for x in range(X):
        r = dens[x]
        u = [vel[d, x] for d in range(3)]
        usq = 1.0 - 1.5 * (u[0] * u[0] + u[1] * u[1] + u[2] * u[2])
        ps = []
        for i in range(19):
            a = along(i, u)
            if a is None:
                ps.append(WEIGHTS[i] * r * usq)
            else:
                ps.append(WEIGHTS[i] * r * (usq + 3.0 * a + 4.5 * a * a))
            pops[i, x] = ps[i]
        rho, moms = moments(ps)
        inv = 1.0 / rho
        mom[0, x] = rho
        for d in range(3):
            mom[1 + d, x] = moms[d] * inv
    ready()
    pl.semaphore_wait(barrier, len(partners))
    send(0)

    def step(n, carry):
        par = lax.rem(n, 2)
        finish(*bundle(par))
        low, high = ry.at[par, 0], ry.at[par, 1]

        def tall(a):
            if a == 0:
                near = [low[2], sz[0], high[2]]
            else:
                at = DEEP if a == 1 else DEEP + 1
                mid = rx[par, INDEX[a], MOMS + 5 + DEEP]
                near = [rxy[par, 0, INDEX[a], at], mid, rxy[par, 1, INDEX[a], at]]
            near = jnp.concatenate(near, axis=0)
            far = [fz[par, INDEX[c], TRAVEL[a], 0] for c in zsides]
            halves = [jnp.where(facing, far[0], near), jnp.where(facing, near, far[-1])]
            return [roll(v, -a * width, 1) for v in halves]

        parts = [tall(a) for a in (0, 1, -1)]
        ends = [
            [roll(fz[par, INDEX[c], TRAVEL[a], 1], -a * width, 1) for a in (0, 1, -1)] for c in zsides
        ]

        def gather(three, slot, add):
            at = slot * width
            rel = lax.rem(elane + (Z - at), Z)
            v = jnp.where(rel < width, three[0], jnp.where(rel < HALF, three[2], three[1]))
            return roll(v, DEEP * block - at + add, 1)

        def packed(slot):
            halves = [gather([p[k] for p in parts], slot, HALF * k) for k in range(2)]
            return jnp.where(left, halves[0], halves[1])

        def packed_far(slot):
            halves = [gather(three, slot, HALF * k) for k, three in enumerate(ends)]
            if len(halves) == 1:
                halves.append(roll(halves[0], HALF, 1))
            return jnp.where(left, halves[0], halves[1])

        rho_z = packed(1)
        u_z = [packed(2 + d) for d in range(3)]
        old = oz[...]
        OZ = packed(0)
        for d, (shift, axis, mask) in enumerate(((block, 1, face_x), (1, 0, face_y), (1, 1, face_z))):
            t = 0.25 * (u_z[d] + roll(u_z[d], shift, axis)) * (old + roll(old, shift, axis))
            t = jnp.where(mask, t, 0.0)
            OZ = OZ + (t - roll(t, -shift, axis))
        oz[...] = OZ

        def around(px, s):
            if px < 0:
                return rxy[par, INDEX[s], 0, px + DEEP]
            if px >= X:
                return rxy[par, INDEX[s], 1, DEEP + 2 + px - X]
            return ry[par, INDEX[s], 3 + px]

        def speed(px):
            if px < 0:
                tiles, mid = [rxy[par, k, 0, 4] for k in range(2)], rx[par, 0, 1]
            elif px >= X:
                tiles, mid = [rxy[par, k, 1, DEEP] for k in range(2)], rx[par, 1, 1]
            else:
                tiles, mid = [ry[par, k, 1 if px == 0 else X + 4] for k in range(2)], mom[1, px]
            return jnp.concatenate([tiles[0], mid, tiles[1]], axis=0)

        def line(k, a, s):
            at, sub = (DEEP + 2 if a == 1 else 0) + k // DEEP, line_row(k, s)
            return rxy[par, INDEX[s], INDEX[a], at, sub : sub + 1, :]

        def outside(px, s):
            if px < 0:
                return line(2 if px == -1 else 5 + px + DEEP, 1, s)
            if px >= X:
                return line(2 if px == X else 5 + px - X - 1, -1, s)
            at = (0 if s == 1 else 4) + px
            return ry[par, INDEX[s], 2, at : at + 1, :]

        def inside(px, s):
            if 0 <= px < X:
                y = yend(s)
                return mom[2, px, y : y + 1, :]
            side, slot = (0, px + DEEP) if px < 0 else (1, px - X)
            at = slot if s == 1 else DEEP + slot
            return rx[par, side, MOMS + 6 + DEEP, at : at + 1, :]

        across = {}
        for lo, hi in ((-1, 0), (X - 1, X)):
            t = 0.25 * (speed(lo) + speed(hi)) * (oe[lo + DEEP] + oe[hi + DEEP])
            across[lo], across[hi] = -t, t
        beside = roll(OZ, 1, 0) + roll(OZ, -1, 0) + roll(OZ, 1, 1) + roll(OZ, -1, 1)
        beside = beside + roll(OZ, block, 1) + roll(OZ, -block, 1)
        CZ = chemical(OZ, beside)
        scale = -0.5 * OZ
        FZ = [
            scale * (roll(CZ, -block, 1) - roll(CZ, block, 1)),
            scale * (roll(CZ, -1, 0) - roll(CZ, 1, 0)),
            scale * (roll(CZ, -1, 1) - roll(CZ, 1, 1)),
        ]

        def sided(i, w):
            a = zsign * w[2]
            for d in range(2):
                if DIRS[i][d]:
                    a = a + w[d] if DIRS[i][d] == 1 else a - w[d]
            return a

        ZH = []
        hit = collide(rho_z, u_z, FZ)
        for k, (up, down) in enumerate(ZPAIRS):
            h = halo_pair(hit(up, packed_far(k), sided))
            ZH.append(roll(h, DIRS[up][1], 0)[own_rows, :])
        own_pair = jnp.where(column == DEEP, OZ, roll(OZ, -HALF, 1))
        order_pair, chem_pair = halo_pair(OZ), halo_pair(CZ)

        OE, C, F = {}, {}, {}

        def complete(px):
            if px < 0:
                mid = rx[par, 0, MOMS + 5 + px + DEEP]
            elif px >= X:
                mid = rx[par, 1, MOMS + 5 + px - X]
            else:
                mid = base[px]
            v = jnp.concatenate([around(px, 1), mid, around(px, -1)], axis=0)
            if px in across:
                v = v + across[px]
            parts = []
            for s, sign, y in ((1, 1.0, 8), (-1, -1.0, 8 + Y)):
                pair = oe[px + DEEP, y - 1 : y, :] + oe[px + DEEP, y : y + 1, :]
                t = 0.25 * (outside(px, s) + inside(px, s)) * pair
                parts.append(seam * jnp.broadcast_to(t, (16, Z)))
            half = E // 2
            if half == 16:
                v = v + jnp.concatenate(parts, axis=0)
            else:
                gap = jnp.zeros((E - 32, Z), jnp.float32)
                v = v + jnp.concatenate([parts[0], gap, parts[1]], axis=0)
            col = roll(own_pair, -((px + DEEP) * block + DEEP), 1)
            OE[px] = jnp.where((elane == 0) | (elane == Z - 1), col, v)

        def potential(px):
            o, col = OE[px], pick(order_pair, px)
            beside = OE[px - 1] + OE[px + 1] + roll(o, 1, 0) + roll(o, -1, 0)
            C[px] = chemical(o, beside + zshift(o, 1, col) + zshift(o, -1, col))

        def push(px):
            c, col = C[px], pick(chem_pair, px)
            y_dn, y_up = roll(c, 1, 0), roll(c, -1, 0)
            z_dn, z_up = zshift(c, 1, col), zshift(c, -1, col)
            scale = -0.5 * OE[px]
            F[px] = [
                scale * (C[px + 1] - C[px - 1]),
                scale * (y_up - y_dn),
                scale * (z_up - z_dn),
            ]
            if 0 <= px < X:
                lap = C[px + 1] + C[px - 1] + y_up + y_dn + z_up + z_dn - 6.0 * c
                base[px] = (OE[px] + mobility * lap)[own_rows, :]
                for s in SIGNS:
                    at = (0 if s == 1 else 4) + px
                    y = 7 if s == 1 else 8 + Y
                    for d in range(3):
                        fy[INDEX[s], d, at : at + 1, :] = F[px][d][y : y + 1, :]

        XH, YH, LH = {}, {}, {}

        def strike(px):
            if 0 <= px < X:
                rho = mom[0, px]
                u = [mom[1 + d, px] for d in range(3)]
                v, flat = forced(rho, 1.0 / rho, u, [f[own_rows, :] for f in F[px]])
                post[0, px] = post[0, px] + WEIGHTS[0] * flat
                for i in range(1, 19, 2):
                    a = along(i, v)
                    even = WEIGHTS[i] * flat + (4.5 * WEIGHTS[i]) * rho * (a * a)
                    odd = (3.0 * WEIGHTS[i]) * rho * a
                    post[i, px] = post[i, px] + even + odd
                    post[i + 1, px] = post[i + 1, px] + even - odd
                return
            a = 1 if px < 0 else -1
            ai = INDEX[a]
            rho = rx[par, ai, 0]
            u = [rx[par, ai, 1 + d] for d in range(3)]
            hit = collide(rho, u, [f[own_rows, :] for f in F[px]])
            for k, i in enumerate(CROSS[0][a]):
                XH[i] = hit(i, rx[par, ai, MOMS + k], along)
            for s in SIGNS:
                i = DIRS.index((a, s, 0))
                head = [line(k, a, s) for k in range(5)]
                y = 7 if s == 1 else 8 + Y
                hit = collide(head[0], head[1:4], [f[y : y + 1, :] for f in F[px]])
                LH[i] = hit(i, head[4], along)

        for px in range(-DEEP, X + DEEP):
            complete(px)
            if px - 1 >= -2:
                potential(px - 1)
            if px - 2 >= -1:
                push(px - 2)
                strike(px - 2)
        for px in range(-DEEP, X + DEEP):
            oe[px + DEEP] = OE[px]
        O = [OE[x][own_rows, :] for x in range(X)]
        for s in SIGNS:
            si = INDEX[s]
            rho = ry[par, si, 0]
            u = [ry[par, si, 1 + d] for d in range(3)]
            hit = collide(rho, u, [fy[si, d] for d in range(3)])
            for k, i in enumerate(CROSS[1][s]):
                YH[i] = hit(i, ry[par, si, MOMS + k], along)

        flows = {}
        pair_of = {i: k for k, both in enumerate(ZPAIRS) for i in both}
        for x in range(X):
            cols = [pick(ZH[k], x - DIRS[up][0]) for k, (up, _) in enumerate(ZPAIRS)]
            ps = []
            for i, (cx, cy, cz) in enumerate(DIRS):
                xs = x - cx
                own = 0 <= xs < X
                p = post[i, xs] if own else XH[i]
                if cy:
                    at = (0 if cy == 1 else 4) + xs
                    p = yshift(p, cy, YH[i][at : at + 1, :] if own else LH[i])
                if cz:
                    p = zshift(p, cz, cols[pair_of[i]])
                pops[i, x] = p
                ps.append(p)
            rho, moms = moments(ps)
            inv = 1.0 / rho
            flows[x] = [m * inv for m in moms]
            mom[0, x] = rho
            for d in range(3):
                mom[1 + d, x] = flows[x][d]

        @pl.when(n == ITERS - 1)
        def _():
            for s in SIGNS:
                cx_[INDEX[s]] = mom[1, xsrc(s)]
                y = ysrc(s)
                for x in range(X):
                    cy_[INDEX[s], 1 + x : 2 + x, :] = mom[2, x, y : y + 1, :]
                cz_[INDEX[s]] = pack([mom[3, x] for x in range(X)], s)
            launch(*farewell())

        tx = {0: 0.0, X: 0.0}
        for x in range(1, X):
            tx[x] = (flows[x][0] + flows[x - 1][0]) * (O[x] + O[x - 1])
        for x in range(X):
            f, o = flows[x], O[x]
            ty = jnp.where(row == 0, 0.0, (f[1] + roll(f[1], 1, 0)) * (o + roll(o, 1, 0)))
            tz = jnp.where(lane == 0, 0.0, (f[2] + roll(f[2], 1, 1)) * (o + roll(o, 1, 1)))
            change = tx[x + 1] - tx[x] + (roll(ty, -1, 0) - ty) + (roll(tz, -1, 1) - tz)
            base[x] = base[x] - 0.25 * change

        @pl.when(n < ITERS - 1)
        def _():
            ready()
            send(1 - par)

        return carry

    lax.fori_loop(0, ITERS, step, 0)
    finish(*farewell())

    pair = halo_pair(oz[...])[own_rows, :]
    for x in range(X):
        o, u = oe[x + DEEP, own_rows, :], [mom[1 + d, x] for d in range(3)]
        change = jnp.zeros((Y, Z), jnp.float32)
        if x == 0:
            change = change + (u[0] + rcx[0]) * (o + oe[DEEP - 1, own_rows, :])
        if x == X - 1:
            change = change - (u[0] + rcx[1]) * (o + oe[DEEP + X, own_rows, :])
        for s in SIGNS:
            at = 7 if s == 1 else 8 + Y
            other = rcy[INDEX[s], 1 + x : 2 + x, :]
            y = yend(s)
            t = (mom[2, x, y : y + 1, :] + other) * (
                oe[x + DEEP, at : at + 1, :] + oe[x + DEEP, 8 + y : 9 + y, :]
            )
            t = jnp.where(row == y, jnp.broadcast_to(t, (Y, Z)), 0.0)
            side = pick(pair, x)
            beside = roll(rcz[INDEX[s]], zend(s) - (1 + x), 1)
            t = t + jnp.where(lane == zend(s), (u[2] + beside) * (o + side), 0.0)
            change = change + t if s == 1 else change - t
        order[x] = base[x] + 0.25 * change


def on_device(sizes, order_param, density, velocity):
    X, Y, Z = order_param.shape
    f32 = jnp.float32
    plane, rows, tall = (Y, Z), (8, Z), (Y + 16, Z)
    planes = MOMS + 5 + DEEP + 2
    lines = 2 * planes * Y + 2 * 8 * (MOMS + 5) + 4 * 8 * DEEP
    lines += (1 if sizes[2] == 2 else 2) * (6 * Y + 8 * DEEP)
    vmem = [
        (19, X, Y, Z), (MOMS, X, Y, Z), (X, Y, Z), (X + 2 * DEEP,) + tall, tall,
        (X, Y, Z), (3, X, Y, Z), (lines, Z),
        (2, planes) + plane, (2, 2, planes) + plane,
        (2, X + 10) + rows, (2, 2, MOMS + 5) + rows, (2, 2, 2, 8) + rows,
        (2,) + plane, (2, 2, 3, 2) + tall, (2, 3) + rows,
        (2,) + plane, (2,) + rows, (2,) + plane,
        (2,) + plane, (2,) + rows, (2,) + plane,
    ]
    sems = [(3,), (1,), (2,), (1,), (1,)]
    spec = pl.BlockSpec(memory_space=pltpu.VMEM)
    return pl.pallas_call(
        functools.partial(kernel, sizes),
        out_shape=(pltpu.VMEM((X, Y, Z), f32), pltpu.VMEM((19, X, Y, Z), f32)),
        in_specs=[pl.BlockSpec(memory_space=pl.ANY)] * 3,
        out_specs=(spec, spec),
        scratch_shapes=[pltpu.VMEM(s, f32) for s in vmem]
        + [pltpu.SemaphoreType.DMA(n) for n in sems],
        compiler_params=pltpu.CompilerParams(collective_id=0, has_side_effects=True),
    )(order_param, density, velocity)


def solution(mesh):
    sizes = tuple(mesh.shape[a] for a in AXES)
    return jax.shard_map(
        functools.partial(on_device, sizes),
        mesh=mesh,
        in_specs=(P("gx", "gy", "gz"), P("gx", "gy", "gz"), P(None, "gx", "gy", "gz")),
        out_specs=(P("gx", "gy", "gz"), P(None, "gx", "gy", "gz")),
        check_vma=False,
    )
```

```python
import functools
import math

import jax
import jax.numpy as jnp
from jax import lax
from jax.experimental import pallas as pl
from jax.experimental.pallas import tpu as pltpu
from jax.sharding import PartitionSpec as P

ITERS = 5
MESH = pl.DeviceIdType.MESH
AXES = ("gx", "gy", "gz")
DIRS = [
    (0, 0, 0),
    (1, 0, 0),
    (-1, 0, 0),
    (0, 1, 0),
    (0, -1, 0),
    (0, 0, 1),
    (0, 0, -1),
    (1, 1, 0),
    (-1, -1, 0),
    (1, -1, 0),
    (-1, 1, 0),
    (1, 0, 1),
    (-1, 0, -1),
    (1, 0, -1),
    (-1, 0, 1),
    (0, 1, 1),
    (0, -1, -1),
    (0, 1, -1),
    (0, -1, 1),
]
WEIGHTS = [1.0 / 3.0] + [1.0 / 18.0] * 6 + [1.0 / 36.0] * 12
quadratic = -0.1
quartic = 0.1
stiffness = 0.02
mobility = 0.5
relax_time = 0.8

SIGNS = (1, -1)
INDEX = {1: 0, -1: 1}
TRAVEL = {0: 0, 1: 1, -1: 2}
CROSS = [{s: [i for i in range(19) if DIRS[i][d] == s] for s in SIGNS} for d in range(3)]
EDGES = [(a, b) for a in SIGNS for b in SIGNS]
ZPAIRS = [
    (DIRS.index((a, b, 1)), DIRS.index((a, b, -1)))
    for a, b in ((0, 0), (1, 0), (-1, 0), (0, 1), (0, -1))
]
DEEP = 3
HALF = 64
MOMS = 4


def kernel(sizes, order_in, dens_in, vel_in, order, pops, *scratch):
    (post, mom, base, oe, oz, dens, vel, bulk) = scratch[0:8]
    (sx, rx, sy, ry, rxy, sz, fz, fy) = scratch[8:16]
    (cx_, cy_, cz_, rcx, rcy, rcz) = scratch[16:22]
    (si_, sa, ra, sc, rc) = scratch[22:27]
    X, Y, Z = order.shape
    E = Y + 8
    own_rows = slice(0, Y)
    block = 2 * DEEP
    width = X * block
    me = [lax.axis_index(a) for a in AXES]
    zsides = (1,) if sizes[2] == 2 else SIGNS

    def device(off):
        return {
            a: lax.rem(me[k] + (off[k] + sizes[k]), sizes[k]) if off[k] else me[k]
            for k, a in enumerate(AXES)
        }

    partners = [
        (a, b, c)
        for a in (1, -1, 0)
        for b in (1, -1, 0)
        for c in zsides + (0,)
        if (a, b, c) != (0, 0, 0)
    ]
    place_of = {off: device(off) for off in partners}
    if sizes[2] == 2:
        place_of[(0, 0, -1)] = place_of[(0, 0, 1)]
    barrier = pltpu.get_barrier_semaphore()
    for off in partners:
        pl.semaphore_signal(barrier, inc=1, device_id=place_of[off], device_id_type=MESH)
    loads = [
        pltpu.make_async_copy(src, dst, si_.at[k])
        for k, (src, dst) in enumerate(((order_in, base), (dens_in, dens), (vel_in, vel)))
    ]
    for load in loads:
        load.start()

    lane = lax.broadcasted_iota(jnp.int32, (Y, Z), 1)
    row = lax.broadcasted_iota(jnp.int32, (Y, Z), 0)
    elane = lax.broadcasted_iota(jnp.int32, (E, Z), 1)
    erow = lax.broadcasted_iota(jnp.int32, (E, Z), 0)
    left = elane < HALF
    frame = jnp.where(left, elane, elane - HALF)
    column = lax.rem(frame, block)
    facing = lax.rem(elane, block) < DEEP
    zsign = jnp.where(left, 1.0, -1.0)
    low_col = lane < HALF
    face_z = column == DEEP
    face_x = (frame // block == DEEP) | (frame // block == DEEP + X)
    face_y = (erow == 0) | (erow == Y)
    sub = lax.broadcasted_iota(jnp.int32, (8, Z), 0)
    last = column == DEEP - 1

    def extend(mid, low, high):
        return jnp.concatenate([mid, jnp.where(sub < 4, high, low)], axis=0)

    def roll(v, s, axis):
        s = s % v.shape[axis]
        return v if s == 0 else pltpu.roll(v, s, axis)

    def zend(s):
        return 0 if s == 1 else Z - 1

    def yend(s):
        return 0 if s == 1 else Y - 1

    def xsrc(s):
        return X - 1 if s == 1 else 0

    def ysrc(s):
        return Y - 1 if s == 1 else 0

    def next_row(s):
        return E - 1 if s == 1 else Y

    def deep_rows(s):
        return pl.ds(8 - DEEP if s == 1 else 0, DEEP)

    def flat_rows(s):
        return pl.ds(0 if s == 1 else 4, X)

    def line_row(k, s):
        return (8 - DEEP if s == 1 else 0) + k % DEEP

    def halo_pair(v):
        return jnp.where(last, v, roll(v, -(HALF + 2), 1))

    def pick(pair, px):
        return roll(pair, -((px + DEEP) * block + DEEP - 1), 1)

    def zshift(v, s, col):
        lanes = lane if v.shape[0] == Y else elane
        return jnp.where(lanes == zend(s), col, roll(v, s, 1))

    def yshift(v, s, halo):
        return jnp.where(row == yend(s), jnp.broadcast_to(halo, v.shape), roll(v, s, 0))

    def pack(planes, s):
        acc = jnp.zeros((Y, Z), jnp.float32)
        for x in range(X):
            at = 1 + x
            acc = jnp.where(lane == at, roll(planes[x], at - (Z - 1 if s == 1 else 0), 1), acc)
        return acc

    def launch(messages, ssem, rsem):
        for src, dst, off in messages:
            pltpu.make_async_remote_copy(
                src_ref=src,
                dst_ref=dst,
                send_sem=ssem,
                recv_sem=rsem,
                device_id=place_of[off],
                device_id_type=MESH,
            ).start()

    def finish(messages, ssem, rsem):
        lines = sum(math.prod(src.shape[:-1]) for src, _, _ in messages)
        span = bulk.at[pl.ds(0, lines)]
        for sem in (rsem, ssem):
            pltpu.make_async_copy(span, span, sem).wait()

    def bundle(par):
        messages = []

        def beside(a, b, c):
            dst = fz.at[par, INDEX[c], TRAVEL[a]]
            rows = {1: pl.ds(Y - DEEP, DEEP), -1: pl.ds(0, DEEP), 0: pl.ds(0, Y)}[b]
            land = pl.ds({1: E - DEEP, -1: Y, 0: 0}[b], DEEP if b else Y)
            planes = pl.ds(0, 1 if a and b else 2)
            messages.append((sz.at[planes, rows, :], dst.at[planes, land, :], (a, b, c)))

        for c in zsides:
            for a, b in EDGES + [(0, 1), (0, -1)]:
                beside(a, b, c)
        for a, b in EDGES:
            bi, ai, rows = INDEX[b], INDEX[a], deep_rows(b)
            src = pl.ds(X + 2 if a == 1 else 0, 8)
            messages.append((sy.at[bi, src, rows, :], rxy.at[par, bi, ai, :, rows, :], (a, b, 0)))
        for s in SIGNS:
            si = INDEX[s]
            messages.append((sy.at[si, pl.ds(2, MOMS + 5)], ry.at[par, si], (0, s, 0)))
        for c in zsides:
            for a in SIGNS:
                beside(a, 0, c)
        for s in SIGNS:
            messages.append((sx.at[INDEX[s]], rx.at[par, INDEX[s]], (s, 0, 0)))
        for c in zsides:
            beside(0, 0, c)
        return messages, sa.at[0], ra.at[par]

    def farewell():
        messages = []
        for s in SIGNS:
            messages.append((cy_.at[INDEX[s]], rcy.at[INDEX[s]], (0, s, 0)))
        for s in SIGNS:
            messages.append((cz_.at[INDEX[s]], rcz.at[INDEX[s]], (0, 0, s)))
        for s in SIGNS:
            messages.append((cx_.at[INDEX[s]], rcx.at[INDEX[s]], (s, 0, 0)))
        return messages, sc.at[0], rc.at[0]

    def moments(ps):
        def total(which):
            return functools.reduce(lambda a, b: a + b, [ps[i] for i in which])

        sums = [[total(CROSS[d][s]) for s in SIGNS] for d in range(3)]
        still = total([i for i in range(19) if DIRS[i][0] == 0])
        return still + sums[0][0] + sums[0][1], [up - down for up, down in sums]

    def chemical(o, beside):
        return quadratic * o + quartic * o * o * o - stiffness * (beside - 6.0 * o)

    def along(i, w):
        a = None
        for d in range(3):
            if DIRS[i][d]:
                t = w[d] if DIRS[i][d] == 1 else -w[d]
                a = t if a is None else a + t
        return a

    keep = 1.0 - 1.0 / relax_time
    mix = 1.0 / relax_time - 1.0

    def relax(x):
        ps = [pops[i, x] for i in range(19)]
        rho, u = mom[0, x], [mom[1 + d, x] for d in range(3)]
        flat = (mix * rho) * (1.0 - 1.5 * (u[0] * u[0] + u[1] * u[1] + u[2] * u[2]))
        out = [keep * ps[0] + WEIGHTS[0] * flat]
        for i in range(1, 19, 2):
            a = along(i, u)
            even = WEIGHTS[i] * flat + (4.5 * mix * WEIGHTS[i]) * rho * (a * a)
            odd = (3.0 * mix * WEIGHTS[i]) * rho * a
            out.append(keep * ps[i] + even + odd)
            out.append(keep * ps[i + 1] + even - odd)
        for i in range(19):
            post[i, x] = out[i]

    def place(acc, v, slot, x):
        at = slot * width + x * block
        mask = (lane >= at) & (lane < at + block)
        return jnp.where(mask, roll(v, at - (Z - DEEP), 1), acc)

    def ready():
        first = jnp.zeros((Y, Z), jnp.float32)
        second = jnp.zeros((Y, Z), jnp.float32)
        for x in range(X):
            heads, b = [mom[g, x] for g in range(MOMS)], base[x]
            u = heads[1:]
            out = [pops[i, x] for i in range(19)]
            for s in SIGNS:
                si = INDEX[s]
                y, at = ysrc(s), (0 if s == 1 else 4) + x
                for g in range(MOMS):
                    sy[si, 2 + g, at : at + 1, :] = heads[g][y : y + 1, :]
                for k, i in enumerate(CROSS[1][s]):
                    sy[si, 2 + MOMS + k, at : at + 1, :] = out[i][y : y + 1, :]
                rows = slice(Y - DEEP, Y) if s == 1 else slice(0, DEEP)
                sy[si, 5 + x, deep_rows(s), :] = b[rows, :]
                if x == 0:
                    sy[si, 3, deep_rows(s), :] = u[0][rows, :]
                if x == X - 1:
                    sy[si, X + 6, deep_rows(s), :] = u[0][rows, :]
                for a in SIGNS:
                    lines = {}
                    if x == xsrc(a):
                        lines = dict(enumerate(heads + [out[DIRS.index((a, s, 0))]]))
                    slot = x - (X - DEEP) if a == 1 else x - 1
                    if 0 <= slot < DEEP - 1:
                        lines[5 + slot] = u[1]
                    for k, v in lines.items():
                        at, sub = (X + 7 if a == 1 else 0) + k // DEEP, line_row(k, s)
                        sy[si, at, sub : sub + 1, :] = v[y : y + 1, :]
            for g, v in enumerate([b] + heads):
                first = place(first, v, g, x)
            for k, (up, down) in enumerate(ZPAIRS):
                second = place(second, jnp.where(low_col, out[down], out[up]), k, x)
        sz[0] = first
        sz[1] = second
        for s in SIGNS:
            si = INDEX[s]
            rows = slice(Y - DEEP, Y) if s == 1 else slice(0, DEEP)
            for at in (4, X + 5):
                sy[si, at, deep_rows(s), :] = first[rows, :]

    def ready_planes():
        for s in SIGNS:
            si, edge = INDEX[s], xsrc(s)
            for g in range(MOMS):
                sx[si, g] = mom[g, edge]
            for k, i in enumerate(CROSS[0][s]):
                sx[si, MOMS + k] = pops[i, edge]
            for slot in range(DEEP):
                x = slot + (X - DEEP if s == 1 else 0)
                sx[si, MOMS + 5 + slot] = base[x]
                sx[si, MOMS + 6 + DEEP, slot : slot + 1, :] = mom[2, x, 0:1, :]
                sx[si, MOMS + 6 + DEEP, DEEP + slot : DEEP + slot + 1, :] = mom[2, x, Y - 1 :, :]
            sx[si, MOMS + 5 + DEEP] = sz[0]

    def send(par):
        messages, ssem, rsem = bundle(par)
        first = [m for m in messages if m[2][1]]
        launch(first, ssem, rsem)
        ready_planes()
        launch(messages[len(first) :], ssem, rsem)
        for x in range(X):
            relax(x)

    def forced(rho, inv, u, force):
        v = [u[d] + force[d] * inv for d in range(3)]
        flat = rho * (1.0 - 1.5 * (v[0] * v[0] + v[1] * v[1] + v[2] * v[2]))
        return v, flat

    def collide(rho, u, force):
        v, flat = forced(rho, 1.0 / rho, u, force)
        thin = mix * rho
        flat = flat + thin * (1.0 - 1.5 * (u[0] * u[0] + u[1] * u[1] + u[2] * u[2]))

        def hit(i, p, along_of):
            a, b = along_of(i, u), along_of(i, v)
            both = thin * (a * (3.0 + 4.5 * a)) + rho * (b * (3.0 + 4.5 * b))
            return keep * p + WEIGHTS[i] * (flat + both)

        return hit

    for ref in (sx, sy, cy_, oe, oz):
        ref[...] = jnp.zeros_like(ref)
    for load in loads:
        load.wait()

    for x in range(X):
        r = dens[x]
        u = [vel[d, x] for d in range(3)]
        usq = 1.0 - 1.5 * (u[0] * u[0] + u[1] * u[1] + u[2] * u[2])
        ps = []
        for i in range(19):
            a = along(i, u)
            if a is None:
                ps.append(WEIGHTS[i] * r * usq)
            else:
                ps.append(WEIGHTS[i] * r * (usq + 3.0 * a + 4.5 * a * a))
            pops[i, x] = ps[i]
        rho, moms = moments(ps)
        inv = 1.0 / rho
        mom[0, x] = rho
        for d in range(3):
            mom[1 + d, x] = moms[d] * inv
    ready()
    pl.semaphore_wait(barrier, len(partners))
    send(0)

    def step(n, carry):
        par = lax.rem(n, 2)
        finish(*bundle(par))
        low, high = ry.at[par, 0], ry.at[par, 1]

        def tall(a):
            if a == 0:
                near = extend(sz[0], low[2], high[2])
            else:
                at = DEEP if a == 1 else DEEP + 1
                mid = rx[par, INDEX[a], MOMS + 5 + DEEP]
                near = extend(mid, rxy[par, 0, INDEX[a], at], rxy[par, 1, INDEX[a], at])
            far = [fz[par, INDEX[c], TRAVEL[a], 0] for c in zsides]
            halves = [jnp.where(facing, far[0], near), jnp.where(facing, near, far[-1])]
            return [roll(v, -a * width, 1) for v in halves]

        parts = [tall(a) for a in (0, 1, -1)]
        ends = [
            [roll(fz[par, INDEX[c], TRAVEL[a], 1], -a * width, 1) for a in (0, 1, -1)] for c in zsides
        ]

        def gather(three, slot, add):
            at = slot * width
            rel = lax.rem(elane + (Z - at), Z)
            v = jnp.where(rel < width, three[0], jnp.where(rel < HALF, three[2], three[1]))
            return roll(v, DEEP * block - at + add, 1)

        def packed(slot):
            halves = [gather([p[k] for p in parts], slot, HALF * k) for k in range(2)]
            return jnp.where(left, halves[0], halves[1])

        def packed_far(slot):
            halves = [gather(three, slot, HALF * k) for k, three in enumerate(ends)]
            if len(halves) == 1:
                halves.append(roll(halves[0], HALF, 1))
            return jnp.where(left, halves[0], halves[1])

        rho_z = packed(1)
        u_z = [packed(2 + d) for d in range(3)]
        old = oz[...]
        OZ = packed(0)
        for d, (shift, axis, mask) in enumerate(((block, 1, face_x), (1, 0, face_y), (1, 1, face_z))):
            t = 0.25 * (u_z[d] + roll(u_z[d], shift, axis)) * (old + roll(old, shift, axis))
            t = jnp.where(mask, t, 0.0)
            OZ = OZ + (t - roll(t, -shift, axis))
        oz[...] = OZ

        def around(px, s):
            if px < 0:
                return rxy[par, INDEX[s], 0, px + DEEP]
            if px >= X:
                return rxy[par, INDEX[s], 1, DEEP + 2 + px - X]
            return ry[par, INDEX[s], 3 + px]

        def speed(px):
            if px < 0:
                tiles, mid = [rxy[par, k, 0, 4] for k in range(2)], rx[par, 0, 1]
            elif px >= X:
                tiles, mid = [rxy[par, k, 1, DEEP] for k in range(2)], rx[par, 1, 1]
            else:
                tiles, mid = [ry[par, k, 1 if px == 0 else X + 4] for k in range(2)], mom[1, px]
            return extend(mid, tiles[0], tiles[1])

        def line(k, a, s):
            at, sub = (DEEP + 2 if a == 1 else 0) + k // DEEP, line_row(k, s)
            return rxy[par, INDEX[s], INDEX[a], at, sub : sub + 1, :]

        def outside(px, s):
            if px < 0:
                return line(2 if px == -1 else 5 + px + DEEP, 1, s)
            if px >= X:
                return line(2 if px == X else 5 + px - X - 1, -1, s)
            at = (0 if s == 1 else 4) + px
            return ry[par, INDEX[s], 2, at : at + 1, :]

        def inside(px, s):
            if 0 <= px < X:
                y = yend(s)
                return mom[2, px, y : y + 1, :]
            side, slot = (0, px + DEEP) if px < 0 else (1, px - X)
            at = slot if s == 1 else DEEP + slot
            return rx[par, side, MOMS + 6 + DEEP, at : at + 1, :]

        across = {}
        for lo, hi in ((-1, 0), (X - 1, X)):
            t = 0.25 * (speed(lo) + speed(hi)) * (oe[lo + DEEP] + oe[hi + DEEP])
            across[lo], across[hi] = -t, t
        beside = roll(OZ, 1, 0) + roll(OZ, -1, 0) + roll(OZ, 1, 1) + roll(OZ, -1, 1)
        beside = beside + roll(OZ, block, 1) + roll(OZ, -block, 1)
        CZ = chemical(OZ, beside)
        scale = -0.5 * OZ
        FZ = [
            scale * (roll(CZ, -block, 1) - roll(CZ, block, 1)),
            scale * (roll(CZ, -1, 0) - roll(CZ, 1, 0)),
            scale * (roll(CZ, -1, 1) - roll(CZ, 1, 1)),
        ]

        def sided(i, w):
            a = zsign * w[2]
            for d in range(2):
                if DIRS[i][d]:
                    a = a + w[d] if DIRS[i][d] == 1 else a - w[d]
            return a

        ZH = []
        hit = collide(rho_z, u_z, FZ)
        for k, (up, down) in enumerate(ZPAIRS):
            h = halo_pair(hit(up, packed_far(k), sided))
            ZH.append(roll(h, DIRS[up][1], 0)[own_rows, :])
        own_pair = jnp.where(column == DEEP, OZ, roll(OZ, -HALF, 1))
        order_pair, chem_pair = halo_pair(OZ), halo_pair(CZ)

        OE, C, F = {}, {}, {}

        def complete(px):
            if px < 0:
                mid = rx[par, 0, MOMS + 5 + px + DEEP]
            elif px >= X:
                mid = rx[par, 1, MOMS + 5 + px - X]
            else:
                mid = base[px]
            v = extend(mid, around(px, 1), around(px, -1))
            if px in across:
                v = v + across[px]
            t = {}
            for s in SIGNS:
                y, z = yend(s), next_row(s)
                pair = oe[px + DEEP, y : y + 1, :] + oe[px + DEEP, z : z + 1, :]
                line_t = 0.25 * (outside(px, s) + inside(px, s)) * pair
                t[s] = jnp.broadcast_to(line_t, (8, Z))
            halo = v[Y:, :] + jnp.where(sub == 0, t[-1], jnp.where(sub == 7, -t[1], 0.0))
            head = v[:8, :] + jnp.where(sub == 0, t[1], 0.0)
            tail = v[Y - 8 : Y, :] - jnp.where(sub == 7, t[-1], 0.0)
            rest = [v[8 : Y - 8, :]] if Y > 16 else []
            v = jnp.concatenate([head] + rest + [tail, halo], axis=0)
            col = roll(own_pair, -((px + DEEP) * block + DEEP), 1)
            OE[px] = jnp.where((elane == 0) | (elane == Z - 1), col, v)

        def potential(px):
            o, col = OE[px], pick(order_pair, px)
            beside = OE[px - 1] + OE[px + 1] + roll(o, 1, 0) + roll(o, -1, 0)
            C[px] = chemical(o, beside + zshift(o, 1, col) + zshift(o, -1, col))

        def push(px):
            c, col = C[px], pick(chem_pair, px)
            y_dn, y_up = roll(c, 1, 0), roll(c, -1, 0)
            z_dn, z_up = zshift(c, 1, col), zshift(c, -1, col)
            scale = -0.5 * OE[px]
            F[px] = [
                scale * (C[px + 1] - C[px - 1]),
                scale * (y_up - y_dn),
                scale * (z_up - z_dn),
            ]
            if 0 <= px < X:
                lap = C[px + 1] + C[px - 1] + y_up + y_dn + z_up + z_dn - 6.0 * c
                base[px] = (OE[px] + mobility * lap)[own_rows, :]
                for s in SIGNS:
                    at = (0 if s == 1 else 4) + px
                    y = next_row(s)
                    for d in range(3):
                        fy[INDEX[s], d, at : at + 1, :] = F[px][d][y : y + 1, :]

        XH, YH, LH = {}, {}, {}

        def strike(px):
            if 0 <= px < X:
                rho = mom[0, px]
                u = [mom[1 + d, px] for d in range(3)]
                v, flat = forced(rho, 1.0 / rho, u, [f[own_rows, :] for f in F[px]])
                post[0, px] = post[0, px] + WEIGHTS[0] * flat
                for i in range(1, 19, 2):
                    a = along(i, v)
                    even = WEIGHTS[i] * flat + (4.5 * WEIGHTS[i]) * rho * (a * a)
                    odd = (3.0 * WEIGHTS[i]) * rho * a
                    post[i, px] = post[i, px] + even + odd
                    post[i + 1, px] = post[i + 1, px] + even - odd
                return
            a = 1 if px < 0 else -1
            ai = INDEX[a]
            rho = rx[par, ai, 0]
            u = [rx[par, ai, 1 + d] for d in range(3)]
            hit = collide(rho, u, [f[own_rows, :] for f in F[px]])
            for k, i in enumerate(CROSS[0][a]):
                XH[i] = hit(i, rx[par, ai, MOMS + k], along)
            for s in SIGNS:
                i = DIRS.index((a, s, 0))
                head = [line(k, a, s) for k in range(5)]
                y = next_row(s)
                hit = collide(head[0], head[1:4], [f[y : y + 1, :] for f in F[px]])
                LH[i] = hit(i, head[4], along)

        for px in range(-DEEP, X + DEEP):
            complete(px)
            if px - 1 >= -2:
                potential(px - 1)
            if px - 2 >= -1:
                push(px - 2)
                strike(px - 2)
        for px in range(-DEEP, X + DEEP):
            oe[px + DEEP] = OE[px]
        O = [OE[x][own_rows, :] for x in range(X)]
        for s in SIGNS:
            si = INDEX[s]
            rho = ry[par, si, 0]
            u = [ry[par, si, 1 + d] for d in range(3)]
            hit = collide(rho, u, [fy[si, d] for d in range(3)])
            for k, i in enumerate(CROSS[1][s]):
                YH[i] = hit(i, ry[par, si, MOMS + k], along)

        flows = {}
        pair_of = {i: k for k, both in enumerate(ZPAIRS) for i in both}
        for x in range(X):
            cols = [pick(ZH[k], x - DIRS[up][0]) for k, (up, _) in enumerate(ZPAIRS)]
            ps = []
            for i, (cx, cy, cz) in enumerate(DIRS):
                xs = x - cx
                own = 0 <= xs < X
                p = post[i, xs] if own else XH[i]
                if cy:
                    at = (0 if cy == 1 else 4) + xs
                    p = yshift(p, cy, YH[i][at : at + 1, :] if own else LH[i])
                if cz:
                    p = zshift(p, cz, cols[pair_of[i]])
                pops[i, x] = p
                ps.append(p)
            rho, moms = moments(ps)
            inv = 1.0 / rho
            flows[x] = [m * inv for m in moms]
            mom[0, x] = rho
            for d in range(3):
                mom[1 + d, x] = flows[x][d]

        @pl.when(n == ITERS - 1)
        def _():
            for s in SIGNS:
                cx_[INDEX[s]] = mom[1, xsrc(s)]
                y = ysrc(s)
                for x in range(X):
                    cy_[INDEX[s], 1 + x : 2 + x, :] = mom[2, x, y : y + 1, :]
                cz_[INDEX[s]] = pack([mom[3, x] for x in range(X)], s)
            launch(*farewell())

        tx = {0: 0.0, X: 0.0}
        for x in range(1, X):
            tx[x] = (flows[x][0] + flows[x - 1][0]) * (O[x] + O[x - 1])
        for x in range(X):
            f, o = flows[x], O[x]
            ty = jnp.where(row == 0, 0.0, (f[1] + roll(f[1], 1, 0)) * (o + roll(o, 1, 0)))
            tz = jnp.where(lane == 0, 0.0, (f[2] + roll(f[2], 1, 1)) * (o + roll(o, 1, 1)))
            change = tx[x + 1] - tx[x] + (roll(ty, -1, 0) - ty) + (roll(tz, -1, 1) - tz)
            base[x] = base[x] - 0.25 * change

        @pl.when(n < ITERS - 1)
        def _():
            ready()
            send(1 - par)

        return carry

    lax.fori_loop(0, ITERS, step, 0)
    finish(*farewell())

    pair = halo_pair(oz[...])[own_rows, :]
    for x in range(X):
        o, u = oe[x + DEEP, own_rows, :], [mom[1 + d, x] for d in range(3)]
        change = jnp.zeros((Y, Z), jnp.float32)
        if x == 0:
            change = change + (u[0] + rcx[0]) * (o + oe[DEEP - 1, own_rows, :])
        if x == X - 1:
            change = change - (u[0] + rcx[1]) * (o + oe[DEEP + X, own_rows, :])
        for s in SIGNS:
            at = next_row(s)
            other = rcy[INDEX[s], 1 + x : 2 + x, :]
            y = yend(s)
            t = (mom[2, x, y : y + 1, :] + other) * (
                oe[x + DEEP, at : at + 1, :] + oe[x + DEEP, y : y + 1, :]
            )
            t = jnp.where(row == y, jnp.broadcast_to(t, (Y, Z)), 0.0)
            side = pick(pair, x)
            beside = roll(rcz[INDEX[s]], zend(s) - (1 + x), 1)
            t = t + jnp.where(lane == zend(s), (u[2] + beside) * (o + side), 0.0)
            change = change + t if s == 1 else change - t
        order[x] = base[x] + 0.25 * change


def on_device(sizes, order_param, density, velocity):
    X, Y, Z = order_param.shape
    f32 = jnp.float32
    plane, rows, tall = (Y, Z), (8, Z), (Y + 8, Z)
    planes = MOMS + 5 + DEEP + 2
    lines = 2 * planes * Y + 2 * 8 * (MOMS + 5) + 4 * 8 * DEEP
    lines += (1 if sizes[2] == 2 else 2) * (6 * Y + 8 * DEEP)
    vmem = [
        (19, X, Y, Z), (MOMS, X, Y, Z), (X, Y, Z), (X + 2 * DEEP,) + tall, tall,
        (X, Y, Z), (3, X, Y, Z), (lines, Z),
        (2, planes) + plane, (2, 2, planes) + plane,
        (2, X + 10) + rows, (2, 2, MOMS + 5) + rows, (2, 2, 2, 8) + rows,
        (2,) + plane, (2, 2, 3, 2) + tall, (2, 3) + rows,
        (2,) + plane, (2,) + rows, (2,) + plane,
        (2,) + plane, (2,) + rows, (2,) + plane,
    ]
    sems = [(3,), (1,), (2,), (1,), (1,)]
    spec = pl.BlockSpec(memory_space=pltpu.VMEM)
    return pl.pallas_call(
        functools.partial(kernel, sizes),
        out_shape=(pltpu.VMEM((X, Y, Z), f32), pltpu.VMEM((19, X, Y, Z), f32)),
        in_specs=[pl.BlockSpec(memory_space=pl.ANY)] * 3,
        out_specs=(spec, spec),
        scratch_shapes=[pltpu.VMEM(s, f32) for s in vmem]
        + [pltpu.SemaphoreType.DMA(n) for n in sems],
        compiler_params=pltpu.CompilerParams(collective_id=0, has_side_effects=True),
    )(order_param, density, velocity)


def solution(mesh):
    sizes = tuple(mesh.shape[a] for a in AXES)
    return jax.shard_map(
        functools.partial(on_device, sizes),
        mesh=mesh,
        in_specs=(P("gx", "gy", "gz"), P("gx", "gy", "gz"), P(None, "gx", "gy", "gz")),
        out_specs=(P("gx", "gy", "gz"), P(None, "gx", "gy", "gz")),
        check_vma=False,
    )
```

```python
import functools
import math

import jax
import jax.numpy as jnp
from jax import lax
from jax.experimental import pallas as pl
from jax.experimental.pallas import tpu as pltpu
from jax.sharding import PartitionSpec as P

ITERS = 5
MESH = pl.DeviceIdType.MESH
AXES = ("gx", "gy", "gz")
DIRS = [
    (0, 0, 0),
    (1, 0, 0),
    (-1, 0, 0),
    (0, 1, 0),
    (0, -1, 0),
    (0, 0, 1),
    (0, 0, -1),
    (1, 1, 0),
    (-1, -1, 0),
    (1, -1, 0),
    (-1, 1, 0),
    (1, 0, 1),
    (-1, 0, -1),
    (1, 0, -1),
    (-1, 0, 1),
    (0, 1, 1),
    (0, -1, -1),
    (0, 1, -1),
    (0, -1, 1),
]
WEIGHTS = [1.0 / 3.0] + [1.0 / 18.0] * 6 + [1.0 / 36.0] * 12
quadratic = -0.1
quartic = 0.1
stiffness = 0.02
mobility = 0.5
relax_time = 0.8

SIGNS = (1, -1)
INDEX = {1: 0, -1: 1}
TRAVEL = {0: 0, 1: 1, -1: 2}
CROSS = [{s: [i for i in range(19) if DIRS[i][d] == s] for s in SIGNS} for d in range(3)]
EDGES = [(a, b) for a in SIGNS for b in SIGNS]
ZPAIRS = [
    (DIRS.index((a, b, 1)), DIRS.index((a, b, -1)))
    for a, b in ((0, 0), (1, 0), (-1, 0), (0, 1), (0, -1))
]
DEEP = 3
HALF = 64
MOMS = 4


def kernel(sizes, order_in, dens_in, vel_in, order, pops, *scratch):
    (post, mom, base, oe, oz, dens, vel, bulk) = scratch[0:8]
    (sx, rx, sy, ry, sxy, rxy, sz, fz, fy, fp) = scratch[8:18]
    (cx_, cy_, cz_, rcx, rcy, rcz) = scratch[18:24]
    (si_, sa, ra, sc, rc) = scratch[24:29]
    X, Y, Z = order.shape
    E = Y + 8
    own_rows = slice(0, Y)
    block = 2 * DEEP
    width = X * block
    me = [lax.axis_index(a) for a in AXES]
    zsides = (1,) if sizes[2] == 2 else SIGNS

    def device(off):
        return {
            a: lax.rem(me[k] + (off[k] + sizes[k]), sizes[k]) if off[k] else me[k]
            for k, a in enumerate(AXES)
        }

    partners = [
        (a, b, c)
        for a in (1, -1, 0)
        for b in (1, -1, 0)
        for c in zsides + (0,)
        if (a, b, c) != (0, 0, 0)
    ]
    place_of = {off: device(off) for off in partners}
    if sizes[2] == 2:
        place_of[(0, 0, -1)] = place_of[(0, 0, 1)]
    barrier = pltpu.get_barrier_semaphore()
    for off in partners:
        pl.semaphore_signal(barrier, inc=1, device_id=place_of[off], device_id_type=MESH)
    loads = [
        pltpu.make_async_copy(src, dst, si_.at[k])
        for k, (src, dst) in enumerate(((order_in, base), (dens_in, dens), (vel_in, vel)))
    ]
    for load in loads:
        load.start()

    lane = lax.broadcasted_iota(jnp.int32, (Y, Z), 1)
    row = lax.broadcasted_iota(jnp.int32, (Y, Z), 0)
    elane = lax.broadcasted_iota(jnp.int32, (E, Z), 1)
    erow = lax.broadcasted_iota(jnp.int32, (E, Z), 0)
    left = elane < HALF
    frame = jnp.where(left, elane, elane - HALF)
    column = lax.rem(frame, block)
    facing = lax.rem(elane, block) < DEEP
    zsign = jnp.where(left, 1.0, -1.0)
    low_col = lane < HALF
    face_z = column == DEEP
    face_x = (frame // block == DEEP) | (frame // block == DEEP + X)
    face_y = (erow == 0) | (erow == Y)
    sub = lax.broadcasted_iota(jnp.int32, (8, Z), 0)
    last = column == DEEP - 1

    def extend(mid, low, high):
        return jnp.concatenate([mid, jnp.where(sub < 4, high, low)], axis=0)

    def roll(v, s, axis):
        s = s % v.shape[axis]
        return v if s == 0 else pltpu.roll(v, s, axis)

    def zend(s):
        return 0 if s == 1 else Z - 1

    def yend(s):
        return 0 if s == 1 else Y - 1

    def xsrc(s):
        return X - 1 if s == 1 else 0

    def ysrc(s):
        return Y - 1 if s == 1 else 0

    def next_row(s):
        return E - 1 if s == 1 else Y

    def deep_rows(s):
        return pl.ds(8 - DEEP if s == 1 else 0, DEEP)

    def flat_rows(s):
        return pl.ds(0 if s == 1 else 4, X)

    def spare(s):
        return 4 if s == 1 else 3

    def deep_row(depth, s):
        return 7 - depth if s == 1 else depth

    def deep_tile(far, a):
        return DEEP - far if a == 1 else far - 1

    def slot_of(k, a, s):
        free = [(2, 2), (3, 1), (3, 2)]
        if k < 3:
            return deep_tile(free[k][0], a), deep_row(free[k][1], s)
        return DEEP + 2, deep_row(k - 3, s)

    def halo_pair(v):
        return jnp.where(last, v, roll(v, -(HALF + 2), 1))

    def pick(pair, px):
        return roll(pair, -((px + DEEP) * block + DEEP - 1), 1)

    def zshift(v, s, col):
        lanes = lane if v.shape[0] == Y else elane
        return jnp.where(lanes == zend(s), col, roll(v, s, 1))

    def yshift(v, s, halo):
        return jnp.where(row == yend(s), jnp.broadcast_to(halo, v.shape), roll(v, s, 0))

    def pack(planes, s):
        acc = jnp.zeros((Y, Z), jnp.float32)
        for x in range(X):
            at = 1 + x
            acc = jnp.where(lane == at, roll(planes[x], at - (Z - 1 if s == 1 else 0), 1), acc)
        return acc

    def launch(messages, ssem, rsem):
        for src, dst, off in messages:
            pltpu.make_async_remote_copy(
                src_ref=src,
                dst_ref=dst,
                send_sem=ssem,
                recv_sem=rsem,
                device_id=place_of[off],
                device_id_type=MESH,
            ).start()

    def finish(messages, ssem, rsem):
        lines = sum(math.prod(src.shape[:-1]) for src, _, _ in messages)
        span = bulk.at[pl.ds(0, lines)]
        for sem in (rsem, ssem):
            pltpu.make_async_copy(span, span, sem).wait()

    def bundle(par):
        messages = []

        def beside(a, b, c):
            dst = fz.at[par, INDEX[c], TRAVEL[a]]
            rows = {1: pl.ds(Y - DEEP, DEEP), -1: pl.ds(0, DEEP), 0: pl.ds(0, Y)}[b]
            land = pl.ds({1: E - DEEP, -1: Y, 0: 0}[b], DEEP if b else Y)
            planes = pl.ds(0, 1 if a and b else 2)
            messages.append((sz.at[planes, rows, :], dst.at[planes, land, :], (a, b, c)))

        for c in zsides:
            for a, b in EDGES + [(0, 1), (0, -1)]:
                beside(a, b, c)
        for a, b in EDGES:
            bi, ai, rows = INDEX[b], INDEX[a], deep_rows(b)
            src, dst = sxy.at[bi, ai, :, rows, :], rxy.at[par, bi, ai, :, rows, :]
            messages.append((src, dst, (a, b, 0)))
        for s in SIGNS:
            si = INDEX[s]
            messages.append((sy.at[si], ry.at[par, si], (0, s, 0)))
        for c in zsides:
            for a in SIGNS:
                beside(a, 0, c)
        for s in SIGNS:
            messages.append((sx.at[INDEX[s]], rx.at[par, INDEX[s]], (s, 0, 0)))
        for c in zsides:
            beside(0, 0, c)
        return messages, sa.at[0], ra.at[par]

    def farewell():
        messages = []
        for s in SIGNS:
            messages.append((cy_.at[INDEX[s]], rcy.at[INDEX[s]], (0, s, 0)))
        for s in SIGNS:
            messages.append((cz_.at[INDEX[s]], rcz.at[INDEX[s]], (0, 0, s)))
        for s in SIGNS:
            messages.append((cx_.at[INDEX[s]], rcx.at[INDEX[s]], (s, 0, 0)))
        return messages, sc.at[0], rc.at[0]

    def moments(ps):
        def total(which):
            return functools.reduce(lambda a, b: a + b, [ps[i] for i in which])

        sums = [[total(CROSS[d][s]) for s in SIGNS] for d in range(3)]
        still = total([i for i in range(19) if DIRS[i][0] == 0])
        return still + sums[0][0] + sums[0][1], [up - down for up, down in sums]

    def chemical(o, beside):
        return quadratic * o + quartic * o * o * o - stiffness * (beside - 6.0 * o)

    def along(i, w):
        a = None
        for d in range(3):
            if DIRS[i][d]:
                t = w[d] if DIRS[i][d] == 1 else -w[d]
                a = t if a is None else a + t
        return a

    keep = 1.0 - 1.0 / relax_time
    mix = 1.0 / relax_time - 1.0

    def relax(x):
        ps = [pops[i, x] for i in range(19)]
        rho, u = mom[0, x], [mom[1 + d, x] for d in range(3)]
        flat = (mix * rho) * (1.0 - 1.5 * (u[0] * u[0] + u[1] * u[1] + u[2] * u[2]))
        out = [keep * ps[0] + WEIGHTS[0] * flat]
        for i in range(1, 19, 2):
            a = along(i, u)
            even = WEIGHTS[i] * flat + (4.5 * mix * WEIGHTS[i]) * rho * (a * a)
            odd = (3.0 * mix * WEIGHTS[i]) * rho * a
            out.append(keep * ps[i] + even + odd)
            out.append(keep * ps[i + 1] + even - odd)
        for i in range(19):
            post[i, x] = out[i]

    def place(acc, v, slot, x):
        at = slot * width + x * block
        mask = (lane >= at) & (lane < at + block)
        return jnp.where(mask, roll(v, at - (Z - DEEP), 1), acc)

    def ready():
        first = jnp.zeros((Y, Z), jnp.float32)
        second = jnp.zeros((Y, Z), jnp.float32)
        for x in range(X):
            heads, b = [mom[g, x] for g in range(MOMS)], base[x]
            u = heads[1:]
            out = [pops[i, x] for i in range(19)]
            for s in SIGNS:
                si = INDEX[s]
                y, at = ysrc(s), (0 if s == 1 else 4) + x
                for k, v in enumerate(heads + [out[i] for i in CROSS[1][s][:-1]]):
                    sy[si, k, at : at + 1, :] = v[y : y + 1, :]
                v, at = out[CROSS[1][s][-1]], spare(s)
                sy[si, x, at : at + 1, :] = v[y : y + 1, :]
                rows = slice(Y - DEEP, Y) if s == 1 else slice(0, DEEP)
                sy[si, 2 + x, deep_rows(s), :] = b[rows, :]
                if x == 0:
                    sy[si, 0, deep_rows(s), :] = u[0][rows, :]
                if x == X - 1:
                    sy[si, X + 2, deep_rows(s), :] = u[0][rows, :]
                for a in SIGNS:
                    ai, far = INDEX[a], X - x if a == 1 else x + 1
                    lines = {}
                    if far <= DEEP:
                        keep_rows = DEEP + 1 - far
                        lo = 8 - keep_rows if s == 1 else 0
                        part = slice(Y - keep_rows, Y) if s == 1 else slice(0, keep_rows)
                        at = deep_tile(far, a)
                        sxy[si, ai, at, lo : lo + keep_rows, :] = b[part, :]
                    if far == 1:
                        sxy[si, ai, DEEP, deep_rows(s), :] = u[0][rows, :]
                        lines = {0: heads[0], 1: u[1], 2: u[2], 3: out[DIRS.index((a, s, 0))]}
                    elif far <= DEEP:
                        lines = {2 + far: u[1]}
                    for k, v in lines.items():
                        at, r = slot_of(k, a, s)
                        sxy[si, ai, at, r : r + 1, :] = v[y : y + 1, :]
            for g, v in enumerate([b] + heads):
                first = place(first, v, g, x)
            for k, (up, down) in enumerate(ZPAIRS):
                second = place(second, jnp.where(low_col, out[down], out[up]), k, x)
        sz[0] = first
        sz[1] = second
        for s in SIGNS:
            si = INDEX[s]
            rows = slice(Y - DEEP, Y) if s == 1 else slice(0, DEEP)
            sy[si, 1, deep_rows(s), :] = first[rows, :]
            for ai in range(2):
                sxy[si, ai, DEEP + 1, deep_rows(s), :] = first[rows, :]

    def ready_planes():
        for s in SIGNS:
            si, edge = INDEX[s], xsrc(s)
            for g in range(MOMS):
                sx[si, g] = mom[g, edge]
            for k, i in enumerate(CROSS[0][s]):
                sx[si, MOMS + k] = pops[i, edge]
            for slot in range(DEEP):
                x = slot + (X - DEEP if s == 1 else 0)
                sx[si, MOMS + 5 + slot] = base[x]
                sx[si, MOMS + 6 + DEEP, slot : slot + 1, :] = mom[2, x, 0:1, :]
                sx[si, MOMS + 6 + DEEP, DEEP + slot : DEEP + slot + 1, :] = mom[2, x, Y - 1 :, :]
            sx[si, MOMS + 5 + DEEP] = sz[0]

    def send(par):
        messages, ssem, rsem = bundle(par)
        first = [m for m in messages if m[2][1]]
        launch(first, ssem, rsem)
        ready_planes()
        launch(messages[len(first) :], ssem, rsem)
        for x in range(X):
            relax(x)

    def forced(rho, inv, u, force):
        v = [u[d] + force[d] * inv for d in range(3)]
        flat = rho * (1.0 - 1.5 * (v[0] * v[0] + v[1] * v[1] + v[2] * v[2]))
        return v, flat

    def collide(rho, u, force):
        v, flat = forced(rho, 1.0 / rho, u, force)
        thin = mix * rho
        flat = flat + thin * (1.0 - 1.5 * (u[0] * u[0] + u[1] * u[1] + u[2] * u[2]))

        def hit(i, p, along_of):
            a, b = along_of(i, u), along_of(i, v)
            both = thin * (a * (3.0 + 4.5 * a)) + rho * (b * (3.0 + 4.5 * b))
            return keep * p + WEIGHTS[i] * (flat + both)

        return hit

    for ref in (sx, sy, sxy, cy_, oe, oz):
        ref[...] = jnp.zeros_like(ref)
    for load in loads:
        load.wait()

    for x in range(X):
        r = dens[x]
        u = [vel[d, x] for d in range(3)]
        usq = 1.0 - 1.5 * (u[0] * u[0] + u[1] * u[1] + u[2] * u[2])
        ps = []
        for i in range(19):
            a = along(i, u)
            if a is None:
                ps.append(WEIGHTS[i] * r * usq)
            else:
                ps.append(WEIGHTS[i] * r * (usq + 3.0 * a + 4.5 * a * a))
            pops[i, x] = ps[i]
        rho, moms = moments(ps)
        inv = 1.0 / rho
        mom[0, x] = rho
        for d in range(3):
            mom[1 + d, x] = moms[d] * inv
    ready()
    pl.semaphore_wait(barrier, len(partners))
    send(0)

    def step(n, carry):
        par = lax.rem(n, 2)
        finish(*bundle(par))
        low, high = ry.at[par, 0], ry.at[par, 1]

        def tall(a):
            if a == 0:
                near = extend(sz[0], low[1], high[1])
            else:
                mid, at = rx[par, INDEX[a], MOMS + 5 + DEEP], DEEP + 1
                near = extend(mid, rxy[par, 0, INDEX[a], at], rxy[par, 1, INDEX[a], at])
            far = [fz[par, INDEX[c], TRAVEL[a], 0] for c in zsides]
            halves = [jnp.where(facing, far[0], near), jnp.where(facing, near, far[-1])]
            return [roll(v, -a * width, 1) for v in halves]

        parts = [tall(a) for a in (0, 1, -1)]
        ends = [
            [roll(fz[par, INDEX[c], TRAVEL[a], 1], -a * width, 1) for a in (0, 1, -1)] for c in zsides
        ]

        def gather(three, slot, add):
            at = slot * width
            rel = lax.rem(elane + (Z - at), Z)
            v = jnp.where(rel < width, three[0], jnp.where(rel < HALF, three[2], three[1]))
            return roll(v, DEEP * block - at + add, 1)

        def packed(slot):
            halves = [gather([p[k] for p in parts], slot, HALF * k) for k in range(2)]
            return jnp.where(left, halves[0], halves[1])

        def packed_far(slot):
            halves = [gather(three, slot, HALF * k) for k, three in enumerate(ends)]
            if len(halves) == 1:
                halves.append(roll(halves[0], HALF, 1))
            return jnp.where(left, halves[0], halves[1])

        rho_z = packed(1)
        u_z = [packed(2 + d) for d in range(3)]
        old = oz[...]
        OZ = packed(0)
        for d, (shift, axis, mask) in enumerate(((block, 1, face_x), (1, 0, face_y), (1, 1, face_z))):
            t = 0.25 * (u_z[d] + roll(u_z[d], shift, axis)) * (old + roll(old, shift, axis))
            t = jnp.where(mask, t, 0.0)
            OZ = OZ + (t - roll(t, -shift, axis))
        oz[...] = OZ

        def around(px, s):
            if px < 0:
                return rxy[par, INDEX[s], 0, px + DEEP]
            if px >= X:
                return rxy[par, INDEX[s], 1, px - X]
            return ry[par, INDEX[s], 2 + px]

        def speed(px):
            if px < 0:
                tiles, mid = [rxy[par, k, 0, DEEP] for k in range(2)], rx[par, 0, 1]
            elif px >= X:
                tiles, mid = [rxy[par, k, 1, DEEP] for k in range(2)], rx[par, 1, 1]
            else:
                tiles, mid = [ry[par, k, 0 if px == 0 else X + 2] for k in range(2)], mom[1, px]
            return extend(mid, tiles[0], tiles[1])

        def line(k, a, s):
            at, r = slot_of(k, a, s)
            return rxy[par, INDEX[s], INDEX[a], at, r : r + 1, :]

        def outside(px, s):
            if px < 0:
                return line(1 if px == -1 else 2 - px, 1, s)
            if px >= X:
                return line(1 if px == X else 3 + px - X, -1, s)
            at = (0 if s == 1 else 4) + px
            return ry[par, INDEX[s], 2, at : at + 1, :]

        def inside(px, s):
            if 0 <= px < X:
                y = yend(s)
                return mom[2, px, y : y + 1, :]
            side, slot = (0, px + DEEP) if px < 0 else (1, px - X)
            at = slot if s == 1 else DEEP + slot
            return rx[par, side, MOMS + 6 + DEEP, at : at + 1, :]

        across = {}
        for lo, hi in ((-1, 0), (X - 1, X)):
            t = 0.25 * (speed(lo) + speed(hi)) * (oe[lo + DEEP] + oe[hi + DEEP])
            across[lo], across[hi] = -t, t
        beside = roll(OZ, 1, 0) + roll(OZ, -1, 0) + roll(OZ, 1, 1) + roll(OZ, -1, 1)
        beside = beside + roll(OZ, block, 1) + roll(OZ, -block, 1)
        CZ = chemical(OZ, beside)
        scale = -0.5 * OZ
        FZ = [
            scale * (roll(CZ, -block, 1) - roll(CZ, block, 1)),
            scale * (roll(CZ, -1, 0) - roll(CZ, 1, 0)),
            scale * (roll(CZ, -1, 1) - roll(CZ, 1, 1)),
        ]

        def sided(i, w):
            a = zsign * w[2]
            for d in range(2):
                if DIRS[i][d]:
                    a = a + w[d] if DIRS[i][d] == 1 else a - w[d]
            return a

        ZH = []
        hit = collide(rho_z, u_z, FZ)
        for k, (up, down) in enumerate(ZPAIRS):
            h = halo_pair(hit(up, packed_far(k), sided))
            ZH.append(roll(h, DIRS[up][1], 0)[own_rows, :])
        own_pair = jnp.where(column == DEEP, OZ, roll(OZ, -HALF, 1))
        order_pair, chem_pair = halo_pair(OZ), halo_pair(CZ)

        OE, C, F = {}, {}, {}

        def complete(px):
            if px < 0:
                mid = rx[par, 0, MOMS + 5 + px + DEEP]
            elif px >= X:
                mid = rx[par, 1, MOMS + 5 + px - X]
            else:
                mid = base[px]
            v = extend(mid, around(px, 1), around(px, -1))
            if px in across:
                v = v + across[px]
            t = {}
            for s in SIGNS:
                y, z = yend(s), next_row(s)
                pair = oe[px + DEEP, y : y + 1, :] + oe[px + DEEP, z : z + 1, :]
                line_t = 0.25 * (outside(px, s) + inside(px, s)) * pair
                t[s] = jnp.broadcast_to(line_t, (8, Z))
            halo = v[Y:, :] + jnp.where(sub == 0, t[-1], jnp.where(sub == 7, -t[1], 0.0))
            head = v[:8, :] + jnp.where(sub == 0, t[1], 0.0)
            tail = v[Y - 8 : Y, :] - jnp.where(sub == 7, t[-1], 0.0)
            rest = [v[8 : Y - 8, :]] if Y > 16 else []
            v = jnp.concatenate([head] + rest + [tail, halo], axis=0)
            col = roll(own_pair, -((px + DEEP) * block + DEEP), 1)
            OE[px] = jnp.where((elane == 0) | (elane == Z - 1), col, v)

        def potential(px):
            o, col = OE[px], pick(order_pair, px)
            beside = OE[px - 1] + OE[px + 1] + roll(o, 1, 0) + roll(o, -1, 0)
            C[px] = chemical(o, beside + zshift(o, 1, col) + zshift(o, -1, col))

        def push(px):
            c, col = C[px], pick(chem_pair, px)
            y_dn, y_up = roll(c, 1, 0), roll(c, -1, 0)
            z_dn, z_up = zshift(c, 1, col), zshift(c, -1, col)
            scale = -0.5 * OE[px]
            F[px] = [
                scale * (C[px + 1] - C[px - 1]),
                scale * (y_up - y_dn),
                scale * (z_up - z_dn),
            ]
            if 0 <= px < X:
                lap = C[px + 1] + C[px - 1] + y_up + y_dn + z_up + z_dn - 6.0 * c
                base[px] = (OE[px] + mobility * lap)[own_rows, :]
                for s in SIGNS:
                    at = (0 if s == 1 else 4) + px
                    y = next_row(s)
                    for d in range(3):
                        fy[INDEX[s], d, at : at + 1, :] = F[px][d][y : y + 1, :]

        XH, YH, LH = {}, {}, {}

        def strike(px):
            if 0 <= px < X:
                rho = mom[0, px]
                u = [mom[1 + d, px] for d in range(3)]
                v, flat = forced(rho, 1.0 / rho, u, [f[own_rows, :] for f in F[px]])
                post[0, px] = post[0, px] + WEIGHTS[0] * flat
                for i in range(1, 19, 2):
                    a = along(i, v)
                    even = WEIGHTS[i] * flat + (4.5 * WEIGHTS[i]) * rho * (a * a)
                    odd = (3.0 * WEIGHTS[i]) * rho * a
                    post[i, px] = post[i, px] + even + odd
                    post[i + 1, px] = post[i + 1, px] + even - odd
                return
            a = 1 if px < 0 else -1
            ai = INDEX[a]
            rho = rx[par, ai, 0]
            u = [rx[par, ai, 1 + d] for d in range(3)]
            hit = collide(rho, u, [f[own_rows, :] for f in F[px]])
            for k, i in enumerate(CROSS[0][a]):
                XH[i] = hit(i, rx[par, ai, MOMS + k], along)
            for s in SIGNS:
                i = DIRS.index((a, s, 0))
                r = deep_row(0, s)
                side = rxy[par, INDEX[s], ai, DEEP, r : r + 1, :]
                head = [line(0, a, s), side] + [line(k, a, s) for k in (1, 2, 3)]
                y = next_row(s)
                hit = collide(head[0], head[1:4], [f[y : y + 1, :] for f in F[px]])
                LH[i] = hit(i, head[4], along)

        for px in range(-DEEP, X + DEEP):
            complete(px)
            if px - 1 >= -2:
                potential(px - 1)
            if px - 2 >= -1:
                push(px - 2)
                strike(px - 2)
        for px in range(-DEEP, X + DEEP):
            oe[px + DEEP] = OE[px]
        O = [OE[x][own_rows, :] for x in range(X)]
        for s in SIGNS:
            si = INDEX[s]
            rho = ry[par, si, 0]
            u = [ry[par, si, 1 + d] for d in range(3)]
            hit = collide(rho, u, [fy[si, d] for d in range(3)])
            for x in range(X):
                at, r = (0 if s == 1 else 4) + x, spare(s)
                fp[si, at : at + 1, :] = ry[par, si, x, r : r + 1, :]
            for k, i in enumerate(CROSS[1][s]):
                p = ry[par, si, MOMS + k] if k < 4 else fp[si]
                YH[i] = hit(i, p, along)

        flows = {}
        pair_of = {i: k for k, both in enumerate(ZPAIRS) for i in both}
        for x in range(X):
            cols = [pick(ZH[k], x - DIRS[up][0]) for k, (up, _) in enumerate(ZPAIRS)]
            ps = []
            for i, (cx, cy, cz) in enumerate(DIRS):
                xs = x - cx
                own = 0 <= xs < X
                p = post[i, xs] if own else XH[i]
                if cy:
                    at = (0 if cy == 1 else 4) + xs
                    p = yshift(p, cy, YH[i][at : at + 1, :] if own else LH[i])
                if cz:
                    p = zshift(p, cz, cols[pair_of[i]])
                pops[i, x] = p
                ps.append(p)
            rho, moms = moments(ps)
            inv = 1.0 / rho
            flows[x] = [m * inv for m in moms]
            mom[0, x] = rho
            for d in range(3):
                mom[1 + d, x] = flows[x][d]

        @pl.when(n == ITERS - 1)
        def _():
            for s in SIGNS:
                cx_[INDEX[s]] = mom[1, xsrc(s)]
                y = ysrc(s)
                for x in range(X):
                    cy_[INDEX[s], 1 + x : 2 + x, :] = mom[2, x, y : y + 1, :]
                cz_[INDEX[s]] = pack([mom[3, x] for x in range(X)], s)
            launch(*farewell())

        tx = {0: 0.0, X: 0.0}
        for x in range(1, X):
            tx[x] = (flows[x][0] + flows[x - 1][0]) * (O[x] + O[x - 1])
        for x in range(X):
            f, o = flows[x], O[x]
            ty = jnp.where(row == 0, 0.0, (f[1] + roll(f[1], 1, 0)) * (o + roll(o, 1, 0)))
            tz = jnp.where(lane == 0, 0.0, (f[2] + roll(f[2], 1, 1)) * (o + roll(o, 1, 1)))
            change = tx[x + 1] - tx[x] + (roll(ty, -1, 0) - ty) + (roll(tz, -1, 1) - tz)
            base[x] = base[x] - 0.25 * change

        @pl.when(n < ITERS - 1)
        def _():
            ready()
            send(1 - par)

        return carry

    lax.fori_loop(0, ITERS, step, 0)
    finish(*farewell())

    pair = halo_pair(oz[...])[own_rows, :]
    for x in range(X):
        o, u = oe[x + DEEP, own_rows, :], [mom[1 + d, x] for d in range(3)]
        change = jnp.zeros((Y, Z), jnp.float32)
        if x == 0:
            change = change + (u[0] + rcx[0]) * (o + oe[DEEP - 1, own_rows, :])
        if x == X - 1:
            change = change - (u[0] + rcx[1]) * (o + oe[DEEP + X, own_rows, :])
        for s in SIGNS:
            at = next_row(s)
            other = rcy[INDEX[s], 1 + x : 2 + x, :]
            y = yend(s)
            t = (mom[2, x, y : y + 1, :] + other) * (
                oe[x + DEEP, at : at + 1, :] + oe[x + DEEP, y : y + 1, :]
            )
            t = jnp.where(row == y, jnp.broadcast_to(t, (Y, Z)), 0.0)
            side = pick(pair, x)
            beside = roll(rcz[INDEX[s]], zend(s) - (1 + x), 1)
            t = t + jnp.where(lane == zend(s), (u[2] + beside) * (o + side), 0.0)
            change = change + t if s == 1 else change - t
        order[x] = base[x] + 0.25 * change


def on_device(sizes, order_param, density, velocity):
    X, Y, Z = order_param.shape
    f32 = jnp.float32
    plane, rows, tall = (Y, Z), (8, Z), (Y + 8, Z)
    planes = MOMS + 5 + DEEP + 2
    lines = 2 * planes * Y + 2 * 8 * (MOMS + 4) + 4 * (DEEP + 3) * DEEP
    lines += (1 if sizes[2] == 2 else 2) * (6 * Y + 8 * DEEP)
    vmem = [
        (19, X, Y, Z), (MOMS, X, Y, Z), (X, Y, Z), (X + 2 * DEEP,) + tall, tall,
        (X, Y, Z), (3, X, Y, Z), (lines, Z),
        (2, planes) + plane, (2, 2, planes) + plane,
        (2, MOMS + 4) + rows, (2, 2, MOMS + 4) + rows,
        (2, 2, DEEP + 3) + rows, (2, 2, 2, DEEP + 3) + rows,
        (2,) + plane, (2, 2, 3, 2) + tall, (2, 3) + rows, (2,) + rows,
        (2,) + plane, (2,) + rows, (2,) + plane,
        (2,) + plane, (2,) + rows, (2,) + plane,
    ]
    sems = [(3,), (1,), (2,), (1,), (1,)]
    spec = pl.BlockSpec(memory_space=pltpu.VMEM)
    kept = pl.pallas_call(
        functools.partial(kernel, sizes),
        out_shape=(pltpu.VMEM((X, Y, Z), f32), pltpu.VMEM((19, X, Y, Z), f32)),
        in_specs=[pl.BlockSpec(memory_space=pl.ANY)] * 3,
        out_specs=(spec, spec),
        scratch_shapes=[pltpu.VMEM(s, f32) for s in vmem]
        + [pltpu.SemaphoreType.DMA(n) for n in sems],
        compiler_params=pltpu.CompilerParams(collective_id=0, has_side_effects=True),
    )(order_param, density, velocity)
    whole = pl.BlockSpec(memory_space=pl.ANY)
    return pl.pallas_call(
        write_out,
        out_shape=tuple(jax.ShapeDtypeStruct(v.shape, f32) for v in kept),
        in_specs=[whole] * 2,
        out_specs=(whole, whole),
        scratch_shapes=[pltpu.SemaphoreType.DMA((2,))],
        compiler_params=pltpu.CompilerParams(vmem_limit_bytes=1 << 20),
    )(*kept)


def write_out(order, pops, order_out, pops_out, sem):
    both = [
        pltpu.make_async_copy(pops, pops_out, sem.at[0]),
        pltpu.make_async_copy(order, order_out, sem.at[1]),
    ]
    for copy in both:
        copy.start()
    for copy in both:
        copy.wait()


def solution(mesh):
    sizes = tuple(mesh.shape[a] for a in AXES)
    return jax.shard_map(
        functools.partial(on_device, sizes),
        mesh=mesh,
        in_specs=(P("gx", "gy", "gz"), P("gx", "gy", "gz"), P(None, "gx", "gy", "gz")),
        out_specs=(P("gx", "gy", "gz"), P(None, "gx", "gy", "gz")),
        check_vma=False,
    )
```

```python
import functools
import math

import jax
import jax.numpy as jnp
from jax import lax
from jax.experimental import pallas as pl
from jax.experimental.pallas import tpu as pltpu
from jax.sharding import PartitionSpec as P

ITERS = 5
MESH = pl.DeviceIdType.MESH
AXES = ("gx", "gy", "gz")
DIRS = [
    (0, 0, 0),
    (1, 0, 0),
    (-1, 0, 0),
    (0, 1, 0),
    (0, -1, 0),
    (0, 0, 1),
    (0, 0, -1),
    (1, 1, 0),
    (-1, -1, 0),
    (1, -1, 0),
    (-1, 1, 0),
    (1, 0, 1),
    (-1, 0, -1),
    (1, 0, -1),
    (-1, 0, 1),
    (0, 1, 1),
    (0, -1, -1),
    (0, 1, -1),
    (0, -1, 1),
]
WEIGHTS = [1.0 / 3.0] + [1.0 / 18.0] * 6 + [1.0 / 36.0] * 12
quadratic = -0.1
quartic = 0.1
stiffness = 0.02
mobility = 0.5
relax_time = 0.8

SIGNS = (1, -1)
INDEX = {1: 0, -1: 1}
TRAVEL = {0: 0, 1: 1, -1: 2}
CROSS = [{s: [i for i in range(19) if DIRS[i][d] == s] for s in SIGNS} for d in range(3)]
EDGES = [(a, b) for a in SIGNS for b in SIGNS]
ZPAIRS = [
    (DIRS.index((a, b, 1)), DIRS.index((a, b, -1)))
    for a, b in ((0, 0), (1, 0), (-1, 0), (0, 1), (0, -1))
]
DEEP = 3
HALF = 64
MOMS = 4


def kernel(sizes, order_in, dens_in, vel_in, order, pops, *scratch):
    (post, mom, base, oe, oz, dens, vel, bulk) = scratch[0:8]
    (sx, rx, sy, ry, sxy, rxy, sz, fz, fy, fp) = scratch[8:18]
    (cx_, cy_, cz_, rcx, rcy, rcz) = scratch[18:24]
    (si_, sa, ra, sc, rc) = scratch[24:29]
    X, Y, Z = order.shape
    E = Y + 8
    own_rows = slice(0, Y)
    block = 2 * DEEP
    width = X * block
    me = [lax.axis_index(a) for a in AXES]
    tiles = Y // 8
    singles = (MOMS + 6 + DEEP) * tiles
    zsides = (1,) if sizes[2] == 2 else SIGNS

    def device(off):
        return {
            a: lax.rem(me[k] + (off[k] + sizes[k]), sizes[k]) if off[k] else me[k]
            for k, a in enumerate(AXES)
        }

    partners = [
        (a, b, c)
        for a in (1, -1, 0)
        for b in (1, -1, 0)
        for c in zsides + (0,)
        if (a, b, c) != (0, 0, 0)
    ]
    place_of = {off: device(off) for off in partners}
    if sizes[2] == 2:
        place_of[(0, 0, -1)] = place_of[(0, 0, 1)]
    barrier = pltpu.get_barrier_semaphore()
    for off in partners:
        pl.semaphore_signal(barrier, inc=1, device_id=place_of[off], device_id_type=MESH)
    loads = [
        pltpu.make_async_copy(src, dst, si_.at[k])
        for k, (src, dst) in enumerate(((order_in, base), (dens_in, dens), (vel_in, vel)))
    ]
    for load in loads:
        load.start()

    lane = lax.broadcasted_iota(jnp.int32, (Y, Z), 1)
    row = lax.broadcasted_iota(jnp.int32, (Y, Z), 0)
    elane = lax.broadcasted_iota(jnp.int32, (E, Z), 1)
    erow = lax.broadcasted_iota(jnp.int32, (E, Z), 0)
    left = elane < HALF
    frame = jnp.where(left, elane, elane - HALF)
    column = lax.rem(frame, block)
    facing = lax.rem(elane, block) < DEEP
    zsign = jnp.where(left, 1.0, -1.0)
    low_col = lane < HALF
    face_z = column == DEEP
    face_x = (frame // block == DEEP) | (frame // block == DEEP + X)
    face_y = (erow == 0) | (erow == Y)
    sub = lax.broadcasted_iota(jnp.int32, (8, Z), 0)
    last = column == DEEP - 1

    def extend(mid, low, high):
        return jnp.concatenate([mid, jnp.where(sub < 4, high, low)], axis=0)

    def roll(v, s, axis):
        s = s % v.shape[axis]
        return v if s == 0 else pltpu.roll(v, s, axis)

    def zend(s):
        return 0 if s == 1 else Z - 1

    def yend(s):
        return 0 if s == 1 else Y - 1

    def xsrc(s):
        return X - 1 if s == 1 else 0

    def ysrc(s):
        return Y - 1 if s == 1 else 0

    def next_row(s):
        return E - 1 if s == 1 else Y

    def deep_rows(s):
        return pl.ds(8 - DEEP if s == 1 else 0, DEEP)

    def flat_rows(s):
        return pl.ds(0 if s == 1 else 4, X)

    def spare(s):
        return 4 if s == 1 else 3

    def deep_row(depth, s):
        return 7 - depth if s == 1 else depth

    def deep_tile(far, a):
        return DEEP - far if a == 1 else far - 1

    def slot_of(k, a, s):
        free = [(2, 2), (3, 1), (3, 2)]
        if k < 3:
            return deep_tile(free[k][0], a), deep_row(free[k][1], s)
        return DEEP + 2, deep_row(k - 3, s)

    def halo_pair(v):
        return jnp.where(last, v, roll(v, -(HALF + 2), 1))

    def pick(pair, px):
        return roll(pair, -((px + DEEP) * block + DEEP - 1), 1)

    def zshift(v, s, col):
        lanes = lane if v.shape[0] == Y else elane
        return jnp.where(lanes == zend(s), col, roll(v, s, 1))

    def yshift(v, s, halo):
        return jnp.where(row == yend(s), jnp.broadcast_to(halo, v.shape), roll(v, s, 0))

    def pack(planes, s):
        acc = jnp.zeros((Y, Z), jnp.float32)
        for x in range(X):
            at = 1 + x
            acc = jnp.where(lane == at, roll(planes[x], at - (Z - 1 if s == 1 else 0), 1), acc)
        return acc

    def launch(messages, ssem, rsem):
        for src, dst, off in messages:
            pltpu.make_async_remote_copy(
                src_ref=src,
                dst_ref=dst,
                send_sem=ssem,
                recv_sem=rsem,
                device_id=place_of[off],
                device_id_type=MESH,
            ).start()

    def finish(messages, ssem, rsem):
        lines = sum(math.prod(src.shape[:-1]) for src, _, _ in messages)
        span = bulk.at[pl.ds(0, lines)]
        for sem in (rsem, ssem):
            pltpu.make_async_copy(span, span, sem).wait()

    def bundle(par):
        messages = []

        def beside(a, b, c):
            dst = fz.at[par, INDEX[c], TRAVEL[a]]
            rows = {1: pl.ds(Y - DEEP, DEEP), -1: pl.ds(0, DEEP), 0: pl.ds(0, Y)}[b]
            land = pl.ds({1: E - DEEP, -1: Y, 0: 0}[b], DEEP if b else Y)
            planes = pl.ds(0, 1 if a else 2)
            messages.append((sz.at[planes, rows, :], dst.at[planes, land, :], (a, b, c)))

        for c in zsides:
            for a, b in EDGES + [(0, 1), (0, -1)]:
                beside(a, b, c)
        for a, b in EDGES:
            bi, ai, rows = INDEX[b], INDEX[a], deep_rows(b)
            src, dst = sxy.at[bi, ai, :, rows, :], rxy.at[par, bi, ai, :, rows, :]
            messages.append((src, dst, (a, b, 0)))
        for s in SIGNS:
            si = INDEX[s]
            messages.append((sy.at[si], ry.at[par, si], (0, s, 0)))
        for c in zsides:
            for a in SIGNS:
                beside(a, 0, c)
        for s in SIGNS:
            messages.append((sx.at[INDEX[s]], rx.at[par, INDEX[s]], (s, 0, 0)))
        for c in zsides:
            beside(0, 0, c)
        return messages, sa.at[0], ra.at[par]

    def farewell():
        messages = []
        for s in SIGNS:
            messages.append((cy_.at[INDEX[s]], rcy.at[INDEX[s]], (0, s, 0)))
        for s in SIGNS:
            messages.append((cz_.at[INDEX[s]], rcz.at[INDEX[s]], (0, 0, s)))
        for s in SIGNS:
            messages.append((cx_.at[INDEX[s]], rcx.at[INDEX[s]], (s, 0, 0)))
        return messages, sc.at[0], rc.at[0]

    def moments(ps):
        def total(which):
            return functools.reduce(lambda a, b: a + b, [ps[i] for i in which])

        sums = [[total(CROSS[d][s]) for s in SIGNS] for d in range(3)]
        still = total([i for i in range(19) if DIRS[i][0] == 0])
        return still + sums[0][0] + sums[0][1], [up - down for up, down in sums]

    def chemical(o, beside):
        return quadratic * o + quartic * o * o * o - stiffness * (beside - 6.0 * o)

    def along(i, w):
        a = None
        for d in range(3):
            if DIRS[i][d]:
                t = w[d] if DIRS[i][d] == 1 else -w[d]
                a = t if a is None else a + t
        return a

    keep = 1.0 - 1.0 / relax_time
    mix = 1.0 / relax_time - 1.0

    def relax(x):
        ps = [pops[i, x] for i in range(19)]
        rho, u = mom[0, x], [mom[1 + d, x] for d in range(3)]
        flat = (mix * rho) * (1.0 - 1.5 * (u[0] * u[0] + u[1] * u[1] + u[2] * u[2]))
        out = [keep * ps[0] + WEIGHTS[0] * flat]
        for i in range(1, 19, 2):
            a = along(i, u)
            even = WEIGHTS[i] * flat + (4.5 * mix * WEIGHTS[i]) * rho * (a * a)
            odd = (3.0 * mix * WEIGHTS[i]) * rho * a
            out.append(keep * ps[i] + even + odd)
            out.append(keep * ps[i + 1] + even - odd)
        for i in range(19):
            post[i, x] = out[i]

    def place(acc, v, slot, x):
        at = slot * width + x * block
        mask = (lane >= at) & (lane < at + block)
        return jnp.where(mask, roll(v, at - (Z - DEEP), 1), acc)

    def ready():
        first = jnp.zeros((Y, Z), jnp.float32)
        second = jnp.zeros((Y, Z), jnp.float32)
        for x in range(X):
            heads, b = [mom[g, x] for g in range(MOMS)], base[x]
            u = heads[1:]
            out = [pops[i, x] for i in range(19)]
            for s in SIGNS:
                si = INDEX[s]
                y, at = ysrc(s), (0 if s == 1 else 4) + x
                for k, v in enumerate(heads + [out[i] for i in CROSS[1][s][:-1]]):
                    sy[si, k, at : at + 1, :] = v[y : y + 1, :]
                v, at = out[CROSS[1][s][-1]], spare(s)
                sy[si, x, at : at + 1, :] = v[y : y + 1, :]
                rows = slice(Y - DEEP, Y) if s == 1 else slice(0, DEEP)
                sy[si, 2 + x, deep_rows(s), :] = b[rows, :]
                if x == 0:
                    sy[si, 0, deep_rows(s), :] = u[0][rows, :]
                if x == X - 1:
                    sy[si, X + 2, deep_rows(s), :] = u[0][rows, :]
                for a in SIGNS:
                    ai, far = INDEX[a], X - x if a == 1 else x + 1
                    lines = {}
                    if far <= DEEP:
                        keep_rows = DEEP + 1 - far
                        lo = 8 - keep_rows if s == 1 else 0
                        part = slice(Y - keep_rows, Y) if s == 1 else slice(0, keep_rows)
                        at = deep_tile(far, a)
                        sxy[si, ai, at, lo : lo + keep_rows, :] = b[part, :]
                    if far == 1:
                        sxy[si, ai, DEEP, deep_rows(s), :] = u[0][rows, :]
                        lines = {0: heads[0], 1: u[1], 2: u[2], 3: out[DIRS.index((a, s, 0))]}
                    elif far <= DEEP:
                        lines = {2 + far: u[1]}
                    for k, v in lines.items():
                        at, r = slot_of(k, a, s)
                        sxy[si, ai, at, r : r + 1, :] = v[y : y + 1, :]
            for g, v in enumerate([b] + heads):
                first = place(first, v, g, x)
            for k, (up, down) in enumerate(ZPAIRS):
                second = place(second, jnp.where(low_col, out[down], out[up]), k, x)
        for a in SIGNS:
            up, down = ZPAIRS[TRAVEL[a]]
            v = jnp.where(low_col, pops[down, xsrc(a)], pops[up, xsrc(a)])
            at = 5 * width + 2 * INDEX[a]
            first = jnp.where((lane >= at) & (lane < at + 2), roll(v, at + 1, 1), first)
        sz[0] = first
        sz[1] = second
        for s in SIGNS:
            si = INDEX[s]
            rows = slice(Y - DEEP, Y) if s == 1 else slice(0, DEEP)
            sy[si, 1, deep_rows(s), :] = first[rows, :]
            for ai in range(2):
                sxy[si, ai, DEEP + 1, deep_rows(s), :] = first[rows, :]

    def ready_planes():
        for s in SIGNS:
            si, edge = INDEX[s], xsrc(s)

            def keep_plane(k, v):
                sx[si, k * tiles : (k + 1) * tiles] = v.reshape(tiles, 8, Z)

            for g in range(MOMS):
                keep_plane(g, mom[g, edge])
            for k, i in enumerate(CROSS[0][s]):
                keep_plane(MOMS + k, pops[i, edge])
            for slot in range(DEEP):
                x = slot + (X - DEEP if s == 1 else 0)
                keep_plane(MOMS + 5 + slot, base[x])
                sx[si, singles, slot : slot + 1, :] = mom[2, x, 0:1, :]
                sx[si, singles, DEEP + slot : DEEP + slot + 1, :] = mom[2, x, Y - 1 :, :]
            keep_plane(MOMS + 5 + DEEP, sz[0])

    def send(par):
        messages, ssem, rsem = bundle(par)
        first = [m for m in messages if m[2][1]]
        launch(first, ssem, rsem)
        ready_planes()
        launch(messages[len(first) :], ssem, rsem)
        for x in range(X):
            relax(x)

    def forced(rho, inv, u, force):
        v = [u[d] + force[d] * inv for d in range(3)]
        flat = rho * (1.0 - 1.5 * (v[0] * v[0] + v[1] * v[1] + v[2] * v[2]))
        return v, flat

    def collide(rho, u, force):
        v, flat = forced(rho, 1.0 / rho, u, force)
        thin = mix * rho
        flat = flat + thin * (1.0 - 1.5 * (u[0] * u[0] + u[1] * u[1] + u[2] * u[2]))

        def hit(i, p, along_of):
            a, b = along_of(i, u), along_of(i, v)
            both = thin * (a * (3.0 + 4.5 * a)) + rho * (b * (3.0 + 4.5 * b))
            return keep * p + WEIGHTS[i] * (flat + both)

        return hit

    for ref in (sx, sy, sxy, cy_, oe, oz):
        ref[...] = jnp.zeros_like(ref)
    for load in loads:
        load.wait()

    for x in range(X):
        r = dens[x]
        u = [vel[d, x] for d in range(3)]
        usq = 1.0 - 1.5 * (u[0] * u[0] + u[1] * u[1] + u[2] * u[2])
        ps = []
        for i in range(19):
            a = along(i, u)
            if a is None:
                ps.append(WEIGHTS[i] * r * usq)
            else:
                ps.append(WEIGHTS[i] * r * (usq + 3.0 * a + 4.5 * a * a))
            pops[i, x] = ps[i]
        rho, moms = moments(ps)
        inv = 1.0 / rho
        mom[0, x] = rho
        for d in range(3):
            mom[1 + d, x] = moms[d] * inv
    ready()
    pl.semaphore_wait(barrier, len(partners))
    send(0)

    def step(n, carry):
        par = lax.rem(n, 2)
        finish(*bundle(par))
        low, high = ry.at[par, 0], ry.at[par, 1]

        def came(si, k):
            return rx[par, si, k * tiles : (k + 1) * tiles].reshape(Y, Z)

        def tall(a):
            if a == 0:
                near = extend(sz[0], low[1], high[1])
            else:
                mid, at = came(INDEX[a], MOMS + 5 + DEEP), DEEP + 1
                near = extend(mid, rxy[par, 0, INDEX[a], at], rxy[par, 1, INDEX[a], at])
            far = [fz[par, INDEX[c], TRAVEL[a], 0] for c in zsides]
            halves = [jnp.where(facing, far[0], near), jnp.where(facing, near, far[-1])]
            return [roll(v, -a * width, 1) for v in halves]

        parts = [tall(a) for a in (0, 1, -1)]
        def gather(three, slot, add):
            at = slot * width
            rel = lax.rem(elane + (Z - at), Z)
            v = jnp.where(rel < width, three[0], jnp.where(rel < HALF, three[2], three[1]))
            return roll(v, DEEP * block - at + add, 1)

        def packed(slot):
            halves = [gather([p[k] for p in parts], slot, HALF * k) for k in range(2)]
            return jnp.where(left, halves[0], halves[1])

        def packed_far(slot):
            shift, halves = (DEEP - slot * X) * block, []
            for k, c in enumerate(SIGNS):
                far = fz[par, INDEX[c if c in zsides else 1], TRAVEL[0], 1]
                halves.append(roll(far, shift + HALF * k, 1))
            v = jnp.where(left, halves[0], halves[1])
            for a in SIGNS:
                if slot == TRAVEL[a]:
                    at = 5 * width + 2 * INDEX[a]
                    to = ((-1 if a == 1 else X) + DEEP) * block + DEEP - 1
                    for c, far, add in ((1, 0, 0), (-1, 1, HALF + 1)):
                        one = fz[par, INDEX[c if c in zsides else 1], TRAVEL[a], 0]
                        v = jnp.where(elane == to + add, roll(one, to + add - at - far, 1), v)
            return v

        rho_z = packed(1)
        u_z = [packed(2 + d) for d in range(3)]
        old = oz[...]
        OZ = packed(0)
        for d, (shift, axis, mask) in enumerate(((block, 1, face_x), (1, 0, face_y), (1, 1, face_z))):
            t = 0.25 * (u_z[d] + roll(u_z[d], shift, axis)) * (old + roll(old, shift, axis))
            t = jnp.where(mask, t, 0.0)
            OZ = OZ + (t - roll(t, -shift, axis))
        oz[...] = OZ

        def around(px, s):
            if px < 0:
                return rxy[par, INDEX[s], 0, px + DEEP]
            if px >= X:
                return rxy[par, INDEX[s], 1, px - X]
            return ry[par, INDEX[s], 2 + px]

        def speed(px):
            if px < 0:
                tiles, mid = [rxy[par, k, 0, DEEP] for k in range(2)], came(0, 1)
            elif px >= X:
                tiles, mid = [rxy[par, k, 1, DEEP] for k in range(2)], came(1, 1)
            else:
                tiles, mid = [ry[par, k, 0 if px == 0 else X + 2] for k in range(2)], mom[1, px]
            return extend(mid, tiles[0], tiles[1])

        def line(k, a, s):
            at, r = slot_of(k, a, s)
            return rxy[par, INDEX[s], INDEX[a], at, r : r + 1, :]

        def outside(px, s):
            if px < 0:
                return line(1 if px == -1 else 2 - px, 1, s)
            if px >= X:
                return line(1 if px == X else 3 + px - X, -1, s)
            at = (0 if s == 1 else 4) + px
            return ry[par, INDEX[s], 2, at : at + 1, :]

        def inside(px, s):
            if 0 <= px < X:
                y = yend(s)
                return mom[2, px, y : y + 1, :]
            side, slot = (0, px + DEEP) if px < 0 else (1, px - X)
            at = slot if s == 1 else DEEP + slot
            return rx[par, side, singles, at : at + 1, :]

        across = {}
        for lo, hi in ((-1, 0), (X - 1, X)):
            t = 0.25 * (speed(lo) + speed(hi)) * (oe[lo + DEEP] + oe[hi + DEEP])
            across[lo], across[hi] = -t, t
        beside = roll(OZ, 1, 0) + roll(OZ, -1, 0) + roll(OZ, 1, 1) + roll(OZ, -1, 1)
        beside = beside + roll(OZ, block, 1) + roll(OZ, -block, 1)
        CZ = chemical(OZ, beside)
        scale = -0.5 * OZ
        FZ = [
            scale * (roll(CZ, -block, 1) - roll(CZ, block, 1)),
            scale * (roll(CZ, -1, 0) - roll(CZ, 1, 0)),
            scale * (roll(CZ, -1, 1) - roll(CZ, 1, 1)),
        ]

        def sided(i, w):
            a = zsign * w[2]
            for d in range(2):
                if DIRS[i][d]:
                    a = a + w[d] if DIRS[i][d] == 1 else a - w[d]
            return a

        ZH = []
        hit = collide(rho_z, u_z, FZ)
        for k, (up, down) in enumerate(ZPAIRS):
            h = halo_pair(hit(up, packed_far(k), sided))
            ZH.append(roll(h, DIRS[up][1], 0)[own_rows, :])
        own_pair = jnp.where(column == DEEP, OZ, roll(OZ, -HALF, 1))
        order_pair, chem_pair = halo_pair(OZ), halo_pair(CZ)

        OE, C, F = {}, {}, {}

        def complete(px):
            if px < 0:
                mid = came(0, MOMS + 5 + px + DEEP)
            elif px >= X:
                mid = came(1, MOMS + 5 + px - X)
            else:
                mid = base[px]
            v = extend(mid, around(px, 1), around(px, -1))
            if px in across:
                v = v + across[px]
            t = {}
            for s in SIGNS:
                y, z = yend(s), next_row(s)
                pair = oe[px + DEEP, y : y + 1, :] + oe[px + DEEP, z : z + 1, :]
                line_t = 0.25 * (outside(px, s) + inside(px, s)) * pair
                t[s] = jnp.broadcast_to(line_t, (8, Z))
            halo = v[Y:, :] + jnp.where(sub == 0, t[-1], jnp.where(sub == 7, -t[1], 0.0))
            head = v[:8, :] + jnp.where(sub == 0, t[1], 0.0)
            tail = v[Y - 8 : Y, :] - jnp.where(sub == 7, t[-1], 0.0)
            rest = [v[8 : Y - 8, :]] if Y > 16 else []
            v = jnp.concatenate([head] + rest + [tail, halo], axis=0)
            col = roll(own_pair, -((px + DEEP) * block + DEEP), 1)
            OE[px] = jnp.where((elane == 0) | (elane == Z - 1), col, v)

        def potential(px):
            o, col = OE[px], pick(order_pair, px)
            beside = OE[px - 1] + OE[px + 1] + roll(o, 1, 0) + roll(o, -1, 0)
            C[px] = chemical(o, beside + zshift(o, 1, col) + zshift(o, -1, col))

        def push(px):
            c, col = C[px], pick(chem_pair, px)
            y_dn, y_up = roll(c, 1, 0), roll(c, -1, 0)
            z_dn, z_up = zshift(c, 1, col), zshift(c, -1, col)
            scale = -0.5 * OE[px]
            F[px] = [
                scale * (C[px + 1] - C[px - 1]),
                scale * (y_up - y_dn),
                scale * (z_up - z_dn),
            ]
            if 0 <= px < X:
                lap = C[px + 1] + C[px - 1] + y_up + y_dn + z_up + z_dn - 6.0 * c
                base[px] = (OE[px] + mobility * lap)[own_rows, :]
                for s in SIGNS:
                    at = (0 if s == 1 else 4) + px
                    y = next_row(s)
                    for d in range(3):
                        fy[INDEX[s], d, at : at + 1, :] = F[px][d][y : y + 1, :]

        XH, YH, LH = {}, {}, {}

        def strike(px):
            if 0 <= px < X:
                rho = mom[0, px]
                u = [mom[1 + d, px] for d in range(3)]
                v, flat = forced(rho, 1.0 / rho, u, [f[own_rows, :] for f in F[px]])
                post[0, px] = post[0, px] + WEIGHTS[0] * flat
                for i in range(1, 19, 2):
                    a = along(i, v)
                    even = WEIGHTS[i] * flat + (4.5 * WEIGHTS[i]) * rho * (a * a)
                    odd = (3.0 * WEIGHTS[i]) * rho * a
                    post[i, px] = post[i, px] + even + odd
                    post[i + 1, px] = post[i + 1, px] + even - odd
                return
            a = 1 if px < 0 else -1
            ai = INDEX[a]
            rho = came(ai, 0)
            u = [came(ai, 1 + d) for d in range(3)]
            hit = collide(rho, u, [f[own_rows, :] for f in F[px]])
            for k, i in enumerate(CROSS[0][a]):
                XH[i] = hit(i, came(ai, MOMS + k), along)
            for s in SIGNS:
                i = DIRS.index((a, s, 0))
                r = deep_row(0, s)
                side = rxy[par, INDEX[s], ai, DEEP, r : r + 1, :]
                head = [line(0, a, s), side] + [line(k, a, s) for k in (1, 2, 3)]
                y = next_row(s)
                hit = collide(head[0], head[1:4], [f[y : y + 1, :] for f in F[px]])
                LH[i] = hit(i, head[4], along)

        for px in range(-DEEP, X + DEEP):
            complete(px)
            if px - 1 >= -2:
                potential(px - 1)
            if px - 2 >= -1:
                push(px - 2)
                strike(px - 2)
        for px in range(-DEEP, X + DEEP):
            oe[px + DEEP] = OE[px]
        O = [OE[x][own_rows, :] for x in range(X)]
        for s in SIGNS:
            si = INDEX[s]
            rho = ry[par, si, 0]
            u = [ry[par, si, 1 + d] for d in range(3)]
            hit = collide(rho, u, [fy[si, d] for d in range(3)])
            for x in range(X):
                at, r = (0 if s == 1 else 4) + x, spare(s)
                fp[si, at : at + 1, :] = ry[par, si, x, r : r + 1, :]
            for k, i in enumerate(CROSS[1][s]):
                p = ry[par, si, MOMS + k] if k < 4 else fp[si]
                YH[i] = hit(i, p, along)

        flows = {}
        pair_of = {i: k for k, both in enumerate(ZPAIRS) for i in both}
        for x in range(X):
            cols = [pick(ZH[k], x - DIRS[up][0]) for k, (up, _) in enumerate(ZPAIRS)]
            ps = []
            for i, (cx, cy, cz) in enumerate(DIRS):
                xs = x - cx
                own = 0 <= xs < X
                p = post[i, xs] if own else XH[i]
                if cy:
                    at = (0 if cy == 1 else 4) + xs
                    p = yshift(p, cy, YH[i][at : at + 1, :] if own else LH[i])
                if cz:
                    p = zshift(p, cz, cols[pair_of[i]])
                pops[i, x] = p
                ps.append(p)
            rho, moms = moments(ps)
            inv = 1.0 / rho
            flows[x] = [m * inv for m in moms]
            mom[0, x] = rho
            for d in range(3):
                mom[1 + d, x] = flows[x][d]

        @pl.when(n == ITERS - 1)
        def _():
            for s in SIGNS:
                cx_[INDEX[s]] = mom[1, xsrc(s)]
                y = ysrc(s)
                for x in range(X):
                    cy_[INDEX[s], 1 + x : 2 + x, :] = mom[2, x, y : y + 1, :]
                cz_[INDEX[s]] = pack([mom[3, x] for x in range(X)], s)
            launch(*farewell())

        tx = {0: 0.0, X: 0.0}
        for x in range(1, X):
            tx[x] = (flows[x][0] + flows[x - 1][0]) * (O[x] + O[x - 1])
        for x in range(X):
            f, o = flows[x], O[x]
            ty = jnp.where(row == 0, 0.0, (f[1] + roll(f[1], 1, 0)) * (o + roll(o, 1, 0)))
            tz = jnp.where(lane == 0, 0.0, (f[2] + roll(f[2], 1, 1)) * (o + roll(o, 1, 1)))
            change = tx[x + 1] - tx[x] + (roll(ty, -1, 0) - ty) + (roll(tz, -1, 1) - tz)
            base[x] = base[x] - 0.25 * change

        @pl.when(n < ITERS - 1)
        def _():
            ready()
            send(1 - par)

        return carry

    lax.fori_loop(0, ITERS, step, 0)
    finish(*farewell())

    pair = halo_pair(oz[...])[own_rows, :]
    for x in range(X):
        o, u = oe[x + DEEP, own_rows, :], [mom[1 + d, x] for d in range(3)]
        change = jnp.zeros((Y, Z), jnp.float32)
        if x == 0:
            change = change + (u[0] + rcx[0]) * (o + oe[DEEP - 1, own_rows, :])
        if x == X - 1:
            change = change - (u[0] + rcx[1]) * (o + oe[DEEP + X, own_rows, :])
        for s in SIGNS:
            at = next_row(s)
            other = rcy[INDEX[s], 1 + x : 2 + x, :]
            y = yend(s)
            t = (mom[2, x, y : y + 1, :] + other) * (
                oe[x + DEEP, at : at + 1, :] + oe[x + DEEP, y : y + 1, :]
            )
            t = jnp.where(row == y, jnp.broadcast_to(t, (Y, Z)), 0.0)
            side = pick(pair, x)
            beside = roll(rcz[INDEX[s]], zend(s) - (1 + x), 1)
            t = t + jnp.where(lane == zend(s), (u[2] + beside) * (o + side), 0.0)
            change = change + t if s == 1 else change - t
        order[x] = base[x] + 0.25 * change


def on_device(sizes, order_param, density, velocity):
    X, Y, Z = order_param.shape
    f32 = jnp.float32
    plane, rows, tall = (Y, Z), (8, Z), (Y + 8, Z)
    stack = (MOMS + 5 + DEEP + 1) * (Y // 8) + 1
    lines = 2 * 8 * stack + 2 * 8 * (MOMS + 4) + 4 * (DEEP + 3) * DEEP
    lines += (1 if sizes[2] == 2 else 2) * (4 * Y + 8 * DEEP)
    vmem = [
        (19, X, Y, Z), (MOMS, X, Y, Z), (X, Y, Z), (X + 2 * DEEP,) + tall, tall,
        (X, Y, Z), (3, X, Y, Z), (lines, Z),
        (2, stack) + rows, (2, 2, stack) + rows,
        (2, MOMS + 4) + rows, (2, 2, MOMS + 4) + rows,
        (2, 2, DEEP + 3) + rows, (2, 2, 2, DEEP + 3) + rows,
        (2,) + plane, (2, 2, 3, 2) + tall, (2, 3) + rows, (2,) + rows,
        (2,) + plane, (2,) + rows, (2,) + plane,
        (2,) + plane, (2,) + rows, (2,) + plane,
    ]
    sems = [(3,), (1,), (2,), (1,), (1,)]
    spec = pl.BlockSpec(memory_space=pltpu.VMEM)
    kept = pl.pallas_call(
        functools.partial(kernel, sizes),
        out_shape=(pltpu.VMEM((X, Y, Z), f32), pltpu.VMEM((19, X, Y, Z), f32)),
        in_specs=[pl.BlockSpec(memory_space=pl.ANY)] * 3,
        out_specs=(spec, spec),
        scratch_shapes=[pltpu.VMEM(s, f32) for s in vmem]
        + [pltpu.SemaphoreType.DMA(n) for n in sems],
        compiler_params=pltpu.CompilerParams(collective_id=0, has_side_effects=True),
    )(order_param, density, velocity)
    whole = pl.BlockSpec(memory_space=pl.ANY)
    return pl.pallas_call(
        write_out,
        out_shape=tuple(jax.ShapeDtypeStruct(v.shape, f32) for v in kept),
        in_specs=[whole] * 2,
        out_specs=(whole, whole),
        scratch_shapes=[pltpu.SemaphoreType.DMA((2,))],
        compiler_params=pltpu.CompilerParams(vmem_limit_bytes=1 << 20),
    )(*kept)


def write_out(order, pops, order_out, pops_out, sem):
    both = [
        pltpu.make_async_copy(pops, pops_out, sem.at[0]),
        pltpu.make_async_copy(order, order_out, sem.at[1]),
    ]
    for copy in both:
        copy.start()
    for copy in both:
        copy.wait()


def solution(mesh):
    sizes = tuple(mesh.shape[a] for a in AXES)
    return jax.shard_map(
        functools.partial(on_device, sizes),
        mesh=mesh,
        in_specs=(P("gx", "gy", "gz"), P("gx", "gy", "gz"), P(None, "gx", "gy", "gz")),
        out_specs=(P("gx", "gy", "gz"), P(None, "gx", "gy", "gz")),
        check_vma=False,
    )
```

```python
import functools
import math

import jax
import jax.numpy as jnp
from jax import lax
from jax.experimental import pallas as pl
from jax.experimental.pallas import tpu as pltpu
from jax.sharding import PartitionSpec as P

ITERS = 5
MESH = pl.DeviceIdType.MESH
AXES = ("gx", "gy", "gz")
DIRS = [
    (0, 0, 0),
    (1, 0, 0),
    (-1, 0, 0),
    (0, 1, 0),
    (0, -1, 0),
    (0, 0, 1),
    (0, 0, -1),
    (1, 1, 0),
    (-1, -1, 0),
    (1, -1, 0),
    (-1, 1, 0),
    (1, 0, 1),
    (-1, 0, -1),
    (1, 0, -1),
    (-1, 0, 1),
    (0, 1, 1),
    (0, -1, -1),
    (0, 1, -1),
    (0, -1, 1),
]
WEIGHTS = [1.0 / 3.0] + [1.0 / 18.0] * 6 + [1.0 / 36.0] * 12
quadratic = -0.1
quartic = 0.1
stiffness = 0.02
mobility = 0.5
relax_time = 0.8

SIGNS = (1, -1)
INDEX = {1: 0, -1: 1}
TRAVEL = {0: 0, 1: 1, -1: 2}
CROSS = [{s: [i for i in range(19) if DIRS[i][d] == s] for s in SIGNS} for d in range(3)]
EDGES = [(a, b) for a in SIGNS for b in SIGNS]
ZPAIRS = [
    (DIRS.index((a, b, 1)), DIRS.index((a, b, -1)))
    for a, b in ((0, 0), (1, 0), (-1, 0), (0, 1), (0, -1))
]
DEEP = 3
HALF = 64
MOMS = 4


def kernel(sizes, order_in, dens_in, vel_in, order, pops, *scratch):
    (post, mom, base, oe, oz, dens, vel, bulk) = scratch[0:8]
    (sx, rx, sy, ry, sxy, rxy, sz, fz, fy, fp) = scratch[8:18]
    (cx_, cy_, cz_, rcx, rcy, rcz) = scratch[18:24]
    (si_, sa, ra, sc, rc) = scratch[24:29]
    X, Y, Z = order.shape
    E = Y + 8
    own_rows = slice(0, Y)
    block = 2 * DEEP
    width = X * block
    me = [lax.axis_index(a) for a in AXES]
    tiles = Y // 8
    singles = (MOMS + 6 + DEEP) * tiles
    zsides = (1,) if sizes[2] == 2 else SIGNS

    def device(off):
        return {
            a: lax.rem(me[k] + (off[k] + sizes[k]), sizes[k]) if off[k] else me[k]
            for k, a in enumerate(AXES)
        }

    partners = [
        (a, b, c)
        for a in (1, -1, 0)
        for b in (1, -1, 0)
        for c in zsides + (0,)
        if (a, b, c) != (0, 0, 0)
    ]
    place_of = {off: device(off) for off in partners}
    if sizes[2] == 2:
        place_of[(0, 0, -1)] = place_of[(0, 0, 1)]
    barrier = pltpu.get_barrier_semaphore()
    for off in partners:
        pl.semaphore_signal(barrier, inc=1, device_id=place_of[off], device_id_type=MESH)
    loads = [
        pltpu.make_async_copy(src, dst, si_.at[k])
        for k, (src, dst) in enumerate(((order_in, base), (dens_in, dens), (vel_in, vel)))
    ]
    for load in loads:
        load.start()

    lane = lax.broadcasted_iota(jnp.int32, (Y, Z), 1)
    row = lax.broadcasted_iota(jnp.int32, (Y, Z), 0)
    elane = lax.broadcasted_iota(jnp.int32, (E, Z), 1)
    erow = lax.broadcasted_iota(jnp.int32, (E, Z), 0)
    left = elane < HALF
    frame = jnp.where(left, elane, elane - HALF)
    column = lax.rem(frame, block)
    facing = lax.rem(elane, block) < DEEP
    zsign = jnp.where(left, 1.0, -1.0)
    low_col = lane < HALF
    face_z = column == DEEP
    face_x = (frame // block == DEEP) | (frame // block == DEEP + X)
    face_y = (erow == 0) | (erow == Y)
    sub = lax.broadcasted_iota(jnp.int32, (8, Z), 0)
    last = column == DEEP - 1

    def extend(mid, low, high):
        return jnp.concatenate([mid, jnp.where(sub < 4, high, low)], axis=0)

    def roll(v, s, axis):
        s = s % v.shape[axis]
        return v if s == 0 else pltpu.roll(v, s, axis)

    def zend(s):
        return 0 if s == 1 else Z - 1

    def yend(s):
        return 0 if s == 1 else Y - 1

    def xsrc(s):
        return X - 1 if s == 1 else 0

    def ysrc(s):
        return Y - 1 if s == 1 else 0

    def next_row(s):
        return E - 1 if s == 1 else Y

    def deep_rows(s):
        return pl.ds(8 - DEEP if s == 1 else 0, DEEP)

    def flat_rows(s):
        return pl.ds(0 if s == 1 else 4, X)

    def spare(s):
        return 4 if s == 1 else 3

    def deep_row(depth, s):
        return 7 - depth if s == 1 else depth

    def deep_tile(far, a):
        return DEEP - far if a == 1 else far - 1

    def slot_of(k, a, s):
        free = [(2, 2), (3, 1), (3, 2)]
        if k < 3:
            return deep_tile(free[k][0], a), deep_row(free[k][1], s)
        return DEEP + 2, deep_row(k - 3, s)

    def halo_pair(v):
        return jnp.where(last, v, roll(v, -(HALF + 2), 1))

    def pick(pair, px):
        return roll(pair, -((px + DEEP) * block + DEEP - 1), 1)

    def zshift(v, s, col):
        lanes = lane if v.shape[0] == Y else elane
        return jnp.where(lanes == zend(s), col, roll(v, s, 1))

    def yshift(v, s, halo):
        return jnp.where(row == yend(s), jnp.broadcast_to(halo, v.shape), roll(v, s, 0))

    def pack(planes, s):
        acc = jnp.zeros((Y, Z), jnp.float32)
        for x in range(X):
            at = 1 + x
            acc = jnp.where(lane == at, roll(planes[x], at - (Z - 1 if s == 1 else 0), 1), acc)
        return acc

    def launch(messages, ssem, rsem):
        for src, dst, off in messages:
            pltpu.make_async_remote_copy(
                src_ref=src,
                dst_ref=dst,
                send_sem=ssem,
                recv_sem=rsem,
                device_id=place_of[off],
                device_id_type=MESH,
            ).start()

    def finish(messages, ssem, rsem):
        lines = sum(math.prod(src.shape[:-1]) for src, _, _ in messages)
        span = bulk.at[pl.ds(0, lines)]
        for sem in (rsem, ssem):
            pltpu.make_async_copy(span, span, sem).wait()

    def bundle(par):
        messages = []

        def beside(a, b, c):
            dst = fz.at[par, INDEX[c], TRAVEL[a]]
            rows = {1: pl.ds(Y - DEEP, DEEP), -1: pl.ds(0, DEEP), 0: pl.ds(0, Y)}[b]
            land = pl.ds({1: E - DEEP, -1: Y, 0: 0}[b], DEEP if b else Y)
            planes = pl.ds(0, 1 if a else 2)
            messages.append((sz.at[planes, rows, :], dst.at[planes, land, :], (a, b, c)))

        for c in zsides:
            for a, b in EDGES + [(0, 1), (0, -1)]:
                beside(a, b, c)
        for a, b in EDGES:
            bi, ai, rows = INDEX[b], INDEX[a], deep_rows(b)
            src, dst = sxy.at[bi, ai, :, rows, :], rxy.at[par, bi, ai, :, rows, :]
            messages.append((src, dst, (a, b, 0)))
        for s in SIGNS:
            si = INDEX[s]
            messages.append((sy.at[si], ry.at[par, si], (0, s, 0)))
        for c in zsides:
            for a in SIGNS:
                beside(a, 0, c)
        for s in SIGNS:
            messages.append((sx.at[INDEX[s]], rx.at[par, INDEX[s]], (s, 0, 0)))
        for c in zsides:
            beside(0, 0, c)
        return messages, sa.at[0], ra.at[par]

    def farewell():
        messages = []
        for s in SIGNS:
            messages.append((cy_.at[INDEX[s]], rcy.at[INDEX[s]], (0, s, 0)))
        for s in SIGNS:
            messages.append((cz_.at[INDEX[s]], rcz.at[INDEX[s]], (0, 0, s)))
        for s in SIGNS:
            messages.append((cx_.at[INDEX[s]], rcx.at[INDEX[s]], (s, 0, 0)))
        return messages, sc.at[0], rc.at[0]

    def moments(ps):
        def total(which):
            return functools.reduce(lambda a, b: a + b, [ps[i] for i in which])

        sums = [[total(CROSS[d][s]) for s in SIGNS] for d in range(3)]
        still = total([i for i in range(19) if DIRS[i][0] == 0])
        return still + sums[0][0] + sums[0][1], [up - down for up, down in sums]

    def chemical(o, beside):
        return quadratic * o + quartic * o * o * o - stiffness * (beside - 6.0 * o)

    def along(i, w):
        a = None
        for d in range(3):
            if DIRS[i][d]:
                t = w[d] if DIRS[i][d] == 1 else -w[d]
                a = t if a is None else a + t
        return a

    keep = 1.0 - 1.0 / relax_time
    mix = 1.0 / relax_time - 1.0

    def relax(x):
        ps = [pops[i, x] for i in range(19)]
        rho, u = mom[0, x], [mom[1 + d, x] for d in range(3)]
        flat = (mix * rho) * (1.0 - 1.5 * (u[0] * u[0] + u[1] * u[1] + u[2] * u[2]))
        out = [keep * ps[0] + WEIGHTS[0] * flat]
        for i in range(1, 19, 2):
            a = along(i, u)
            even = WEIGHTS[i] * flat + (4.5 * mix * WEIGHTS[i]) * rho * (a * a)
            odd = (3.0 * mix * WEIGHTS[i]) * rho * a
            out.append(keep * ps[i] + even + odd)
            out.append(keep * ps[i + 1] + even - odd)
        for i in range(19):
            post[i, x] = out[i]

    def place(acc, v, slot, x):
        at = slot * width + x * block
        mask = (lane >= at) & (lane < at + block)
        return jnp.where(mask, roll(v, at - (Z - DEEP), 1), acc)

    def ready():
        first = jnp.zeros((Y, Z), jnp.float32)
        second = jnp.zeros((Y, Z), jnp.float32)
        for x in range(X):
            heads, b = [mom[g, x] for g in range(MOMS)], base[x]
            u = heads[1:]
            out = [pops[i, x] for i in range(19)]
            for s in SIGNS:
                si = INDEX[s]
                y, at = ysrc(s), (0 if s == 1 else 4) + x
                for k, v in enumerate(heads + [out[i] for i in CROSS[1][s][:-1]]):
                    sy[si, k, at : at + 1, :] = v[y : y + 1, :]
                v, at = out[CROSS[1][s][-1]], spare(s)
                sy[si, x, at : at + 1, :] = v[y : y + 1, :]
                rows = slice(Y - DEEP, Y) if s == 1 else slice(0, DEEP)
                sy[si, 2 + x, deep_rows(s), :] = b[rows, :]
                if x == 0:
                    sy[si, 0, deep_rows(s), :] = u[0][rows, :]
                if x == X - 1:
                    sy[si, X + 2, deep_rows(s), :] = u[0][rows, :]
                for a in SIGNS:
                    ai, far = INDEX[a], X - x if a == 1 else x + 1
                    lines = {}
                    if far <= DEEP:
                        keep_rows = DEEP + 1 - far
                        lo = 8 - keep_rows if s == 1 else 0
                        part = slice(Y - keep_rows, Y) if s == 1 else slice(0, keep_rows)
                        at = deep_tile(far, a)
                        sxy[si, ai, at, lo : lo + keep_rows, :] = b[part, :]
                    if far == 1:
                        sxy[si, ai, DEEP, deep_rows(s), :] = u[0][rows, :]
                        lines = {0: heads[0], 1: u[1], 2: u[2], 3: out[DIRS.index((a, s, 0))]}
                    elif far <= DEEP:
                        lines = {2 + far: u[1]}
                    for k, v in lines.items():
                        at, r = slot_of(k, a, s)
                        sxy[si, ai, at, r : r + 1, :] = v[y : y + 1, :]
            for g, v in enumerate([b] + heads):
                first = place(first, v, g, x)
            for k, (up, down) in enumerate(ZPAIRS):
                second = place(second, jnp.where(low_col, out[down], out[up]), k, x)
        for a in SIGNS:
            up, down = ZPAIRS[TRAVEL[a]]
            v = jnp.where(low_col, pops[down, xsrc(a)], pops[up, xsrc(a)])
            at = 5 * width + 2 * INDEX[a]
            first = jnp.where((lane >= at) & (lane < at + 2), roll(v, at + 1, 1), first)
        sz[0] = first
        sz[1] = second
        for s in SIGNS:
            si = INDEX[s]
            rows = slice(Y - DEEP, Y) if s == 1 else slice(0, DEEP)
            sy[si, 1, deep_rows(s), :] = first[rows, :]
            for ai in range(2):
                sxy[si, ai, DEEP + 1, deep_rows(s), :] = first[rows, :]

    def ready_planes():
        for s in SIGNS:
            si, edge = INDEX[s], xsrc(s)

            def keep_plane(k, v):
                sx[si, k * tiles : (k + 1) * tiles] = v.reshape(tiles, 8, Z)

            for g in range(MOMS):
                keep_plane(g, mom[g, edge])
            for k, i in enumerate(CROSS[0][s]):
                keep_plane(MOMS + k, pops[i, edge])
            for slot in range(DEEP):
                x = slot + (X - DEEP if s == 1 else 0)
                keep_plane(MOMS + 5 + slot, base[x])
                sx[si, singles, slot : slot + 1, :] = mom[2, x, 0:1, :]
                sx[si, singles, DEEP + slot : DEEP + slot + 1, :] = mom[2, x, Y - 1 :, :]
            keep_plane(MOMS + 5 + DEEP, sz[0])

    def send(par):
        messages, ssem, rsem = bundle(par)
        first = [m for m in messages if m[2][1]]
        launch(first, ssem, rsem)
        ready_planes()
        launch(messages[len(first) :], ssem, rsem)
        for x in range(X):
            relax(x)

    def forced(rho, inv, u, force):
        v = [u[d] + force[d] * inv for d in range(3)]
        flat = rho * (1.0 - 1.5 * (v[0] * v[0] + v[1] * v[1] + v[2] * v[2]))
        return v, flat

    def collide(rho, u, force):
        v, flat = forced(rho, 1.0 / rho, u, force)
        thin = mix * rho
        flat = flat + thin * (1.0 - 1.5 * (u[0] * u[0] + u[1] * u[1] + u[2] * u[2]))

        def hit(i, p, along_of):
            a, b = along_of(i, u), along_of(i, v)
            both = thin * (a * (3.0 + 4.5 * a)) + rho * (b * (3.0 + 4.5 * b))
            return keep * p + WEIGHTS[i] * (flat + both)

        return hit

    for ref in (sx, sy, sxy, cy_, oe, oz):
        ref[...] = jnp.zeros_like(ref)
    for load in loads:
        load.wait()

    for x in range(X):
        r = dens[x]
        u = [vel[d, x] for d in range(3)]
        usq = 1.0 - 1.5 * (u[0] * u[0] + u[1] * u[1] + u[2] * u[2])
        ps = []
        for i in range(19):
            a = along(i, u)
            if a is None:
                ps.append(WEIGHTS[i] * r * usq)
            else:
                ps.append(WEIGHTS[i] * r * (usq + 3.0 * a + 4.5 * a * a))
            pops[i, x] = ps[i]
        rho, moms = moments(ps)
        inv = 1.0 / rho
        mom[0, x] = rho
        for d in range(3):
            mom[1 + d, x] = moms[d] * inv
    ready()
    pl.semaphore_wait(barrier, len(partners))
    send(0)

    def step(n, carry):
        par = lax.rem(n, 2)
        finish(*bundle(par))
        low, high = ry.at[par, 0], ry.at[par, 1]

        def came(si, k):
            return rx[par, si, k * tiles : (k + 1) * tiles].reshape(Y, Z)

        def tall(a):
            if a == 0:
                near = extend(sz[0], low[1], high[1])
            else:
                mid, at = came(INDEX[a], MOMS + 5 + DEEP), DEEP + 1
                near = extend(mid, rxy[par, 0, INDEX[a], at], rxy[par, 1, INDEX[a], at])
            far = [fz[par, INDEX[c], TRAVEL[a], 0] for c in zsides]
            halves = [jnp.where(facing, far[0], near), jnp.where(facing, near, far[-1])]
            return [roll(v, -a * width, 1) for v in halves]

        parts = [tall(a) for a in (0, 1, -1)]
        def gather(three, slot, add):
            at = slot * width
            rel = lax.rem(elane + (Z - at), Z)
            v = jnp.where(rel < width, three[0], jnp.where(rel < HALF, three[2], three[1]))
            return roll(v, DEEP * block - at + add, 1)

        def packed(slot):
            halves = [gather([p[k] for p in parts], slot, HALF * k) for k in range(2)]
            return jnp.where(left, halves[0], halves[1])

        def packed_far(slot):
            shift, halves = (DEEP - slot * X) * block, []
            for k, c in enumerate(SIGNS):
                far = fz[par, INDEX[c if c in zsides else 1], TRAVEL[0], 1]
                halves.append(roll(far, shift + HALF * k, 1))
            v = jnp.where(left, halves[0], halves[1])
            for a in SIGNS:
                if slot == TRAVEL[a]:
                    at = 5 * width + 2 * INDEX[a]
                    to = ((-1 if a == 1 else X) + DEEP) * block + DEEP - 1
                    for c, far, add in ((1, 0, 0), (-1, 1, HALF + 1)):
                        one = fz[par, INDEX[c if c in zsides else 1], TRAVEL[a], 0]
                        v = jnp.where(elane == to + add, roll(one, to + add - at - far, 1), v)
            return v

        rho_z = packed(1)
        u_z = [packed(2 + d) for d in range(3)]
        old = oz[...]
        OZ = packed(0)
        for d, (shift, axis, mask) in enumerate(((block, 1, face_x), (1, 0, face_y), (1, 1, face_z))):
            t = 0.25 * (u_z[d] + roll(u_z[d], shift, axis)) * (old + roll(old, shift, axis))
            t = jnp.where(mask, t, 0.0)
            OZ = OZ + (t - roll(t, -shift, axis))
        oz[...] = OZ

        def around(px, s):
            if px < 0:
                return rxy[par, INDEX[s], 0, px + DEEP]
            if px >= X:
                return rxy[par, INDEX[s], 1, px - X]
            return ry[par, INDEX[s], 2 + px]

        def speed(px):
            if px < 0:
                tiles, mid = [rxy[par, k, 0, DEEP] for k in range(2)], came(0, 1)
            elif px >= X:
                tiles, mid = [rxy[par, k, 1, DEEP] for k in range(2)], came(1, 1)
            else:
                tiles, mid = [ry[par, k, 0 if px == 0 else X + 2] for k in range(2)], mom[1, px]
            return extend(mid, tiles[0], tiles[1])

        def line(k, a, s):
            at, r = slot_of(k, a, s)
            return rxy[par, INDEX[s], INDEX[a], at, r : r + 1, :]

        def outside(px, s):
            if px < 0:
                return line(1 if px == -1 else 2 - px, 1, s)
            if px >= X:
                return line(1 if px == X else 3 + px - X, -1, s)
            at = (0 if s == 1 else 4) + px
            return ry[par, INDEX[s], 2, at : at + 1, :]

        def inside(px, s):
            if 0 <= px < X:
                y = yend(s)
                return mom[2, px, y : y + 1, :]
            side, slot = (0, px + DEEP) if px < 0 else (1, px - X)
            at = slot if s == 1 else DEEP + slot
            return rx[par, side, singles, at : at + 1, :]

        across = {}
        for lo, hi in ((-1, 0), (X - 1, X)):
            t = 0.25 * (speed(lo) + speed(hi)) * (oe[lo + DEEP] + oe[hi + DEEP])
            across[lo], across[hi] = -t, t
        beside = roll(OZ, 1, 0) + roll(OZ, -1, 0) + roll(OZ, 1, 1) + roll(OZ, -1, 1)
        beside = beside + roll(OZ, block, 1) + roll(OZ, -block, 1)
        CZ = chemical(OZ, beside)
        scale = -0.5 * OZ
        FZ = [
            scale * (roll(CZ, -block, 1) - roll(CZ, block, 1)),
            scale * (roll(CZ, -1, 0) - roll(CZ, 1, 0)),
            scale * (roll(CZ, -1, 1) - roll(CZ, 1, 1)),
        ]

        def sided(i, w):
            a = zsign * w[2]
            for d in range(2):
                if DIRS[i][d]:
                    a = a + w[d] if DIRS[i][d] == 1 else a - w[d]
            return a

        ZH = []
        hit = collide(rho_z, u_z, FZ)
        for k, (up, down) in enumerate(ZPAIRS):
            h = halo_pair(hit(up, packed_far(k), sided))
            ZH.append(roll(h, DIRS[up][1], 0)[own_rows, :])
        own_pair = jnp.where(column == DEEP, OZ, roll(OZ, -HALF, 1))
        order_pair, chem_pair = halo_pair(OZ), halo_pair(CZ)

        OE, C, F = {}, {}, {}

        def complete(px):
            if px < 0:
                mid = came(0, MOMS + 5 + px + DEEP)
            elif px >= X:
                mid = came(1, MOMS + 5 + px - X)
            else:
                mid = base[px]
            v = extend(mid, around(px, 1), around(px, -1))
            if px in across:
                v = v + across[px]
            t = {}
            for s in SIGNS:
                y, z = yend(s), next_row(s)
                pair = oe[px + DEEP, y : y + 1, :] + oe[px + DEEP, z : z + 1, :]
                line_t = 0.25 * (outside(px, s) + inside(px, s)) * pair
                t[s] = jnp.broadcast_to(line_t, (8, Z))
            halo = v[Y:, :] + jnp.where(sub == 0, t[-1], jnp.where(sub == 7, -t[1], 0.0))
            head = v[:8, :] + jnp.where(sub == 0, t[1], 0.0)
            tail = v[Y - 8 : Y, :] - jnp.where(sub == 7, t[-1], 0.0)
            rest = [v[8 : Y - 8, :]] if Y > 16 else []
            v = jnp.concatenate([head] + rest + [tail, halo], axis=0)
            col = roll(own_pair, -((px + DEEP) * block + DEEP), 1)
            OE[px] = jnp.where((elane == 0) | (elane == Z - 1), col, v)

        def potential(px):
            o, col = OE[px], pick(order_pair, px)
            beside = OE[px - 1] + OE[px + 1] + roll(o, 1, 0) + roll(o, -1, 0)
            C[px] = chemical(o, beside + zshift(o, 1, col) + zshift(o, -1, col))

        def push(px):
            c, col = C[px], pick(chem_pair, px)
            y_dn, y_up = roll(c, 1, 0), roll(c, -1, 0)
            z_dn, z_up = zshift(c, 1, col), zshift(c, -1, col)
            scale = -0.5 * OE[px]
            F[px] = [
                scale * (C[px + 1] - C[px - 1]),
                scale * (y_up - y_dn),
                scale * (z_up - z_dn),
            ]
            if 0 <= px < X:
                lap = C[px + 1] + C[px - 1] + y_up + y_dn + z_up + z_dn - 6.0 * c
                base[px] = (OE[px] + mobility * lap)[own_rows, :]
                for s in SIGNS:
                    at = (0 if s == 1 else 4) + px
                    y = next_row(s)
                    for d in range(3):
                        fy[INDEX[s], d, at : at + 1, :] = F[px][d][y : y + 1, :]

        XH, YH, LH = {}, {}, {}

        def strike(px):
            if 0 <= px < X:
                rho = mom[0, px]
                u = [mom[1 + d, px] for d in range(3)]
                v, flat = forced(rho, 1.0 / rho, u, [f[own_rows, :] for f in F[px]])
                post[0, px] = post[0, px] + WEIGHTS[0] * flat
                for i in range(1, 19, 2):
                    a = along(i, v)
                    even = WEIGHTS[i] * flat + (4.5 * WEIGHTS[i]) * rho * (a * a)
                    odd = (3.0 * WEIGHTS[i]) * rho * a
                    post[i, px] = post[i, px] + even + odd
                    post[i + 1, px] = post[i + 1, px] + even - odd
                return
            a = 1 if px < 0 else -1
            ai = INDEX[a]
            rho = came(ai, 0)
            u = [came(ai, 1 + d) for d in range(3)]
            hit = collide(rho, u, [f[own_rows, :] for f in F[px]])
            for k, i in enumerate(CROSS[0][a]):
                XH[i] = hit(i, came(ai, MOMS + k), along)
            for s in SIGNS:
                i = DIRS.index((a, s, 0))
                r = deep_row(0, s)
                side = rxy[par, INDEX[s], ai, DEEP, r : r + 1, :]
                head = [line(0, a, s), side] + [line(k, a, s) for k in (1, 2, 3)]
                y = next_row(s)
                hit = collide(head[0], head[1:4], [f[y : y + 1, :] for f in F[px]])
                LH[i] = hit(i, head[4], along)

        for px in range(-DEEP, X + DEEP):
            complete(px)
            if px - 1 >= -2:
                potential(px - 1)
            if px - 2 >= -1:
                push(px - 2)
                strike(px - 2)
        for px in range(-DEEP, X + DEEP):
            oe[px + DEEP] = OE[px]
        O = [OE[x][own_rows, :] for x in range(X)]
        for s in SIGNS:
            si = INDEX[s]
            rho = ry[par, si, 0]
            u = [ry[par, si, 1 + d] for d in range(3)]
            hit = collide(rho, u, [fy[si, d] for d in range(3)])
            for x in range(X):
                at, r = (0 if s == 1 else 4) + x, spare(s)
                fp[si, at : at + 1, :] = ry[par, si, x, r : r + 1, :]
            for k, i in enumerate(CROSS[1][s]):
                p = ry[par, si, MOMS + k] if k < 4 else fp[si]
                YH[i] = hit(i, p, along)

        flows = {}
        pair_of = {i: k for k, both in enumerate(ZPAIRS) for i in both}
        for x in range(X):
            cols = [pick(ZH[k], x - DIRS[up][0]) for k, (up, _) in enumerate(ZPAIRS)]
            ps = []
            for i, (cx, cy, cz) in enumerate(DIRS):
                xs = x - cx
                own = 0 <= xs < X
                p = post[i, xs] if own else XH[i]
                if cy:
                    at = (0 if cy == 1 else 4) + xs
                    p = yshift(p, cy, YH[i][at : at + 1, :] if own else LH[i])
                if cz:
                    p = zshift(p, cz, cols[pair_of[i]])
                pops[i, x] = p
                ps.append(p)
            rho, moms = moments(ps)
            inv = 1.0 / rho
            flows[x] = [m * inv for m in moms]
            mom[0, x] = rho
            for d in range(3):
                mom[1 + d, x] = flows[x][d]

        tx = {0: 0.0, X: 0.0}
        for x in range(1, X):
            tx[x] = (flows[x][0] + flows[x - 1][0]) * (O[x] + O[x - 1])
        for x in range(X):
            f, o = flows[x], O[x]
            ty = jnp.where(row == 0, 0.0, (f[1] + roll(f[1], 1, 0)) * (o + roll(o, 1, 0)))
            tz = jnp.where(lane == 0, 0.0, (f[2] + roll(f[2], 1, 1)) * (o + roll(o, 1, 1)))
            change = tx[x + 1] - tx[x] + (roll(ty, -1, 0) - ty) + (roll(tz, -1, 1) - tz)
            base[x] = base[x] - 0.25 * change

        ready()

        @pl.when(n == ITERS - 1)
        def _():
            for s in SIGNS:
                cx_[INDEX[s]] = mom[1, xsrc(s)]
                y = ysrc(s)
                for x in range(X):
                    cy_[INDEX[s], 1 + x : 2 + x, :] = mom[2, x, y : y + 1, :]
                cz_[INDEX[s]] = pack([mom[3, x] for x in range(X)], s)
            launch(*farewell())

        @pl.when(n < ITERS - 1)
        def _():
            send(1 - par)

        return carry

    lax.fori_loop(0, ITERS, step, 0)
    finish(*farewell())

    pair = halo_pair(oz[...])[own_rows, :]
    for x in range(X):
        o, u = oe[x + DEEP, own_rows, :], [mom[1 + d, x] for d in range(3)]
        change = jnp.zeros((Y, Z), jnp.float32)
        if x == 0:
            change = change + (u[0] + rcx[0]) * (o + oe[DEEP - 1, own_rows, :])
        if x == X - 1:
            change = change - (u[0] + rcx[1]) * (o + oe[DEEP + X, own_rows, :])
        for s in SIGNS:
            at = next_row(s)
            other = rcy[INDEX[s], 1 + x : 2 + x, :]
            y = yend(s)
            t = (mom[2, x, y : y + 1, :] + other) * (
                oe[x + DEEP, at : at + 1, :] + oe[x + DEEP, y : y + 1, :]
            )
            t = jnp.where(row == y, jnp.broadcast_to(t, (Y, Z)), 0.0)
            side = pick(pair, x)
            beside = roll(rcz[INDEX[s]], zend(s) - (1 + x), 1)
            t = t + jnp.where(lane == zend(s), (u[2] + beside) * (o + side), 0.0)
            change = change + t if s == 1 else change - t
        order[x] = base[x] + 0.25 * change


def on_device(sizes, order_param, density, velocity):
    X, Y, Z = order_param.shape
    f32 = jnp.float32
    plane, rows, tall = (Y, Z), (8, Z), (Y + 8, Z)
    stack = (MOMS + 5 + DEEP + 1) * (Y // 8) + 1
    lines = 2 * 8 * stack + 2 * 8 * (MOMS + 4) + 4 * (DEEP + 3) * DEEP
    lines += (1 if sizes[2] == 2 else 2) * (4 * Y + 8 * DEEP)
    vmem = [
        (19, X, Y, Z), (MOMS, X, Y, Z), (X, Y, Z), (X + 2 * DEEP,) + tall, tall,
        (X, Y, Z), (3, X, Y, Z), (lines, Z),
        (2, stack) + rows, (2, 2, stack) + rows,
        (2, MOMS + 4) + rows, (2, 2, MOMS + 4) + rows,
        (2, 2, DEEP + 3) + rows, (2, 2, 2, DEEP + 3) + rows,
        (2,) + plane, (2, 2, 3, 2) + tall, (2, 3) + rows, (2,) + rows,
        (2,) + plane, (2,) + rows, (2,) + plane,
        (2,) + plane, (2,) + rows, (2,) + plane,
    ]
    sems = [(3,), (1,), (2,), (1,), (1,)]
    spec = pl.BlockSpec(memory_space=pltpu.VMEM)
    kept = pl.pallas_call(
        functools.partial(kernel, sizes),
        out_shape=(pltpu.VMEM((X, Y, Z), f32), pltpu.VMEM((19, X, Y, Z), f32)),
        in_specs=[pl.BlockSpec(memory_space=pl.ANY)] * 3,
        out_specs=(spec, spec),
        scratch_shapes=[pltpu.VMEM(s, f32) for s in vmem]
        + [pltpu.SemaphoreType.DMA(n) for n in sems],
        compiler_params=pltpu.CompilerParams(collective_id=0, has_side_effects=True),
    )(order_param, density, velocity)
    whole = pl.BlockSpec(memory_space=pl.ANY)
    return pl.pallas_call(
        write_out,
        out_shape=tuple(jax.ShapeDtypeStruct(v.shape, f32) for v in kept),
        in_specs=[whole] * 2,
        out_specs=(whole, whole),
        scratch_shapes=[pltpu.SemaphoreType.DMA((2,))],
        compiler_params=pltpu.CompilerParams(vmem_limit_bytes=1 << 20),
    )(*kept)


def write_out(order, pops, order_out, pops_out, sem):
    both = [
        pltpu.make_async_copy(pops, pops_out, sem.at[0]),
        pltpu.make_async_copy(order, order_out, sem.at[1]),
    ]
    for copy in both:
        copy.start()
    for copy in both:
        copy.wait()


def solution(mesh):
    sizes = tuple(mesh.shape[a] for a in AXES)
    return jax.shard_map(
        functools.partial(on_device, sizes),
        mesh=mesh,
        in_specs=(P("gx", "gy", "gz"), P("gx", "gy", "gz"), P(None, "gx", "gy", "gz")),
        out_specs=(P("gx", "gy", "gz"), P(None, "gx", "gy", "gz")),
        check_vma=False,
    )
```
